16 devices in a mesh: dp: 2 (over z), tp: 8 (over y, x, core).
Axes of the slice: x: 2, y: 2, z: 2, core: 2. Of those that a mesh axis runs over, the one named last changes fastest.
Arguments:
- hidden: bfloat16 [6, 128, 6144], P('dp', 'tp'), parts along dimension 0
- ln1_gain: float32 [6144], replicated
- ln1_bias: float32 [6144], replicated
- w_qkv: bfloat16 [6144, 3, 48, 128], P(None, None, 'tp')
- b_qkv: bfloat16 [3, 48, 128], P(None, 'tp')
- w_out: bfloat16 [48, 128, 6144], P('tp')
- b_out: bfloat16 [6144], replicated
- ln2_gain: float32 [6144], replicated
- ln2_bias: float32 [6144], replicated
- w_up: bfloat16 [6144, 24576], P(None, 'tp')
- b_up: bfloat16 [24576], P('tp')
- w_down: bfloat16 [24576, 6144], P('tp')
- b_down: bfloat16 [6144], replicated
Outputs:
- output: bfloat16 [6, 128, 6144], P('dp', 'tp'), parts along dimension 0
There are 2 independent parts. The reference program is written for one: setup_inputs(seed, part) draws one part's arguments, and reference() takes and returns one part's arrays. A program takes and returns all parts, laid end to end along the dimension named above; an argument that names none is the same for every part.
All inputs are finite; a program needn't handle non-finite values.
Results may differ from the reference program's by a relative error of at most 0.0102007.
Values are sent between devices in bfloat16 or wider.
A program may use at most 1 GiB of HBM per device.

```python
import math
import jax
import jax.numpy as jnp
from jax import lax

N_BATCH = 3
SEQ_LEN = 128
D_MODEL = 6144
N_HEADS = 48

HEAD_DIM = D_MODEL // N_HEADS
FF_DIM = 4 * D_MODEL
LN_EPS = 1e-5


def layer_norm(inputs, gain_vec, shift_vec):
    as_f32 = inputs.astype(jnp.float32)
    row_mean = jnp.mean(as_f32, axis=-1, keepdims=True)
    centered = as_f32 - row_mean
    variance = jnp.mean(centered * centered, axis=-1, keepdims=True)
    return (centered * lax.rsqrt(variance + LN_EPS) * gain_vec + shift_vec).astype(jnp.bfloat16)


def setup_inputs(seed: int = 0, part: int = 0) -> dict:
    root_key = jax.random.key(seed)
    sub_keys = jax.random.split(root_key, 13)
    qk_gain = (0.5 * math.log(SEQ_LEN)) ** 0.25
    col_gain = jnp.array([qk_gain, qk_gain, 1.0], jnp.float32).reshape(1, 3, 1, 1)
    hidden = jax.random.normal(jax.random.fold_in(sub_keys[0], part), (N_BATCH, SEQ_LEN, D_MODEL), jnp.float32)
    w_qkv = jax.random.normal(sub_keys[3], (D_MODEL, 3, N_HEADS, HEAD_DIM), jnp.float32) * col_gain * D_MODEL ** -0.5
    return {
        "hidden": hidden.astype(jnp.bfloat16),
        "ln1_gain": 1.0 + 0.3 * jax.random.normal(sub_keys[1], (D_MODEL,), jnp.float32),
        "ln1_bias": 0.3 * jax.random.normal(sub_keys[2], (D_MODEL,), jnp.float32),
        "w_qkv": w_qkv.astype(jnp.bfloat16),
        "b_qkv": (0.5 * jax.random.normal(sub_keys[4], (3, N_HEADS, HEAD_DIM), jnp.float32)).astype(jnp.bfloat16),
        "w_out": (jax.random.normal(sub_keys[5], (N_HEADS, HEAD_DIM, D_MODEL), jnp.float32) * D_MODEL ** -0.5).astype(jnp.bfloat16),
        "b_out": (0.3 * jax.random.normal(sub_keys[6], (D_MODEL,), jnp.float32)).astype(jnp.bfloat16),
        "ln2_gain": 1.0 + 0.3 * jax.random.normal(sub_keys[7], (D_MODEL,), jnp.float32),
        "ln2_bias": 0.3 * jax.random.normal(sub_keys[8], (D_MODEL,), jnp.float32),
        "w_up": (jax.random.normal(sub_keys[9], (D_MODEL, FF_DIM), jnp.float32) * D_MODEL ** -0.5).astype(jnp.bfloat16),
        "b_up": (0.5 * jax.random.normal(sub_keys[10], (FF_DIM,), jnp.float32)).astype(jnp.bfloat16),
        "w_down": (jax.random.normal(sub_keys[11], (FF_DIM, D_MODEL), jnp.float32) * FF_DIM ** -0.5).astype(jnp.bfloat16),
        "b_down": (0.3 * jax.random.normal(sub_keys[12], (D_MODEL,), jnp.float32)).astype(jnp.bfloat16),
    }


def reference(hidden, ln1_gain, ln1_bias, w_qkv, b_qkv, w_out, b_out, ln2_gain, ln2_bias, w_up, b_up, w_down, b_down):
    normed = layer_norm(hidden, ln1_gain, ln1_bias).reshape(N_BATCH * SEQ_LEN, D_MODEL)
    qkv_acc = jnp.dot(normed, w_qkv.reshape(D_MODEL, 3 * D_MODEL), preferred_element_type=jnp.float32)
    qkv_all = (qkv_acc + b_qkv.reshape(3 * D_MODEL).astype(jnp.float32)).astype(jnp.bfloat16)
    head_major = jnp.transpose(qkv_all.reshape(N_BATCH, SEQ_LEN, 3, N_HEADS, HEAD_DIM), (2, 3, 0, 1, 4))
    positions = jnp.arange(SEQ_LEN)
    causal = positions[:, None] >= positions[None, :]

    def one_head(operands):
        queries, keys_all, values = operands
        logits = jnp.einsum("bqd,bkd->bqk", queries.astype(jnp.float32), keys_all.astype(jnp.float32)) * HEAD_DIM ** -0.5
        logits = jnp.where(causal, logits, -1e30)
        row_max = jnp.max(logits, axis=-1, keepdims=True)
        exp_vals = jnp.exp(logits - row_max)
        weights_bf = (exp_vals / jnp.sum(exp_vals, axis=-1, keepdims=True)).astype(jnp.bfloat16)
        return jnp.einsum("bqk,bkd->bqd", weights_bf.astype(jnp.float32), values.astype(jnp.float32)).astype(jnp.bfloat16)

    context = lax.map(one_head, (head_major[0], head_major[1], head_major[2]))
    attn_sum = jnp.einsum("hbsd,hde->bse", context.astype(jnp.float32), w_out.astype(jnp.float32))
    resid_mid = (hidden.astype(jnp.float32) + (attn_sum + b_out.astype(jnp.float32))).astype(jnp.bfloat16)
    normed_mid = layer_norm(resid_mid, ln2_gain, ln2_bias).reshape(N_BATCH * SEQ_LEN, D_MODEL)
    up_proj = jnp.dot(normed_mid, w_up, preferred_element_type=jnp.float32) + b_up.astype(jnp.float32)
    gelu_out = jax.nn.gelu(up_proj, approximate=True).astype(jnp.bfloat16)
    down_sum = jnp.dot(gelu_out, w_down, preferred_element_type=jnp.float32) + b_down.astype(jnp.float32)
    return (resid_mid.astype(jnp.float32) + down_sum.reshape(N_BATCH, SEQ_LEN, D_MODEL)).astype(jnp.bfloat16)
```

```python
import functools

import jax
import jax.numpy as jnp
from jax import lax
from jax.experimental import pallas as pl
from jax.experimental.pallas import tpu as pltpu
from jax.sharding import PartitionSpec as P

MESH = pl.DeviceIdType.MESH
F32 = jnp.float32
BF16 = jnp.bfloat16
LN_EPS = 1e-5

N_DEV = 8
B, S_LOC = 3, 16
ROWS = B * S_LOC
M = N_DEV * ROWS
D = 6144
HEADS, HD = 6, 128
NQ = HEADS * HD
FF = 3072
NU = 6
KC = D // NU
NC = 768
NCH = D // NC
NS = 13
T_QKV = NU * 3
T_OUT = T_QKV + NCH
T_UP = T_OUT + NU * (FF // NC)
T_ALL = T_UP + NCH * (FF // KC)


def rows2d(v):
    return v.reshape(-1, v.shape[-1])


def kernel(x_hbm, wq_hbm, wo_hbm, wu_hbm, wd_hbm, g1_ref, c1_ref, bq_ref, bo_ref, g2_ref, c2_ref, bu_ref, bd_ref, out_ref,
           xv, hg1, hg2, acc, qkv, ctx, ub, part, s1, r1a, r1b, s2, r2a, r2b, s3, r3a, r3b, keep, x1, ring,
           x_sem, w_sem, ag_send, ag_recv, rs_send, rs_recv):
    me = lax.axis_index("tp")
    core = lax.rem(me, 2)
    xbit = lax.rem(me // 2, 2)
    ybit = me // 4
    dx = 2 - 4 * xbit
    dy = 4 - 8 * ybit
    ds = 1 - 2 * core
    sis = me + ds
    n1 = me + (1 - core) * dx + core * dy
    n2 = me + (1 - core) * dy + core * dx
    dg = me + dx + dy

    def tile_copies(i, static=None):
        slot = lax.rem(i, NS) if not isinstance(i, int) else i % NS
        buf, sem = ring.at[slot], w_sem.at[slot]

        def q_tile():
            u, t = i // 3, lax.rem(i, 3) if not isinstance(i, int) else i % 3
            k0 = pl.multiple_of(u * KC, KC)
            return [pltpu.make_async_copy(wq_hbm.at[t, h, pl.ds(k0, KC), :], buf.at[:, h * HD:(h + 1) * HD], sem) for h in range(HEADS)]

        def o_tile():
            n0 = pl.multiple_of((i - T_QKV) * NC, NC)
            return [pltpu.make_async_copy(wo_hbm.at[:, pl.ds(n0, NC)], buf.at[0:NQ, :], sem)]

        def u_tile():
            j = i - T_OUT
            k0 = pl.multiple_of((j // 4) * KC, KC)
            n0 = pl.multiple_of(lax.rem(j, 4) * NC if not isinstance(j, int) else (j % 4) * NC, NC)
            return [pltpu.make_async_copy(wu_hbm.at[pl.ds(k0, KC), pl.ds(n0, NC)], buf, sem)]

        def d_tile():
            j = i - T_UP
            n0 = pl.multiple_of((j // 3) * NC, NC)
            k0 = pl.multiple_of(lax.rem(j, 3) * KC if not isinstance(j, int) else (j % 3) * KC, KC)
            return [pltpu.make_async_copy(wd_hbm.at[pl.ds(k0, KC), pl.ds(n0, NC)], buf, sem)]

        return ((0, T_QKV, q_tile), (T_QKV, T_OUT, o_tile), (T_OUT, T_UP, u_tile), (T_UP, T_ALL, d_tile))

    def start_tile(i):
        for lo, hi, make in tile_copies(i):
            if isinstance(i, int):
                if lo <= i < hi:
                    for c in make():
                        c.start()
            else:
                @pl.when(jnp.logical_and(i >= lo, i < hi))
                def _():
                    for c in make():
                        c.start()

    def wait_tile(i, rows=KC):
        slot = lax.rem(i, NS)
        buf = ring.at[slot]
        pltpu.make_async_copy(wu_hbm.at[0:rows, 0:NC], buf.at[0:rows, :], w_sem.at[slot]).wait()
        return buf

    def ag_msg(p, hg, u, j):
        block = (me, me, me, n1, n1, n2, dg)[j]
        to = (n1, n2, sis, n2, sis, sis, sis)[j]
        return pltpu.make_async_remote_copy(
            src_ref=hg.at[u, block], dst_ref=hg.at[u, block], send_sem=ag_send.at[p, u, j], recv_sem=ag_recv.at[p, u, j],
            device_id={"tp": to}, device_id_type=MESH)

    def ag_wait_recv(p, hg, u, j):
        block = (n1, n2, sis, dg, n2 + ds, n1 + ds, dg + ds)[j]
        pltpu.make_async_remote_copy(
            src_ref=hg.at[u, block], dst_ref=hg.at[u, block], send_sem=ag_send.at[p, u, j], recv_sem=ag_recv.at[p, u, j],
            device_id={"tp": me}, device_id_type=MESH).wait_recv()

    def ag_own(p, hg, u):
        for j in (0, 1, 2):
            ag_msg(p, hg, u, j).start()

    def ag_step(p, hg, u, compute):
        @pl.when(u < NU)
        def _():
            ag_wait_recv(p, hg, u, 0)
            ag_msg(p, hg, u, 3).start()
            ag_msg(p, hg, u, 4).start()
            ag_wait_recv(p, hg, u, 1)
            ag_msg(p, hg, u, 5).start()

        @pl.when(u + 2 < NU)
        def _():
            ag_own(p, hg, u + 2)

        @pl.when(jnp.logical_and(u >= 1, u < NU + 1))
        def _():
            ag_wait_recv(p, hg, u - 1, 3)
            ag_msg(p, hg, u - 1, 6).start()

        @pl.when(u >= 2)
        def _():
            for j in (2, 4, 5, 6):
                ag_wait_recv(p, hg, u - 2, j)
            compute(u - 2)

    def ag_drain(p, hg):
        def body(u, _):
            for j in range(7):
                ag_msg(p, hg, u, j).wait_send()
            return 0
        lax.fori_loop(0, NU, body, 0)

    def rs_msg(p, n, j, r1, r2, r3):
        src = (s1, s2, s3)[j]
        dst = (r1, r2, r3)[j]
        to = (sis, n1, n2)[j]
        return pltpu.make_async_remote_copy(
            src_ref=src.at[n], dst_ref=dst.at[n], send_sem=rs_send.at[p, n, j], recv_sem=rs_recv.at[p, n, j],
            device_id={"tp": to}, device_id_type=MESH)

    c_me, c_n1, c_n2, c_dg = me // 2, n1 // 2, n2 // 2, dg // 2

    def rs_phase(p, r1, r2, r3, product, finish):
        def body(n, _):
            @pl.when(n < NCH)
            def _():
                product(n, lax.rem(n, 2))
                for q in range(4):
                    s1[n, q] = part[lax.rem(n, 2), 2 * q + 1 - core].astype(BF16)

                rs_msg(p, n, 0, r1, r2, r3).start()

            @pl.when(jnp.logical_and(n >= 1, n < NCH + 1))
            def _():
                m = n - 1
                rs_msg(p, m, 0, r1, r2, r3).wait_recv()
                slot = lax.rem(m, 2)

                def total(q):
                    return part[slot, 2 * q + core] + r1[m, q].astype(F32)

                s2[m, 0] = total(c_n1).astype(BF16)
                s2[m, 1] = total(c_dg).astype(BF16)
                keep[m, 0] = total(c_me)
                keep[m, 1] = total(c_n2)
                rs_msg(p, m, 1, r1, r2, r3).start()

            @pl.when(jnp.logical_and(n >= 3, n < NCH + 3))
            def _():
                m = n - 3
                rs_msg(p, m, 1, r1, r2, r3).wait_recv()
                s3[m] = (keep[m, 1] + r2[m, 1].astype(F32)).astype(BF16)
                keep[m, 0] = keep[m, 0] + r2[m, 0].astype(F32)
                rs_msg(p, m, 2, r1, r2, r3).start()

            @pl.when(n >= 5)
            def _():
                m = n - 5
                rs_msg(p, m, 2, r1, r2, r3).wait_recv()
                finish(m, keep[m, 0] + r3[m].astype(F32))
            return 0

        lax.fori_loop(0, NCH + 5, body, 0)

        def drain(n, _):
            for j in range(3):
                rs_msg(p, n, j, r1, r2, r3).wait_send()
            return 0
        lax.fori_loop(0, NCH, drain, 0)

    def layer_norm(load, g_ref, c_ref, hg):
        stats = []
        for b in range(B):
            xf = load(b).astype(F32)
            mean = jnp.mean(xf, axis=-1, keepdims=True)
            cen = xf - mean
            var = jnp.mean(cen * cen, axis=-1, keepdims=True)
            stats.append((mean, lax.rsqrt(var + LN_EPS)))
        for u in range(NU):
            cols = slice(u * KC, (u + 1) * KC)
            for b in range(B):
                mean, rstd = stats[b]
                h = (load(b, cols).astype(F32) - mean) * rstd * g_ref[:, cols] + c_ref[:, cols]
                hg[u, me, b * S_LOC:(b + 1) * S_LOC, :] = h.astype(BF16)

    x_copy = pltpu.make_async_copy(x_hbm, xv, x_sem)
    x_copy.start()
    for i in range(NS):
        start_tile(i)
    barrier = pltpu.get_barrier_semaphore()
    for other in (sis, n1, n2):
        pl.semaphore_signal(barrier, inc=1, device_id={"tp": other}, device_id_type=MESH)
    pl.semaphore_wait(barrier, 3)
    x_copy.wait()

    layer_norm(lambda b, cols=slice(None): xv[b, :, cols], g1_ref, c1_ref, hg1)
    ag_own(0, hg1, 0)
    ag_own(0, hg1, 1)

    acc[:, 0:3 * NQ] = jnp.zeros((M, 3 * NQ), F32)

    def qkv_chunk(u):
        lhs = rows2d(hg1[u])
        for t in range(3):
            i = u * 3 + t
            w = wait_tile(i)
            acc[:, t * NQ:(t + 1) * NQ] += jnp.dot(lhs, w[...], preferred_element_type=F32)
            start_tile(i + NS)

    def qkv_body(u, _):
        ag_step(0, hg1, u, qkv_chunk)
        return 0
    lax.fori_loop(0, NU + 2, qkv_body, 0)
    ag_drain(0, hg1)

    for t in range(3):
        bias = bq_ref[t].astype(F32)
        for h in range(HEADS):
            c0 = (t * HEADS + h) * HD
            v = acc[:, c0:c0 + HD] + bias[h:h + 1, :]
            qkv[:, :, :, c0:c0 + HD] = v.astype(BF16).reshape(N_DEV, B, S_LOC, HD)

    seq = N_DEV * S_LOC
    causal = lax.broadcasted_iota(jnp.int32, (seq, seq), 0) >= lax.broadcasted_iota(jnp.int32, (seq, seq), 1)

    def attn_body(h, _):
        for b in range(B):
            def head(t):
                c0 = pl.multiple_of((t * HEADS + h) * HD, HD)
                return rows2d(qkv[:, b, :, pl.ds(c0, HD)])
            q, k, v = head(0), head(1), head(2)
            logits = lax.dot_general(q, k, (((1,), (1,)), ((), ())), preferred_element_type=F32) * HD ** -0.5
            logits = jnp.where(causal, logits, -1e30)
            e = jnp.exp(logits - jnp.max(logits, axis=-1, keepdims=True))
            w = (e / jnp.sum(e, axis=-1, keepdims=True)).astype(BF16)
            o = jnp.dot(w, v, preferred_element_type=F32).astype(BF16)
            ctx[:, b, :, pl.ds(pl.multiple_of(h * HD, HD), HD)] = o.reshape(N_DEV, S_LOC, HD)
        return 0
    lax.fori_loop(0, HEADS, attn_body, 0)

    def out_product(n, slot):
        w = wait_tile(T_QKV + n, NQ)
        part[slot] = jnp.dot(rows2d(ctx[...]), w[0:NQ, :], preferred_element_type=F32).reshape(N_DEV, ROWS, NC)
        start_tile(T_QKV + n + NS)

    def out_finish(n, total):
        cols = pl.ds(pl.multiple_of(n * NC, NC), NC)
        xs = rows2d(xv[:, :, cols]).astype(F32)
        x1[:, cols] = (xs + (total + bo_ref[:, cols])).astype(BF16)

    rs_phase(0, r1a, r2a, r3a, out_product, out_finish)

    layer_norm(lambda b, cols=slice(None): x1[b * S_LOC:(b + 1) * S_LOC, cols], g2_ref, c2_ref, hg2)
    ag_own(1, hg2, 0)
    ag_own(1, hg2, 1)

    acc[...] = jnp.zeros((M, FF), F32)

    def up_chunk(u):
        lhs = rows2d(hg2[u])
        for n in range(FF // NC):
            i = T_OUT + u * (FF // NC) + n
            w = wait_tile(i)
            acc[:, n * NC:(n + 1) * NC] += jnp.dot(lhs, w[...], preferred_element_type=F32)
            start_tile(i + NS)

    def up_body(u, _):
        ag_step(1, hg2, u, up_chunk)
        return 0
    lax.fori_loop(0, NU + 2, up_body, 0)
    ag_drain(1, hg2)

    def gelu_body(d, _):
        r = pl.ds(pl.multiple_of(d * ROWS, ROWS), ROWS)
        ub[r, :] = jax.nn.gelu(acc[r, :] + bu_ref[...], approximate=True).astype(BF16)
        return 0
    lax.fori_loop(0, N_DEV, gelu_body, 0)

    def down_product(n, slot):
        for k in range(FF // KC):
            i = T_UP + n * (FF // KC) + k
            w = wait_tile(i)
            d = jnp.dot(ub[:, k * KC:(k + 1) * KC], w[...], preferred_element_type=F32).reshape(N_DEV, ROWS, NC)
            if k == 0:
                part[slot] = d
            else:
                part[slot] += d
            start_tile(i + NS)

    def down_finish(n, total):
        cols = pl.ds(pl.multiple_of(n * NC, NC), NC)
        res = x1[:, cols].astype(F32) + (total + bd_ref[:, cols])
        out_ref[:, :, cols] = res.astype(BF16).reshape(B, S_LOC, NC)

    rs_phase(1, r1b, r2b, r3b, down_product, down_finish)


def solution(mesh):
    def device_body(hidden, ln1_gain, ln1_bias, w_qkv, b_qkv, w_out, b_out, ln2_gain, ln2_bias, w_up, b_up, w_down, b_down):
        any_spec = pl.BlockSpec(memory_space=pl.ANY)
        vmem = pl.BlockSpec(memory_space=pltpu.VMEM)

        def row(v):
            return v.astype(F32).reshape(1, -1)

        rs_buf = [pltpu.VMEM((NCH, 4, ROWS, NC), BF16), pltpu.VMEM((NCH, 2, ROWS, NC), BF16), pltpu.VMEM((NCH, ROWS, NC), BF16)]
        return pl.pallas_call(
            kernel,
            out_shape=jax.ShapeDtypeStruct((B, S_LOC, D), BF16),
            in_specs=[any_spec] * 5 + [vmem] * 8,
            out_specs=vmem,
            scratch_shapes=[
                pltpu.VMEM((B, S_LOC, D), BF16),
                pltpu.VMEM((NU, N_DEV, ROWS, KC), BF16),
                pltpu.VMEM((NU, N_DEV, ROWS, KC), BF16),
                pltpu.VMEM((M, FF), F32),
                pltpu.VMEM((N_DEV, B, S_LOC, 3 * NQ), BF16),
                pltpu.VMEM((N_DEV, B, S_LOC, NQ), BF16),
                pltpu.VMEM((M, FF), BF16),
                pltpu.VMEM((2, N_DEV, ROWS, NC), F32),
                rs_buf[0], rs_buf[0], rs_buf[0],
                rs_buf[1], rs_buf[1], rs_buf[1],
                rs_buf[2], rs_buf[2], rs_buf[2],
                pltpu.VMEM((NCH, 2, ROWS, NC), F32),
                pltpu.VMEM((ROWS, D), BF16),
                pltpu.VMEM((NS, KC, NC), BF16),
                pltpu.SemaphoreType.DMA,
                pltpu.SemaphoreType.DMA((NS,)),
                pltpu.SemaphoreType.DMA((2, NU, 7)),
                pltpu.SemaphoreType.DMA((2, NU, 7)),
                pltpu.SemaphoreType.DMA((2, NCH, 3)),
                pltpu.SemaphoreType.DMA((2, NCH, 3)),
            ],
            compiler_params=pltpu.CompilerParams(collective_id=0, has_side_effects=True, vmem_limit_bytes=67_043_328),
            name="decoder_layer",
        )(hidden, jnp.transpose(w_qkv, (1, 2, 0, 3)), w_out.reshape(HEADS * HD, D), w_up, w_down,
          row(ln1_gain), row(ln1_bias), b_qkv, row(b_out), row(ln2_gain), row(ln2_bias), row(b_up), row(b_down))

    in_layout = (P("dp", "tp", None), P(), P(), P(None, None, "tp", None), P(None, "tp", None), P("tp", None, None), P(), P(), P(), P(None, "tp"), P("tp"), P("tp", None), P())
    return jax.shard_map(device_body, mesh=mesh, in_specs=in_layout, out_specs=P("dp", "tp", None), check_vma=False)
```

```python
import functools

import jax
import jax.numpy as jnp
from jax import lax
from jax.experimental import pallas as pl
from jax.experimental.pallas import tpu as pltpu
from jax.sharding import PartitionSpec as P

MESH = pl.DeviceIdType.MESH
F32 = jnp.float32
BF16 = jnp.bfloat16
LN_EPS = 1e-5

N_DEV = 8
B, S_LOC = 3, 16
ROWS = B * S_LOC
M = N_DEV * ROWS
D = 6144
HEADS, HD = 6, 128
NQ = HEADS * HD
FF = 3072
NU = 6
KC = D // NU
NC = 768
NCH = D // NC
NS = 13
T_QKV = NU * 3
T_OUT = T_QKV + NCH
T_UP = T_OUT + NU * (FF // NC)
T_ALL = T_UP + NCH * (FF // KC)


def rows2d(v):
    return v.reshape(-1, v.shape[-1])


def kernel(x_hbm, wq_hbm, wo_hbm, wu_hbm, wd_hbm, g1_ref, c1_ref, bq_ref, bo_ref, g2_ref, c2_ref, bu_ref, bd_ref, out_ref,
           xv, hg1, hg2, acc, qkv, ctx, ub, part, s1, r1a, r1b, s2, r2a, r2b, s3, r3a, r3b, keep, x1, ring, bo_row, bd_row, bu_row,
           x_sem, w_sem, ag_send, ag_recv, rs_send, rs_recv):
    me = lax.axis_index("tp")
    core = lax.rem(me, 2)
    xbit = lax.rem(me // 2, 2)
    ybit = me // 4
    dx = 2 - 4 * xbit
    dy = 4 - 8 * ybit
    ds = 1 - 2 * core
    sis = me + ds
    n1 = me + (1 - core) * dx + core * dy
    n2 = me + (1 - core) * dy + core * dx
    dg = me + dx + dy

    def tile_copies(i, static=None):
        slot = lax.rem(i, NS) if not isinstance(i, int) else i % NS
        buf, sem = ring.at[slot], w_sem.at[slot]

        def q_tile():
            u, t = i // 3, lax.rem(i, 3) if not isinstance(i, int) else i % 3
            k0 = pl.multiple_of(u * KC, KC)
            return [pltpu.make_async_copy(wq_hbm.at[t, h, pl.ds(k0, KC), :], buf.at[:, h * HD:(h + 1) * HD], sem) for h in range(HEADS)]

        def o_tile():
            n0 = pl.multiple_of((i - T_QKV) * NC, NC)
            return [pltpu.make_async_copy(wo_hbm.at[:, pl.ds(n0, NC)], buf.at[0:NQ, :], sem)]

        def u_tile():
            j = i - T_OUT
            k0 = pl.multiple_of((j // 4) * KC, KC)
            n0 = pl.multiple_of(lax.rem(j, 4) * NC if not isinstance(j, int) else (j % 4) * NC, NC)
            return [pltpu.make_async_copy(wu_hbm.at[pl.ds(k0, KC), pl.ds(n0, NC)], buf, sem)]

        def d_tile():
            j = i - T_UP
            n0 = pl.multiple_of((j // 3) * NC, NC)
            k0 = pl.multiple_of(lax.rem(j, 3) * KC if not isinstance(j, int) else (j % 3) * KC, KC)
            return [pltpu.make_async_copy(wd_hbm.at[pl.ds(k0, KC), pl.ds(n0, NC)], buf, sem)]

        return ((0, T_QKV, q_tile), (T_QKV, T_OUT, o_tile), (T_OUT, T_UP, u_tile), (T_UP, T_ALL, d_tile))

    def start_tile(i):
        for lo, hi, make in tile_copies(i):
            if isinstance(i, int):
                if lo <= i < hi:
                    for c in make():
                        c.start()
            else:
                @pl.when(jnp.logical_and(i >= lo, i < hi))
                def _():
                    for c in make():
                        c.start()

    def wait_tile(i, rows=KC):
        slot = lax.rem(i, NS)
        buf = ring.at[slot]
        pltpu.make_async_copy(wu_hbm.at[0:rows, 0:NC], buf.at[0:rows, :], w_sem.at[slot]).wait()
        return buf

    def ag_msg(p, hg, u, j):
        block = (me, me, me, n1, n1, n2, dg)[j]
        to = (n1, n2, sis, n2, sis, sis, sis)[j]
        return pltpu.make_async_remote_copy(
            src_ref=hg.at[u, block], dst_ref=hg.at[u, block], send_sem=ag_send.at[p, u, j], recv_sem=ag_recv.at[p, u, j],
            device_id={"tp": to}, device_id_type=MESH)

    def ag_wait_recv(p, hg, u, j):
        block = (n1, n2, sis, dg, n2 + ds, n1 + ds, dg + ds)[j]
        pltpu.make_async_remote_copy(
            src_ref=hg.at[u, block], dst_ref=hg.at[u, block], send_sem=ag_send.at[p, u, j], recv_sem=ag_recv.at[p, u, j],
            device_id={"tp": me}, device_id_type=MESH).wait_recv()

    def ag_own(p, hg, u):
        for j in (0, 1, 2):
            ag_msg(p, hg, u, j).start()

    def ag_step(p, hg, u, compute):
        @pl.when(u < NU)
        def _():
            ag_wait_recv(p, hg, u, 0)
            ag_msg(p, hg, u, 3).start()
            ag_msg(p, hg, u, 4).start()
            ag_wait_recv(p, hg, u, 1)
            ag_msg(p, hg, u, 5).start()

        @pl.when(u + 2 < NU)
        def _():
            ag_own(p, hg, u + 2)

        @pl.when(jnp.logical_and(u >= 1, u < NU + 1))
        def _():
            ag_wait_recv(p, hg, u - 1, 3)
            ag_msg(p, hg, u - 1, 6).start()

        @pl.when(u >= 2)
        def _():
            for j in (2, 4, 5, 6):
                ag_wait_recv(p, hg, u - 2, j)
            compute(u - 2)

    def ag_drain(p, hg):
        def body(u, _):
            for j in range(7):
                ag_msg(p, hg, u, j).wait_send()
            return 0
        lax.fori_loop(0, NU, body, 0)

    def rs_msg(p, n, j, r1, r2, r3):
        src = (s1, s2, s3)[j]
        dst = (r1, r2, r3)[j]
        to = (sis, n1, n2)[j]
        return pltpu.make_async_remote_copy(
            src_ref=src.at[n], dst_ref=dst.at[n], send_sem=rs_send.at[p, n, j], recv_sem=rs_recv.at[p, n, j],
            device_id={"tp": to}, device_id_type=MESH)

    c_me, c_n1, c_n2, c_dg = me // 2, n1 // 2, n2 // 2, dg // 2

    def rs_phase(p, r1, r2, r3, product, finish):
        def body(n, _):
            @pl.when(n < NCH)
            def _():
                product(n, lax.rem(n, 2))
                for q in range(4):
                    s1[n, q] = part[lax.rem(n, 2), 2 * q + 1 - core].astype(BF16)

                rs_msg(p, n, 0, r1, r2, r3).start()

            @pl.when(jnp.logical_and(n >= 1, n < NCH + 1))
            def _():
                m = n - 1
                rs_msg(p, m, 0, r1, r2, r3).wait_recv()
                slot = lax.rem(m, 2)

                def total(q):
                    return part[slot, 2 * q + core] + r1[m, q].astype(F32)

                s2[m, 0] = total(c_n1).astype(BF16)
                s2[m, 1] = total(c_dg).astype(BF16)
                keep[m, 0] = total(c_me)
                keep[m, 1] = total(c_n2)
                rs_msg(p, m, 1, r1, r2, r3).start()

            @pl.when(jnp.logical_and(n >= 3, n < NCH + 3))
            def _():
                m = n - 3
                rs_msg(p, m, 1, r1, r2, r3).wait_recv()
                s3[m] = (keep[m, 1] + r2[m, 1].astype(F32)).astype(BF16)
                keep[m, 0] = keep[m, 0] + r2[m, 0].astype(F32)
                rs_msg(p, m, 2, r1, r2, r3).start()

            @pl.when(n >= 5)
            def _():
                m = n - 5
                rs_msg(p, m, 2, r1, r2, r3).wait_recv()
                finish(m, keep[m, 0] + r3[m].astype(F32))
            return 0

        lax.fori_loop(0, NCH + 5, body, 0)

        def drain(n, _):
            for j in range(3):
                rs_msg(p, n, j, r1, r2, r3).wait_send()
            return 0
        lax.fori_loop(0, NCH, drain, 0)

    def layer_norm(load, g_ref, c_ref, hg):
        stats = []
        for b in range(B):
            xf = load(b).astype(F32)
            mean = jnp.mean(xf, axis=-1, keepdims=True)
            cen = xf - mean
            var = jnp.mean(cen * cen, axis=-1, keepdims=True)
            stats.append((mean, lax.rsqrt(var + LN_EPS)))
        for u in range(NU):
            cols = slice(u * KC, (u + 1) * KC)
            for b in range(B):
                mean, rstd = stats[b]
                h = (load(b, cols).astype(F32) - mean) * rstd * g_ref[:, cols] + c_ref[:, cols]
                hg[u, me, b * S_LOC:(b + 1) * S_LOC, :] = h.astype(BF16)

    x_copy = pltpu.make_async_copy(x_hbm, xv, x_sem)
    x_copy.start()
    barrier = pltpu.get_barrier_semaphore()
    for other in (sis, n1, n2):
        pl.semaphore_signal(barrier, inc=1, device_id={"tp": other}, device_id_type=MESH)
    for dst, src in ((bo_row, bo_ref), (bd_row, bd_ref), (bu_row, bu_ref)):
        wide = src[...].astype(F32)
        for r in range(src.shape[0]):
            dst[:, r * HD:(r + 1) * HD] = wide[r:r + 1, :]
    x_copy.wait()
    for i in range(NS):
        start_tile(i)
    pl.semaphore_wait(barrier, 3)

    layer_norm(lambda b, cols=slice(None): xv[b, :, cols], g1_ref, c1_ref, hg1)
    ag_own(0, hg1, 0)
    ag_own(0, hg1, 1)

    acc[:, 0:3 * NQ] = jnp.zeros((M, 3 * NQ), F32)

    def qkv_chunk(u):
        ws = [wait_tile(u * 3 + t) for t in range(3)]
        lhs = rows2d(hg1[u])
        for t in range(3):
            acc[:, t * NQ:(t + 1) * NQ] += jnp.dot(lhs, ws[t][...], preferred_element_type=F32)
        for t in range(3):
            start_tile(u * 3 + t + NS)

    def qkv_body(u, _):
        ag_step(0, hg1, u, qkv_chunk)
        return 0
    lax.fori_loop(0, NU + 2, qkv_body, 0)
    ag_drain(0, hg1)

    for t in range(3):
        bias = bq_ref[t].astype(F32)
        for h in range(HEADS):
            c0 = (t * HEADS + h) * HD
            v = acc[:, c0:c0 + HD] + bias[h:h + 1, :]
            qkv[:, :, :, c0:c0 + HD] = v.astype(BF16).reshape(N_DEV, B, S_LOC, HD)

    seq = N_DEV * S_LOC
    causal = lax.broadcasted_iota(jnp.int32, (seq, seq), 0) >= lax.broadcasted_iota(jnp.int32, (seq, seq), 1)

    def attn_body(h, _):
        for b in range(B):
            def head(t):
                c0 = pl.multiple_of((t * HEADS + h) * HD, HD)
                return rows2d(qkv[:, b, :, pl.ds(c0, HD)])
            q, k, v = head(0), head(1), head(2)
            logits = lax.dot_general(q, k, (((1,), (1,)), ((), ())), preferred_element_type=F32) * HD ** -0.5
            logits = jnp.where(causal, logits, -1e30)
            e = jnp.exp(logits - jnp.max(logits, axis=-1, keepdims=True))
            w = (e / jnp.sum(e, axis=-1, keepdims=True)).astype(BF16)
            o = jnp.dot(w, v, preferred_element_type=F32).astype(BF16)
            ctx[:, b, :, pl.ds(pl.multiple_of(h * HD, HD), HD)] = o.reshape(N_DEV, S_LOC, HD)
        return 0
    lax.fori_loop(0, HEADS, attn_body, 0)

    def out_product(n, slot):
        w = wait_tile(T_QKV + n, NQ)
        part[slot] = jnp.dot(rows2d(ctx[...]), w[0:NQ, :], preferred_element_type=F32).reshape(N_DEV, ROWS, NC)
        start_tile(T_QKV + n + NS)

    def out_finish(n, total):
        cols = pl.ds(pl.multiple_of(n * NC, NC), NC)
        xs = rows2d(xv[:, :, cols]).astype(F32)
        x1[:, cols] = (xs + (total + bo_row[:, cols])).astype(BF16)

    rs_phase(0, r1a, r2a, r3a, out_product, out_finish)

    layer_norm(lambda b, cols=slice(None): x1[b * S_LOC:(b + 1) * S_LOC, cols], g2_ref, c2_ref, hg2)
    ag_own(1, hg2, 0)
    ag_own(1, hg2, 1)

    acc[...] = jnp.zeros((M, FF), F32)

    def up_chunk(u):
        ws = [wait_tile(T_OUT + u * 4 + n) for n in range(4)]
        lhs = rows2d(hg2[u])
        for n in range(4):
            for h in range(3):
                c = n * NC + h * 256
                acc[:, c:c + 256] += jnp.dot(lhs, ws[n][:, h * 256:(h + 1) * 256], preferred_element_type=F32)
        for n in range(4):
            start_tile(T_OUT + u * 4 + n + NS)

    def up_body(u, _):
        ag_step(1, hg2, u, up_chunk)
        return 0
    lax.fori_loop(0, NU + 2, up_body, 0)
    ag_drain(1, hg2)

    def gelu_body(d, _):
        r = pl.ds(pl.multiple_of(d * ROWS, ROWS), ROWS)
        ub[r, :] = jax.nn.gelu(acc[r, :] + bu_row[...], approximate=True).astype(BF16)
        return 0
    lax.fori_loop(0, N_DEV, gelu_body, 0)

    def down_product(n, slot):
        ws = [wait_tile(T_UP + n * 3 + k) for k in range(3)]
        for h in range(3):
            d = sum(jnp.dot(ub[:, k * KC:(k + 1) * KC], ws[k][:, h * 256:(h + 1) * 256], preferred_element_type=F32) for k in range(3))
            part[slot, :, :, h * 256:(h + 1) * 256] = d.reshape(N_DEV, ROWS, 256)
        for k in range(3):
            start_tile(T_UP + n * 3 + k + NS)

    def down_finish(n, total):
        cols = pl.ds(pl.multiple_of(n * NC, NC), NC)
        res = x1[:, cols].astype(F32) + (total + bd_row[:, cols])
        out_ref[:, :, cols] = res.astype(BF16).reshape(B, S_LOC, NC)

    rs_phase(1, r1b, r2b, r3b, down_product, down_finish)


def solution(mesh):
    def device_body(hidden, ln1_gain, ln1_bias, w_qkv, b_qkv, w_out, b_out, ln2_gain, ln2_bias, w_up, b_up, w_down, b_down):
        any_spec = pl.BlockSpec(memory_space=pl.ANY)
        vmem = pl.BlockSpec(memory_space=pltpu.VMEM)

        def row(v):
            return v.reshape(1, -1)

        def tile(v):
            return v.reshape(-1, HD)

        rs_buf = [pltpu.VMEM((NCH, 4, ROWS, NC), BF16), pltpu.VMEM((NCH, 2, ROWS, NC), BF16), pltpu.VMEM((NCH, ROWS, NC), BF16)]
        return pl.pallas_call(
            kernel,
            out_shape=jax.ShapeDtypeStruct((B, S_LOC, D), BF16),
            in_specs=[any_spec] * 5 + [vmem] * 8,
            out_specs=vmem,
            scratch_shapes=[
                pltpu.VMEM((B, S_LOC, D), BF16),
                pltpu.VMEM((NU, N_DEV, ROWS, KC), BF16),
                pltpu.VMEM((NU, N_DEV, ROWS, KC), BF16),
                pltpu.VMEM((M, FF), F32),
                pltpu.VMEM((N_DEV, B, S_LOC, 3 * NQ), BF16),
                pltpu.VMEM((N_DEV, B, S_LOC, NQ), BF16),
                pltpu.VMEM((M, FF), BF16),
                pltpu.VMEM((2, N_DEV, ROWS, NC), F32),
                rs_buf[0], rs_buf[0], rs_buf[0],
                rs_buf[1], rs_buf[1], rs_buf[1],
                rs_buf[2], rs_buf[2], rs_buf[2],
                pltpu.VMEM((NCH, 2, ROWS, NC), F32),
                pltpu.VMEM((ROWS, D), BF16),
                pltpu.VMEM((NS, KC, NC), BF16),
                pltpu.VMEM((1, D), F32),
                pltpu.VMEM((1, D), F32),
                pltpu.VMEM((1, FF), F32),
                pltpu.SemaphoreType.DMA,
                pltpu.SemaphoreType.DMA((NS,)),
                pltpu.SemaphoreType.DMA((2, NU, 7)),
                pltpu.SemaphoreType.DMA((2, NU, 7)),
                pltpu.SemaphoreType.DMA((2, NCH, 3)),
                pltpu.SemaphoreType.DMA((2, NCH, 3)),
            ],
            compiler_params=pltpu.CompilerParams(collective_id=0, has_side_effects=True, vmem_limit_bytes=66_000_000),
            name="decoder_layer",
        )(hidden, jnp.transpose(w_qkv, (1, 2, 0, 3)), w_out.reshape(HEADS * HD, D), w_up, w_down,
          row(ln1_gain), row(ln1_bias), b_qkv, tile(b_out), row(ln2_gain), row(ln2_bias), tile(b_up), tile(b_down))

    in_layout = (P("dp", "tp", None), P(), P(), P(None, None, "tp", None), P(None, "tp", None), P("tp", None, None), P(), P(), P(), P(None, "tp"), P("tp"), P("tp", None), P())
    return jax.shard_map(device_body, mesh=mesh, in_specs=in_layout, out_specs=P("dp", "tp", None), check_vma=False)
```

```python
import jax
import jax.numpy as jnp
from jax import lax
from jax.experimental import pallas as pl
from jax.experimental.pallas import tpu as pltpu
from jax.sharding import PartitionSpec as P

MESH = pl.DeviceIdType.MESH
F32 = jnp.float32
BF16 = jnp.bfloat16
LN_EPS = 1e-5

N_DEV = 8
B, S_LOC = 3, 16
ROWS = B * S_LOC
SEQ = N_DEV * S_LOC
M = N_DEV * ROWS
D = 6144
HEADS, HD = 6, 128
NQ = HEADS * HD
FF = 3072
KC = 1024
NC = 768
NP = NC // 3
NU = D // KC
HALF = D // 2
NV = 2 * B
NCH = 12
CW = 512
NS = 17
T_SEQ = 18 + 8
T_OUT = B * T_SEQ
T_UP = T_OUT + NU * (FF // NC)
T_ALL = T_UP + NCH * 2


def rows2d(v):
    return v.reshape(-1, v.shape[-1])


def dot(a, b):
    return jnp.dot(a, b, preferred_element_type=F32)


def kernel(x_hbm, wq_hbm, wo_hbm, wu_hbm, wd_hbm, g1_ref, c1_ref, bq_ref, bo_ref, g2_ref, c2_ref, bu_ref, bd_ref, out_ref,
           xv, hg1, hg2, acc, qkv, ctx, ub, part, s1, r1, s2, r2, s3, r3, keep, x1, ring, bo_row, bd_row, bu_row,
           x_sem, w_sem, a1_send, a1_recv, a2_send, a2_recv, rs_send, rs_recv):
    me = lax.axis_index("tp")
    core = lax.rem(me, 2)
    xbit = lax.rem(me // 2, 2)
    ybit = me // 4
    dx = 2 - 4 * xbit
    dy = 4 - 8 * ybit
    ds = 1 - 2 * core
    sis = me + ds
    n1 = me + (1 - core) * dx + core * dy
    n2 = me + (1 - core) * dy + core * dx
    dg = me + dx + dy
    c_me, c_n1, c_n2, c_dg = me // 2, n1 // 2, n2 // 2, dg // 2

    def start_tile(i):
        slot = lax.rem(i, NS)
        buf, sem = ring.at[slot], w_sem.at[slot]

        @pl.when(i < T_OUT)
        def _():
            r = lax.rem(i, T_SEQ)

            @pl.when(r < 18)
            def _():
                k0 = pl.multiple_of(lax.rem(r, NU) * KC, KC)
                for h in range(HEADS):
                    pltpu.make_async_copy(wq_hbm.at[r // NU, h, pl.ds(k0, KC), :], buf.at[:, h * HD:(h + 1) * HD], sem).start()

            @pl.when(r >= 18)
            def _():
                n0 = pl.multiple_of((r - 18) * NC, NC)
                pltpu.make_async_copy(wo_hbm.at[:, pl.ds(n0, NC)], buf.at[0:NQ, :], sem).start()

        @pl.when(jnp.logical_and(i >= T_OUT, i < T_UP))
        def _():
            j = i - T_OUT
            k0 = pl.multiple_of((j // 4) * KC, KC)
            n0 = pl.multiple_of(lax.rem(j, 4) * NC, NC)
            pltpu.make_async_copy(wu_hbm.at[pl.ds(k0, KC), pl.ds(n0, NC)], buf, sem).start()

        @pl.when(jnp.logical_and(i >= T_UP, i < T_ALL))
        def _():
            j = i - T_UP
            for p in range(3):
                b = lax.rem(j, 2) * 3 + p
                k0 = pl.multiple_of((b // 2) * KC, KC)
                n0 = pl.multiple_of((j // 2) * CW + lax.rem(b, 2) * NP, NP)
                pltpu.make_async_copy(wd_hbm.at[pl.ds(k0, KC), pl.ds(n0, NP)], buf.at[:, p * NP:(p + 1) * NP], sem).start()

    def start_tiles(i, count):
        def body(k, _):
            start_tile(i + k)
            return 0
        lax.fori_loop(0, count, body, 0)

    def wait_tile(i, rows=KC):
        slot = lax.rem(i, NS)
        buf = ring.at[slot]
        pltpu.make_async_copy(wu_hbm.at[0:rows, 0:NC], buf.at[0:rows, :], w_sem.at[slot]).wait()
        return buf

    def a1_copy(v, j, block, to):
        ref = hg1.at[v, block]
        return pltpu.make_async_remote_copy(src_ref=ref, dst_ref=ref, send_sem=a1_send.at[v, j], recv_sem=a1_recv.at[v, j],
                                            device_id={"tp": to}, device_id_type=MESH)

    def a2_copy(u, h, j, block, to):
        ref = hg2.at[u, block, pl.ds(32 * h, 32 - 16 * h), :]
        return pltpu.make_async_remote_copy(src_ref=ref, dst_ref=ref, send_sem=a2_send.at[u, h, j], recv_sem=a2_recv.at[u, h, j],
                                            device_id={"tp": to}, device_id_type=MESH)

    def send(make, j):
        make(j, (me, me, me, n1, n1, n2, dg)[j], (n1, n2, sis, n2, sis, sis, sis)[j]).start()

    def wait_send(make, j):
        make(j, (me, me, me, n1, n1, n2, dg)[j], (n1, n2, sis, n2, sis, sis, sis)[j]).wait_send()

    def arrived(make, j):
        make(j, (n1, n2, sis, dg, n2 + ds, n1 + ds, dg + ds)[j], me).wait_recv()

    def own(make):
        for j in (0, 1, 2):
            send(make, j)

    def forward(make):
        arrived(make, 0)
        send(make, 3)
        send(make, 4)
        arrived(make, 1)
        send(make, 5)

    def forward_diag(make):
        arrived(make, 3)
        send(make, 6)

    def complete(make):
        for j in (2, 4, 5, 6):
            arrived(make, j)

    def a1(v):
        return lambda j, block, to: a1_copy(v, j, block, to)

    def a2(u, h):
        return lambda j, block, to: a2_copy(u, h, j, block, to)

    def a1_step(v):
        with jax.named_scope("a1_step"):
            @pl.when(v < NV)
            def _():
                forward(a1(v))

            @pl.when(v + 2 < NV)
            def _():
                own(a1(v + 2))

            @pl.when(jnp.logical_and(v >= 1, v < NV + 1))
            def _():
                forward_diag(a1(v - 1))

    def rs_copy(p, c, j):
        src, dst, to = ((s1, r1, sis), (s2, r2, n1), (s3, r3, n2))[j]
        return pltpu.make_async_remote_copy(src_ref=src.at[c], dst_ref=dst.at[c], send_sem=rs_send.at[p, c, j], recv_sem=rs_recv.at[p, c, j],
                                            device_id={"tp": to}, device_id_type=MESH)

    def rs_stage1(p, c):
        slot = lax.rem(c, 2)
        for q in range(4):
            s1[c, q] = part[slot, 2 * q + 1 - core].astype(BF16)
        rs_copy(p, c, 0).start()

    def rs_stage2(p, c):
        slot = lax.rem(c, 2)
        with jax.named_scope("rs_wait1"):
            rs_copy(p, c, 0).wait_recv()

        def total(q):
            return part[slot, 2 * q + core] + r1[c, q].astype(F32)

        s2[c, 0] = total(c_n1).astype(BF16)
        s2[c, 1] = total(c_dg).astype(BF16)
        keep[c, 0] = total(c_me)
        keep[c, 1] = total(c_n2)
        rs_copy(p, c, 1).start()

    def rs_stage3(p, c):
        with jax.named_scope("rs_wait2"):
            rs_copy(p, c, 1).wait_recv()
        s3[c] = (keep[c, 1] + r2[c, 1].astype(F32)).astype(BF16)
        keep[c, 0] = keep[c, 0] + r2[c, 0].astype(F32)
        rs_copy(p, c, 2).start()

    def rs_stage4(p, c):
        with jax.named_scope("rs_wait3"):
            rs_copy(p, c, 2).wait_recv()
        return keep[c, 0] + r3[c].astype(F32)

    def rs_drain(p):
        def body(c, _):
            for j in range(3):
                rs_copy(p, c, j).wait_send()
            return 0
        lax.fori_loop(0, NCH, body, 0)

    def row_stats(xf):
        mean = jnp.mean(xf, axis=-1, keepdims=True)
        cen = xf - mean
        var = jnp.mean(cen * cen, axis=-1, keepdims=True)
        return mean, lax.rsqrt(var + LN_EPS)

    x_copy = pltpu.make_async_copy(x_hbm, xv, x_sem)
    x_copy.start()
    barrier = pltpu.get_barrier_semaphore()
    for other in (sis, n1, n2):
        pl.semaphore_signal(barrier, inc=1, device_id={"tp": other}, device_id_type=MESH)
    for dst, src in ((bo_row, bo_ref), (bd_row, bd_ref), (bu_row, bu_ref)):
        wide = src[...].astype(F32)
        for r in range(src.shape[0]):
            dst[:, r * HD:(r + 1) * HD] = wide[r:r + 1, :]
    with jax.named_scope("entry_x"):
        x_copy.wait()
    start_tiles(0, NS)

    with jax.named_scope("ln1"):
        for b in range(B):
            mean, rstd = row_stats(xv[b].astype(F32))
            for k in range(2):
                cols = slice(k * HALF, (k + 1) * HALF)
                h = (xv[b, :, cols].astype(F32) - mean) * rstd * g1_ref[:, cols] + c1_ref[:, cols]
                hg1[2 * b + k, me] = h.astype(BF16)
    with jax.named_scope("entry_barrier"):
        pl.semaphore_wait(barrier, 3)
    own(a1(0))
    own(a1(1))

    causal = lax.broadcasted_iota(jnp.int32, (SEQ, SEQ), 0) >= lax.broadcasted_iota(jnp.int32, (SEQ, SEQ), 1)

    def project(s, t):
        i0 = s * T_SEQ + t * NU
        with jax.named_scope("wait_w"):
            ws = [wait_tile(i0 + j) for j in range(NU)]
        with jax.named_scope("qkv"):
            lhs = [rows2d(hg1[2 * s + j // 3, :, :, (j % 3) * KC:(j % 3 + 1) * KC]) for j in range(NU)]
            for p in range(3):
                v = sum(dot(lhs[j], ws[j][:, p * NP:(p + 1) * NP]) for j in range(NU))
                for k in range(2):
                    h = 2 * p + k
                    bias = bq_ref[t].astype(F32)[h:h + 1, :]
                    qkv[:, t * NQ + h * HD:t * NQ + (h + 1) * HD] = (v[:, k * HD:(k + 1) * HD] + bias).astype(BF16)
        start_tiles(i0 + NS, NU)

    def attend():
        with jax.named_scope("attn"):
            def head(t, h):
                return qkv[:, t * NQ + h * HD:t * NQ + (h + 1) * HD]

            logits = [lax.dot_general(head(0, h), head(1, h), (((1,), (1,)), ((), ())), preferred_element_type=F32) for h in range(HEADS)]
            weights = []
            for x in logits:
                x = jnp.where(causal, x * HD ** -0.5, -1e30)
                e = jnp.exp(x - jnp.max(x, axis=-1, keepdims=True))
                weights.append((e * (1.0 / jnp.sum(e, axis=-1, keepdims=True))).astype(BF16))
            for h in range(HEADS):
                ctx[:, h * HD:(h + 1) * HD] = dot(weights[h], head(2, h)).astype(BF16)

    def out_product(s, n):
        i0 = s * T_SEQ + 18 + 2 * n
        ws = [wait_tile(i0 + j, NQ) for j in range(2)]
        with jax.named_scope("out"):
            for p in range(6):
                d = dot(ctx[...], ws[p // 3][0:NQ, (p % 3) * NP:(p % 3 + 1) * NP])
                g, half = p // 2, p % 2
                part[n % 2, :, g * S_LOC:(g + 1) * S_LOC, half * NP:(half + 1) * NP] = d.reshape(N_DEV, S_LOC, NP)
        start_tiles(i0 + NS, 2)
        rs_stage1(0, 4 * s + n)

    def out_finish(s, n):
        total = rs_stage4(0, 4 * s + n)
        r = pl.ds(pl.multiple_of(s * S_LOC, S_LOC), S_LOC)
        for g in range(3):
            cols = slice((3 * n + g) * CW, (3 * n + g + 1) * CW)
            x1[r, cols] = (xv[s, :, cols].astype(F32) + (total[g * S_LOC:(g + 1) * S_LOC] + bo_row[:, cols])).astype(BF16)

    def norm2(s):
        with jax.named_scope("ln2"):
            r = pl.ds(pl.multiple_of(s * S_LOC, S_LOC), S_LOC)
            mean, rstd = row_stats(x1[r, :].astype(F32))
            for u in range(NU):
                cols = slice(u * KC, (u + 1) * KC)
                h = (x1[r, cols].astype(F32) - mean) * rstd * g2_ref[:, cols] + c2_ref[:, cols]
                hg2[u, me, r, :] = h.astype(BF16)

    a1_step(0)
    a1_step(1)

    def seq_body(s, _):
        now = s < B
        before = s >= 1

        @pl.when(now)
        def _():
            with jax.named_scope("a1_complete"):
                complete(a1(2 * s))
            a1_step(2 * s + 2)
            with jax.named_scope("a1_complete"):
                complete(a1(2 * s + 1))
            project(s, 0)
            a1_step(2 * s + 3)
            project(s, 1)

        @pl.when(before)
        def _():
            rs_stage3(0, 4 * s - 4)

        @pl.when(now)
        def _():
            project(s, 2)

        @pl.when(before)
        def _():
            rs_stage3(0, 4 * s - 3)

        @pl.when(now)
        def _():
            attend()

        @pl.when(before)
        def _():
            rs_stage3(0, 4 * s - 2)
            out_finish(s - 1, 0)

        @pl.when(now)
        def _():
            out_product(s, 0)

        @pl.when(before)
        def _():
            rs_stage3(0, 4 * s - 1)
            out_finish(s - 1, 1)

        @pl.when(now)
        def _():
            out_product(s, 1)
            rs_stage2(0, 4 * s)

        @pl.when(before)
        def _():
            out_finish(s - 1, 2)

        @pl.when(now)
        def _():
            out_product(s, 2)
            rs_stage2(0, 4 * s + 1)

        @pl.when(before)
        def _():
            out_finish(s - 1, 3)

        @pl.when(now)
        def _():
            out_product(s, 3)
            rs_stage2(0, 4 * s + 2)

        @pl.when(before)
        def _():
            norm2(s - 1)

        @pl.when(now)
        def _():
            rs_stage2(0, 4 * s + 3)

        @pl.when(s == B - 1)
        def _():
            own(a2(0, 0))
            own(a2(1, 0))
        return 0
    lax.fori_loop(0, B + 1, seq_body, 0)

    own(a2(0, 1))
    own(a2(1, 1))

    def a1_drain(v, _):
        for j in range(7):
            wait_send(a1(v), j)
        return 0
    lax.fori_loop(0, NV, a1_drain, 0)
    rs_drain(0)

    acc[...] = jnp.zeros((M, FF), F32)

    def up_chunk(u):
        i0 = T_OUT + u * 4
        with jax.named_scope("wait_w"):
            ws = [wait_tile(i0 + n) for n in range(4)]
        with jax.named_scope("up"):
            lhs = rows2d(hg2[u])
            for n in range(4):
                for p in range(3):
                    c = n * NC + p * NP
                    acc[:, c:c + NP] += dot(lhs, ws[n][:, p * NP:(p + 1) * NP])
        start_tiles(i0 + NS, 4)

    def up_body(u, _):
        with jax.named_scope("a2_step"):
            @pl.when(u < NU)
            def _():
                for h in range(2):
                    forward(a2(u, h))

            @pl.when(u + 2 < NU)
            def _():
                for h in range(2):
                    own(a2(u + 2, h))

            @pl.when(jnp.logical_and(u >= 1, u < NU + 1))
            def _():
                for h in range(2):
                    forward_diag(a2(u - 1, h))

        @pl.when(u >= 2)
        def _():
            with jax.named_scope("a2_complete"):
                for h in range(2):
                    complete(a2(u - 2, h))
            up_chunk(u - 2)
        return 0
    lax.fori_loop(0, NU + 2, up_body, 0)

    def a2_drain(u, _):
        for h in range(2):
            for j in range(7):
                wait_send(a2(u, h), j)
        return 0
    lax.fori_loop(0, NU, a2_drain, 0)

    def gelu_body(d, _):
        r = pl.ds(pl.multiple_of(d * ROWS, ROWS), ROWS)
        ub[r, :] = jax.nn.gelu(acc[r, :] + bu_row[...], approximate=True).astype(BF16)
        return 0
    with jax.named_scope("gelu"):
        lax.fori_loop(0, N_DEV, gelu_body, 0)

    def down_product(n):
        i0 = T_UP + 2 * n
        ws = [wait_tile(i0 + j) for j in range(2)]
        slot = lax.rem(n, 2)
        with jax.named_scope("down"):
            for half in range(2):
                d = sum(dot(ub[:, k * KC:(k + 1) * KC], ws[(2 * k + half) // 3][:, ((2 * k + half) % 3) * NP:((2 * k + half) % 3 + 1) * NP]) for k in range(3))
                part[slot, :, :, half * NP:(half + 1) * NP] = d.reshape(N_DEV, ROWS, NP)
        start_tiles(i0 + NS, 2)
        rs_stage1(1, n)

    def down_body(n, _):
        @pl.when(n < NCH)
        def _():
            down_product(n)

        @pl.when(jnp.logical_and(n >= 1, n < NCH + 1))
        def _():
            rs_stage2(1, n - 1)

        @pl.when(jnp.logical_and(n >= 3, n < NCH + 3))
        def _():
            rs_stage3(1, n - 3)

        @pl.when(n >= 5)
        def _():
            total = rs_stage4(1, n - 5)
            cols = pl.ds(pl.multiple_of((n - 5) * CW, CW), CW)
            res = x1[:, cols].astype(F32) + (total + bd_row[:, cols])
            out_ref[:, :, cols] = res.astype(BF16).reshape(B, S_LOC, CW)
        return 0
    lax.fori_loop(0, NCH + 5, down_body, 0)
    rs_drain(1)


def solution(mesh):
    def device_body(hidden, ln1_gain, ln1_bias, w_qkv, b_qkv, w_out, b_out, ln2_gain, ln2_bias, w_up, b_up, w_down, b_down):
        any_spec = pl.BlockSpec(memory_space=pl.ANY)
        vmem = pl.BlockSpec(memory_space=pltpu.VMEM)

        def row(v):
            return v.reshape(1, -1)

        def tile(v):
            return v.reshape(-1, HD)

        two = pltpu.VMEM((NCH, 2, ROWS, CW), BF16)
        four = pltpu.VMEM((NCH, 4, ROWS, CW), BF16)
        one = pltpu.VMEM((NCH, ROWS, CW), BF16)
        dma = pltpu.SemaphoreType.DMA
        return pl.pallas_call(
            kernel,
            out_shape=jax.ShapeDtypeStruct((B, S_LOC, D), BF16),
            in_specs=[any_spec] * 5 + [vmem] * 8,
            out_specs=vmem,
            scratch_shapes=[
                pltpu.VMEM((B, S_LOC, D), BF16),
                pltpu.VMEM((NV, N_DEV, S_LOC, HALF), BF16),
                pltpu.VMEM((NU, N_DEV, ROWS, KC), BF16),
                pltpu.VMEM((M, FF), F32),
                pltpu.VMEM((SEQ, 3 * NQ), BF16),
                pltpu.VMEM((SEQ, NQ), BF16),
                pltpu.VMEM((M, FF), BF16),
                pltpu.VMEM((2, N_DEV, ROWS, CW), F32),
                four, four, two, two, one, one,
                pltpu.VMEM((NCH, 2, ROWS, CW), F32),
                pltpu.VMEM((ROWS, D), BF16),
                pltpu.VMEM((NS, KC, NC), BF16),
                pltpu.VMEM((1, D), F32),
                pltpu.VMEM((1, D), F32),
                pltpu.VMEM((1, FF), F32),
                dma, dma((NS,)),
                dma((NV, 7)), dma((NV, 7)),
                dma((NU, 2, 7)), dma((NU, 2, 7)),
                dma((2, NCH, 3)), dma((2, NCH, 3)),
            ],
            compiler_params=pltpu.CompilerParams(collective_id=0, has_side_effects=True, vmem_limit_bytes=67_043_328),
            name="decoder_layer",
        )(hidden, jnp.transpose(w_qkv, (1, 2, 0, 3)), w_out.reshape(HEADS * HD, D), w_up, w_down,
          row(ln1_gain), row(ln1_bias), b_qkv, tile(b_out), row(ln2_gain), row(ln2_bias), tile(b_up), tile(b_down))

    in_layout = (P("dp", "tp", None), P(), P(), P(None, None, "tp", None), P(None, "tp", None), P("tp", None, None), P(), P(), P(), P(None, "tp"), P("tp"), P("tp", None), P())
    return jax.shard_map(device_body, mesh=mesh, in_specs=in_layout, out_specs=P("dp", "tp", None), check_vma=False)
```

```python
import jax
import jax.numpy as jnp
from jax import lax
from jax.experimental import pallas as pl
from jax.experimental.pallas import tpu as pltpu
from jax.sharding import PartitionSpec as P

MESH = pl.DeviceIdType.MESH
F32 = jnp.float32
BF16 = jnp.bfloat16
LN_EPS = 1e-5

N_DEV = 8
B, S_LOC = 3, 16
ROWS = B * S_LOC
SEQ = N_DEV * S_LOC
M = N_DEV * ROWS
D = 6144
HEADS, HD = 6, 128
NQ = HEADS * HD
FF = 3072
KC = 1024
NC = 768
NP = NC // 3
NU = D // KC
VK = 4
VW = D // VK
NV = VK * B
AHEAD = 3
NCH = 12
CW = 512
NS = 18
RING = 16


def rows2d(v):
    return v.reshape(-1, v.shape[-1])


def dot(a, b):
    return jnp.dot(a, b, preferred_element_type=F32)


def kernel(x_hbm, wq_hbm, wo_hbm, wu_hbm, wd_hbm, g1_ref, c1_ref, bq_ref, bo_ref, g2_ref, c2_ref, bu_ref, bd_ref, out_ref,
           xv, hg1, hg2, acc, qkv, ctx, ub, part, s1, r1, s2, r2, s3, r3, keep, ring, wo, bo_row, bd_row, bu_row,
           x_sem, w_sem, wo_sem, a1_send, a1_recv, a2_send, a2_recv, rs_send, rs_recv):
    me = lax.axis_index("tp")
    core = lax.rem(me, 2)
    xbit = lax.rem(me // 2, 2)
    ybit = me // 4
    dx = 2 - 4 * xbit
    dy = 4 - 8 * ybit
    ds = 1 - 2 * core
    sis = me + ds
    n1 = me + (1 - core) * dx + core * dy
    n2 = me + (1 - core) * dy + core * dx
    dg = me + dx + dy
    c_me, c_n1, c_n2, c_dg = me // 2, n1 // 2, n2 // 2, dg // 2

    def start_qkv(t):
        for j in range(NU):
            i = t * NU + j
            for h in range(HEADS):
                pltpu.make_async_copy(wq_hbm.at[t, h, j * KC:(j + 1) * KC, :], ring.at[i, :, h * HD:(h + 1) * HD], w_sem.at[i]).start()

    def up_copy(k, n):
        slot = lax.rem(4 * k, RING) + n
        k0 = pl.multiple_of(k * KC, KC)
        return pltpu.make_async_copy(wu_hbm.at[pl.ds(k0, KC), n * NC:(n + 1) * NC], ring.at[slot], w_sem.at[slot])

    def down_copy(n, k):
        slot = lax.rem(8 + 3 * n + k, RING)
        n0 = pl.multiple_of(n * CW, CW)
        return pltpu.make_async_copy(wd_hbm.at[k * KC:(k + 1) * KC, pl.ds(n0, CW)], ring.at[slot, :, 0:CW], w_sem.at[slot])

    def start_down(first):
        for j in range(first, first + 4):
            down_copy(j // 3, j % 3).start()

    def out_copy(n):
        return pltpu.make_async_copy(wo_hbm.at[:, n * 3 * CW:(n + 1) * 3 * CW], wo.at[n % 2], wo_sem.at[n % 2])

    def a1_copy(v, j, block, to):
        ref = hg1.at[v, block]
        return pltpu.make_async_remote_copy(src_ref=ref, dst_ref=ref, send_sem=a1_send.at[v, j], recv_sem=a1_recv.at[v, j],
                                            device_id={"tp": to}, device_id_type=MESH)

    def a2_copy(u, h, j, block, to):
        ref = hg2.at[u, block, pl.ds(32 * h, 32 - 16 * h), :]
        return pltpu.make_async_remote_copy(src_ref=ref, dst_ref=ref, send_sem=a2_send.at[u, h, j], recv_sem=a2_recv.at[u, h, j],
                                            device_id={"tp": to}, device_id_type=MESH)

    def send(make, j):
        make(j, (me, me, me, n1, n1, n2, dg)[j], (n1, n2, sis, n2, sis, sis, sis)[j]).start()

    def wait_send(make, j):
        make(j, (me, me, me, n1, n1, n2, dg)[j], (n1, n2, sis, n2, sis, sis, sis)[j]).wait_send()

    def arrived(make, j):
        make(j, (n1, n2, sis, dg, n2 + ds, n1 + ds, dg + ds)[j], me).wait_recv()

    def own(make):
        for j in (0, 1, 2):
            send(make, j)

    def forward(make):
        arrived(make, 0)
        send(make, 3)
        send(make, 4)
        arrived(make, 1)
        send(make, 5)

    def forward_diag(make):
        arrived(make, 3)
        send(make, 6)

    def complete(make):
        for j in (2, 4, 5, 6):
            arrived(make, j)

    def a1(v):
        return lambda j, block, to: a1_copy(v, j, block, to)

    def a2(u, h):
        return lambda j, block, to: a2_copy(u, h, j, block, to)

    def a1_step(v):
        if isinstance(v, int):
            if v < NV:
                forward(a1(v))
            if v + AHEAD < NV:
                own(a1(v + AHEAD))
            if 1 <= v < NV + 1:
                forward_diag(a1(v - 1))
            return
        with jax.named_scope("a1_step"):
            @pl.when(v < NV)
            def _():
                forward(a1(v))

            @pl.when(v + AHEAD < NV)
            def _():
                own(a1(v + AHEAD))

            @pl.when(v < NV + 1)
            def _():
                forward_diag(a1(v - 1))

    def rs_copy(p, c, j):
        src, dst, to = ((s1, r1, sis), (s2, r2, n1), (s3, r3, n2))[j]
        return pltpu.make_async_remote_copy(src_ref=src.at[c], dst_ref=dst.at[c], send_sem=rs_send.at[p, c, j], recv_sem=rs_recv.at[p, c, j],
                                            device_id={"tp": to}, device_id_type=MESH)

    def rs_stage1(p, c):
        slot = lax.rem(c, 3)
        for q in range(4):
            s1[c, q] = part[slot, 2 * q + 1 - core].astype(BF16)
        rs_copy(p, c, 0).start()

    def rs_stage2(p, c):
        slot = lax.rem(c, 3)
        with jax.named_scope("rs_wait1"):
            rs_copy(p, c, 0).wait_recv()

        def total(q):
            return part[slot, 2 * q + core] + r1[c, q].astype(F32)

        s2[c, 0] = total(c_n1).astype(BF16)
        s2[c, 1] = total(c_dg).astype(BF16)
        keep[c, 0] = total(c_me)
        keep[c, 1] = total(c_n2)
        rs_copy(p, c, 1).start()

    def rs_stage3(p, c):
        with jax.named_scope("rs_wait2"):
            rs_copy(p, c, 1).wait_recv()
        s3[c] = (keep[c, 1] + r2[c, 1].astype(F32)).astype(BF16)
        keep[c, 0] = keep[c, 0] + r2[c, 0].astype(F32)
        rs_copy(p, c, 2).start()

    def rs_stage4(p, c):
        with jax.named_scope("rs_wait3"):
            rs_copy(p, c, 2).wait_recv()
        return keep[c, 0] + r3[c].astype(F32)

    def rs_drain(p):
        def body(c, _):
            for j in range(3):
                rs_copy(p, c, j).wait_send()
            return 0
        lax.fori_loop(0, NCH, body, 0)

    def row_stats(xf):
        mean = jnp.mean(xf, axis=-1, keepdims=True)
        cen = xf - mean
        var = jnp.mean(cen * cen, axis=-1, keepdims=True)
        return mean, lax.rsqrt(var + LN_EPS)

    x_copy = pltpu.make_async_copy(x_hbm, xv, x_sem)
    x_copy.start()
    barrier = pltpu.get_barrier_semaphore()
    for other in (sis, n1, n2):
        pl.semaphore_signal(barrier, inc=1, device_id={"tp": other}, device_id_type=MESH)
    for dst, src in ((bo_row, bo_ref), (bd_row, bd_ref), (bu_row, bu_ref)):
        wide = src[...].astype(F32)
        for r in range(src.shape[0]):
            dst[:, r * HD:(r + 1) * HD] = wide[r:r + 1, :]
    with jax.named_scope("entry_x"):
        x_copy.wait()
    start_qkv(0)

    with jax.named_scope("ln1"):
        for b in range(B):
            mean, rstd = row_stats(xv[b].astype(F32))
            for k in range(VK):
                cols = slice(k * VW, (k + 1) * VW)
                h = (xv[b, :, cols].astype(F32) - mean) * rstd * g1_ref[:, cols] + c1_ref[:, cols]
                hg1[VK * b + k, me] = h.astype(BF16)
    with jax.named_scope("entry_barrier"):
        pl.semaphore_wait(barrier, 3)
    for v in range(AHEAD):
        own(a1(v))

    causal = lax.broadcasted_iota(jnp.int32, (SEQ, SEQ), 0) >= lax.broadcasted_iota(jnp.int32, (SEQ, SEQ), 1)

    def project(s, t):
        @pl.when(s == 0)
        def _():
            for j in range(NU):
                i = t * NU + j
                pltpu.make_async_copy(wu_hbm.at[0:KC, 0:NC], ring.at[i], w_sem.at[i]).wait()

        with jax.named_scope("qkv"):
            lhs = []
            for f in range(D // 512):
                lhs.append((rows2d(hg1[VK * s + f // 3, :, :, (f % 3) * 512:(f % 3 + 1) * 512]), t * NU + f // 2, (f % 2) * 512))
            bias = bq_ref[t].astype(F32)
            for p in range(3):
                v = sum(dot(a, ring[i, r0:r0 + 512, p * NP:(p + 1) * NP]) for a, i, r0 in lhs)
                for k in range(2):
                    h = 2 * p + k
                    cols = pl.ds(pl.multiple_of(t * NQ + h * HD, HD), HD)
                    qkv[:, cols] = (v[:, k * HD:(k + 1) * HD] + bias[h:h + 1, :]).astype(BF16)

        @pl.when(s == B - 1)
        def _():
            for tt, lo, hi in ((0, 0, 4), (1, 4, 12), (2, 12, 16)):
                @pl.when(t == tt)
                def _():
                    for i in range(lo, hi):
                        up_copy(i // 4, i % 4).start()

    def attend():
        with jax.named_scope("attn"):
            def head(t, h):
                return qkv[:, t * NQ + h * HD:t * NQ + (h + 1) * HD]

            logits = [lax.dot_general(head(0, h), head(1, h), (((1,), (1,)), ((), ())), preferred_element_type=F32) for h in range(HEADS)]
            weights = []
            for x in logits:
                x = jnp.where(causal, x * HD ** -0.5, -1e30)
                e = jnp.exp(x - jnp.max(x, axis=-1, keepdims=True))
                weights.append((e * (1.0 / jnp.sum(e, axis=-1, keepdims=True))).astype(BF16))
            for h in range(HEADS):
                ctx[:, h * HD:(h + 1) * HD] = dot(weights[h], head(2, h)).astype(BF16)

    def out_product(s, n):
        out_copy(n).wait()
        c = 4 * s + n
        slot = lax.rem(c, 3)
        with jax.named_scope("out"):
            for p in range(6):
                d = dot(ctx[...], wo[n % 2, :, p * NP:(p + 1) * NP])
                g, half = p // 2, p % 2
                part[slot, :, g * S_LOC:(g + 1) * S_LOC, half * NP:(half + 1) * NP] = d.reshape(N_DEV, S_LOC, NP)
            rs_stage1(0, c)
        if n < 2:
            out_copy(n + 2).start()
        else:
            @pl.when(s < B - 1)
            def _():
                out_copy(n - 2).start()

    def out_finish(s, n):
        total = rs_stage4(0, 4 * s + n)
        for g in range(3):
            cols = slice((3 * n + g) * CW, (3 * n + g + 1) * CW)
            out_ref[s, :, cols] = (xv[s, :, cols].astype(F32) + (total[g * S_LOC:(g + 1) * S_LOC] + bo_row[:, cols])).astype(BF16)

    def norm2(s):
        with jax.named_scope("ln2"):
            r = pl.ds(pl.multiple_of(s * S_LOC, S_LOC), S_LOC)
            mean, rstd = row_stats(out_ref[s].astype(F32))
            for u in range(NU):
                cols = slice(u * KC, (u + 1) * KC)
                h = (out_ref[s, :, cols].astype(F32) - mean) * rstd * g2_ref[:, cols] + c2_ref[:, cols]
                hg2[u, me, r, :] = h.astype(BF16)

    a1_step(0)
    start_qkv(1)
    a1_step(1)
    start_qkv(2)
    a1_step(2)
    out_copy(0).start()
    out_copy(1).start()
    a1_step(3)
    a1_step(4)

    def seq_body(s, _):
        b0 = 4 * s - 4

        def before(f):
            pl.when(s >= 1)(f)

        with jax.named_scope("a1_complete"):
            for k in range(VK):
                complete(a1(VK * s + k))

        def qkv_body(t, _):
            project(s, t)

            @pl.when(jnp.logical_and(s >= 1, t == 0))
            def _():
                rs_stage2(0, b0 + 3)

            @pl.when(jnp.logical_and(s >= 1, t >= 1))
            def _():
                rs_stage3(0, b0 + t - 1)
            a1_step(VK * s + 5 + t)
            return 0
        lax.fori_loop(0, 3, qkv_body, 0)
        attend()
        before(lambda: rs_stage3(0, b0 + 2))
        a1_step(VK * s + 8)
        out_product(s, 0)
        before(lambda: out_finish(s - 1, 0))
        out_product(s, 1)

        @before
        def _():
            rs_stage3(0, b0 + 3)
            out_finish(s - 1, 1)

        out_product(s, 2)
        rs_stage2(0, 4 * s)
        before(lambda: out_finish(s - 1, 2))
        out_product(s, 3)
        rs_stage2(0, 4 * s + 1)

        @before
        def _():
            out_finish(s - 1, 3)
            norm2(s - 1)

        rs_stage2(0, 4 * s + 2)
        return 0
    lax.fori_loop(0, B, seq_body, 0)

    c0, last = NCH - 4, B - 1
    rs_stage2(0, c0 + 3)
    own(a2(0, 0))
    own(a2(1, 0))
    rs_stage3(0, c0)
    rs_stage3(0, c0 + 1)
    out_finish(last, 0)
    rs_stage3(0, c0 + 2)
    out_finish(last, 1)
    rs_stage3(0, c0 + 3)
    forward(a2(0, 0))
    out_finish(last, 2)
    forward(a2(1, 0))
    forward_diag(a2(0, 0))
    out_finish(last, 3)
    norm2(last)
    own(a2(0, 1))
    own(a2(1, 1))
    forward_diag(a2(1, 0))

    def a1_drain(v, _):
        for j in range(7):
            wait_send(a1(v), j)
        return 0
    lax.fori_loop(0, NV, a1_drain, 0)
    rs_drain(0)

    def up_chunk(u, first=False, final=False):
        for n in range(4):
            up_copy(u, n).wait()
        if not first and not final:
            @pl.when(u <= 2)
            def _():
                for n in range(4):
                    up_copy(u + 3, n).start()
            pl.when(u == 3)(lambda: start_down(0))
            pl.when(u == 4)(lambda: start_down(4))
        with jax.named_scope("up"):
            if final:
                start_down(8)
            lhs = rows2d(hg2[u])
            slot = lax.rem(4 * u, RING)
            for n in range(4):
                for p in range(3):
                    c = slice(n * NC + p * NP, n * NC + (p + 1) * NP)
                    d = dot(lhs, ring[slot + n, :, p * NP:(p + 1) * NP])
                    if first:
                        acc[:, c] = d
                    elif final:
                        ub[:, c] = jax.nn.gelu(acc[:, c] + d + bu_row[:, c], approximate=True).astype(BF16)
                    else:
                        acc[:, c] += d

    def a2_done(u):
        with jax.named_scope("a2_complete"):
            for h in range(2):
                complete(a2(u, h))

    with jax.named_scope("a2_step"):
        forward(a2(0, 1))
        for h in range(2):
            own(a2(2, h))
        forward(a2(1, 1))
        for h in range(2):
            own(a2(3, h))
        forward_diag(a2(0, 1))
    a2_done(0)
    up_chunk(0, first=True)

    def up_body(u, _):
        with jax.named_scope("a2_step"):
            for h in range(2):
                forward(a2(u + 1, h))

            @pl.when(u + 3 < NU)
            def _():
                for h in range(2):
                    own(a2(u + 3, h))

            @pl.when(u > 1)
            def _():
                forward_diag(a2(u, 0))
            forward_diag(a2(u, 1))
        a2_done(u)
        up_chunk(u)
        return 0
    lax.fori_loop(1, NU - 1, up_body, 0)

    for h in range(2):
        forward_diag(a2(NU - 1, h))
    a2_done(NU - 1)
    up_chunk(NU - 1, final=True)
    start_down(12)

    def a2_drain(u, _):
        for h in range(2):
            for j in range(7):
                wait_send(a2(u, h), j)
        return 0
    lax.fori_loop(0, NU, a2_drain, 0)

    def down_product(n):
        for k in range(3):
            down_copy(n, k).wait()
        slot = lax.rem(n, 3)
        with jax.named_scope("down"):
            for half in range(2):
                d = sum(dot(ub[:, k * KC:(k + 1) * KC], ring[lax.rem(8 + 3 * n + k, RING), :, half * NP:(half + 1) * NP]) for k in range(3))
                part[slot, :, :, half * NP:(half + 1) * NP] = d.reshape(N_DEV, ROWS, NP)
            rs_stage1(1, n)

        @pl.when(n + 5 < NCH)
        def _():
            down_copy(n + 5, 1).start()
            down_copy(n + 5, 2).start()

        @pl.when(n + 6 < NCH)
        def _():
            down_copy(n + 6, 0).start()

    def down_body(n, _):
        @pl.when(n < NCH)
        def _():
            down_product(n)

        @pl.when(jnp.logical_and(n >= 1, n < NCH + 1))
        def _():
            rs_stage2(1, n - 1)

        @pl.when(jnp.logical_and(n >= 3, n < NCH + 3))
        def _():
            rs_stage3(1, n - 3)

        @pl.when(n >= 5)
        def _():
            total = rs_stage4(1, n - 5)
            cols = pl.ds(pl.multiple_of((n - 5) * CW, CW), CW)
            res = rows2d(out_ref[:, :, cols]).astype(F32) + (total + bd_row[:, cols])
            out_ref[:, :, cols] = res.astype(BF16).reshape(B, S_LOC, CW)
        return 0
    lax.fori_loop(0, NCH + 5, down_body, 0)
    rs_drain(1)


def solution(mesh):
    def device_body(hidden, ln1_gain, ln1_bias, w_qkv, b_qkv, w_out, b_out, ln2_gain, ln2_bias, w_up, b_up, w_down, b_down):
        any_spec = pl.BlockSpec(memory_space=pl.ANY)
        vmem = pl.BlockSpec(memory_space=pltpu.VMEM)

        def row(v):
            return v.reshape(1, -1)

        def tile(v):
            return v.reshape(-1, HD)

        two = pltpu.VMEM((NCH, 2, ROWS, CW), BF16)
        four = pltpu.VMEM((NCH, 4, ROWS, CW), BF16)
        one = pltpu.VMEM((NCH, ROWS, CW), BF16)
        dma = pltpu.SemaphoreType.DMA
        return pl.pallas_call(
            kernel,
            out_shape=jax.ShapeDtypeStruct((B, S_LOC, D), BF16),
            in_specs=[any_spec] * 5 + [vmem] * 8,
            out_specs=vmem,
            scratch_shapes=[
                pltpu.VMEM((B, S_LOC, D), BF16),
                pltpu.VMEM((NV, N_DEV, S_LOC, VW), BF16),
                pltpu.VMEM((NU, N_DEV, ROWS, KC), BF16),
                pltpu.VMEM((M, FF), F32),
                pltpu.VMEM((SEQ, 3 * NQ), BF16),
                pltpu.VMEM((SEQ, NQ), BF16),
                pltpu.VMEM((M, FF), BF16),
                pltpu.VMEM((3, N_DEV, ROWS, CW), F32),
                four, four, two, two, one, one,
                pltpu.VMEM((NCH, 2, ROWS, CW), F32),
                pltpu.VMEM((NS, KC, NC), BF16),
                pltpu.VMEM((2, NQ, 3 * CW), BF16),
                pltpu.VMEM((1, D), F32),
                pltpu.VMEM((1, D), F32),
                pltpu.VMEM((1, FF), F32),
                dma, dma((NS,)), dma((2,)),
                dma((NV, 7)), dma((NV, 7)),
                dma((NU, 2, 7)), dma((NU, 2, 7)),
                dma((2, NCH, 3)), dma((2, NCH, 3)),
            ],
            compiler_params=pltpu.CompilerParams(collective_id=0, has_side_effects=True, vmem_limit_bytes=67_043_328),
            name="decoder_layer",
        )(hidden, jnp.transpose(w_qkv, (1, 2, 0, 3)), w_out.reshape(HEADS * HD, D), w_up, w_down,
          row(ln1_gain), row(ln1_bias), b_qkv, tile(b_out), row(ln2_gain), row(ln2_bias), tile(b_up), tile(b_down))

    in_layout = (P("dp", "tp", None), P(), P(), P(None, None, "tp", None), P(None, "tp", None), P("tp", None, None), P(), P(), P(), P(None, "tp"), P("tp"), P("tp", None), P())
    return jax.shard_map(device_body, mesh=mesh, in_specs=in_layout, out_specs=P("dp", "tp", None), check_vma=False)
```

```python
import jax
import jax.numpy as jnp
from jax import lax
from jax.experimental import pallas as pl
from jax.experimental.pallas import tpu as pltpu
from jax.sharding import PartitionSpec as P

MESH = pl.DeviceIdType.MESH
F32 = jnp.float32
BF16 = jnp.bfloat16
LN_EPS = 1e-5

N_DEV = 8
B, S_LOC = 3, 16
ROWS = B * S_LOC
SEQ = N_DEV * S_LOC
M = N_DEV * ROWS
D = 6144
HEADS, HD = 6, 128
NQ = HEADS * HD
FF = 3072
KC = 1024
NC = 768
NP = NC // 3
NU = D // KC
VK = 4
VW = D // VK
NV = VK * B
AHEAD = 4
NCH = 12
CW = 512
NS = 18
RING = 16


def rows2d(v):
    return v.reshape(-1, v.shape[-1])


def dot(a, b):
    return jnp.dot(a, b, preferred_element_type=F32)


def kernel(x_hbm, wq_hbm, wo_hbm, wu_hbm, wd_hbm, g1_ref, c1_ref, bq_ref, bo_ref, g2_ref, c2_ref, bu_ref, bd_ref, out_ref,
           xv, hg1, hg2, acc, qkv, ctx, ub, part, s1, r1, s2, r2, s3, r3, keep, ring, wo, bo_row, bd_row, bu_row,
           x_sem, w_sem, wo_sem, a1_send, a1_recv, a2_send, a2_recv, rs_send, rs_recv):
    me = lax.axis_index("tp")
    core = lax.rem(me, 2)
    xbit = lax.rem(me // 2, 2)
    ybit = me // 4
    dx = 2 - 4 * xbit
    dy = 4 - 8 * ybit
    ds = 1 - 2 * core
    sis = me + ds
    n1 = me + (1 - core) * dx + core * dy
    n2 = me + (1 - core) * dy + core * dx
    dg = me + dx + dy
    c_me, c_n1, c_n2, c_dg = me // 2, n1 // 2, n2 // 2, dg // 2

    def start_qkv(t):
        for j in range(NU):
            i = t * NU + j
            for h in range(HEADS):
                pltpu.make_async_copy(wq_hbm.at[t, h, j * KC:(j + 1) * KC, :], ring.at[i, :, h * HD:(h + 1) * HD], w_sem.at[i]).start()

    def up_copy(k, n):
        slot = lax.rem(4 * k, RING) + n
        k0 = pl.multiple_of(k * KC, KC)
        return pltpu.make_async_copy(wu_hbm.at[pl.ds(k0, KC), n * NC:(n + 1) * NC], ring.at[slot], w_sem.at[slot])

    def down_copy(n, k):
        slot = lax.rem(8 + 3 * n + k, RING)
        n0 = pl.multiple_of(n * CW, CW)
        return pltpu.make_async_copy(wd_hbm.at[k * KC:(k + 1) * KC, pl.ds(n0, CW)], ring.at[slot, :, 0:CW], w_sem.at[slot])

    def start_down(first):
        for j in range(first, first + 4):
            down_copy(j // 3, j % 3).start()

    def out_copies(n):
        cols = slice(n * 3 * CW, (n + 1) * 3 * CW)
        if n < 3:
            return [pltpu.make_async_copy(wo_hbm.at[:, cols], wo.at[n], wo_sem.at[n])]
        return [pltpu.make_async_copy(wo_hbm.at[k * M:(k + 1) * M, cols], ub.at[:, k * 3 * CW:(k + 1) * 3 * CW], wo_sem.at[n + k]) for k in range(2)]

    def a1_copy(v, j, block, to):
        ref = hg1.at[v, block]
        return pltpu.make_async_remote_copy(src_ref=ref, dst_ref=ref, send_sem=a1_send.at[v, j], recv_sem=a1_recv.at[v, j],
                                            device_id={"tp": to}, device_id_type=MESH)

    def a2_copy(u, h, j, block, to):
        ref = hg2.at[u, block, pl.ds(32 * h, 32 - 16 * h), :]
        return pltpu.make_async_remote_copy(src_ref=ref, dst_ref=ref, send_sem=a2_send.at[u, h, j], recv_sem=a2_recv.at[u, h, j],
                                            device_id={"tp": to}, device_id_type=MESH)

    def send(make, j):
        make(j, (me, me, me, n1, n1, n2, dg)[j], (n1, n2, sis, n2, sis, sis, sis)[j]).start()

    def wait_send(make, j):
        make(j, (me, me, me, n1, n1, n2, dg)[j], (n1, n2, sis, n2, sis, sis, sis)[j]).wait_send()

    def arrived(make, j):
        make(j, (n1, n2, sis, dg, n2 + ds, n1 + ds, dg + ds)[j], me).wait_recv()

    def own(make):
        for j in (0, 1, 2):
            send(make, j)

    def forward(make):
        arrived(make, 0)
        send(make, 3)
        send(make, 4)
        arrived(make, 1)
        send(make, 5)

    def forward_diag(make):
        arrived(make, 3)
        send(make, 6)

    def complete(make):
        for j in (2, 4, 5, 6):
            arrived(make, j)

    def a1(v):
        return lambda j, block, to: a1_copy(v, j, block, to)

    def a2(u, h):
        return lambda j, block, to: a2_copy(u, h, j, block, to)

    def a1_step(v):
        if isinstance(v, int):
            if v < NV:
                forward(a1(v))
            if v + AHEAD < NV:
                own(a1(v + AHEAD))
            if 1 <= v < NV + 1:
                forward_diag(a1(v - 1))
            return
        with jax.named_scope("a1_step"):
            @pl.when(v < NV)
            def _():
                forward(a1(v))

            @pl.when(v < NV + 1)
            def _():
                forward_diag(a1(v - 1))

    def rs_copy(p, c, j):
        src, dst, to = ((s1, r1, sis), (s2, r2, n1), (s3, r3, n2))[j]
        return pltpu.make_async_remote_copy(src_ref=src.at[lax.rem(c, 4) if j == 0 else c], dst_ref=dst.at[c], send_sem=rs_send.at[p, c, j], recv_sem=rs_recv.at[p, c, j],
                                            device_id={"tp": to}, device_id_type=MESH)

    def rs_stage1(p, c):
        slot = lax.rem(c, 3)

        @pl.when(c >= 4)
        def _():
            rs_copy(p, c - 4, 0).wait_send()

        for q in range(4):
            s1[lax.rem(c, 4), q] = part[slot, 2 * q + 1 - core].astype(BF16)
        rs_copy(p, c, 0).start()

    def rs_stage2(p, c):
        slot = lax.rem(c, 3)
        with jax.named_scope("rs_wait1"):
            rs_copy(p, c, 0).wait_recv()

        def total(q):
            return part[slot, 2 * q + core] + r1[c, q].astype(F32)

        s2[c, 0] = total(c_n1).astype(BF16)
        s2[c, 1] = total(c_dg).astype(BF16)
        keep[lax.rem(c, 8), 0] = total(c_me)
        keep[lax.rem(c, 8), 1] = total(c_n2)
        rs_copy(p, c, 1).start()

    def rs_stage3(p, c):
        with jax.named_scope("rs_wait2"):
            rs_copy(p, c, 1).wait_recv()
        s3[c] = (keep[lax.rem(c, 8), 1] + r2[c, 1].astype(F32)).astype(BF16)
        keep[lax.rem(c, 8), 0] = keep[lax.rem(c, 8), 0] + r2[c, 0].astype(F32)
        rs_copy(p, c, 2).start()

    def rs_stage4(p, c):
        with jax.named_scope("rs_wait3"):
            rs_copy(p, c, 2).wait_recv()
        return keep[lax.rem(c, 8), 0] + r3[c].astype(F32)

    def rs_drain(p):
        def body(c, _):
            for j in (1, 2):
                rs_copy(p, c, j).wait_send()
            return 0
        lax.fori_loop(0, NCH, body, 0)
        for c in range(NCH - 4, NCH):
            rs_copy(p, c, 0).wait_send()

    def row_stats(xf):
        mean = jnp.mean(xf, axis=-1, keepdims=True)
        cen = xf - mean
        var = jnp.mean(cen * cen, axis=-1, keepdims=True)
        return mean, lax.rsqrt(var + LN_EPS)

    x_copy = pltpu.make_async_copy(x_hbm, xv, x_sem)
    x_copy.start()
    barrier = pltpu.get_barrier_semaphore()
    for other in (sis, n1, n2):
        pl.semaphore_signal(barrier, inc=1, device_id={"tp": other}, device_id_type=MESH)
    for dst, src in ((bo_row, bo_ref), (bd_row, bd_ref), (bu_row, bu_ref)):
        wide = src[...].astype(F32)
        for r in range(src.shape[0]):
            dst[:, r * HD:(r + 1) * HD] = wide[r:r + 1, :]
    with jax.named_scope("entry_x"):
        x_copy.wait()
    start_qkv(0)

    with jax.named_scope("ln1"):
        for b in range(B):
            mean, rstd = row_stats(xv[b].astype(F32))
            for k in range(VK):
                cols = slice(k * VW, (k + 1) * VW)
                h = (xv[b, :, cols].astype(F32) - mean) * rstd * g1_ref[:, cols] + c1_ref[:, cols]
                hg1[VK * b + k, me] = h.astype(BF16)
    with jax.named_scope("entry_barrier"):
        pl.semaphore_wait(barrier, 3)
    for v in range(AHEAD):
        own(a1(v))

    causal = lax.broadcasted_iota(jnp.int32, (SEQ, SEQ), 0) >= lax.broadcasted_iota(jnp.int32, (SEQ, SEQ), 1)

    def project(s, t):
        @pl.when(s == 0)
        def _():
            for j in range(NU):
                i = t * NU + j
                pltpu.make_async_copy(wu_hbm.at[0:KC, 0:NC], ring.at[i], w_sem.at[i]).wait()

        with jax.named_scope("qkv"):
            lhs = []
            for f in range(D // 512):
                lhs.append((rows2d(hg1[VK * s + f // 3, :, :, (f % 3) * 512:(f % 3 + 1) * 512]), t * NU + f // 2, (f % 2) * 512))
            bias = bq_ref[t].astype(F32)
            for p in range(3):
                v = sum(dot(a, ring[i, r0:r0 + 512, p * NP:(p + 1) * NP]) for a, i, r0 in lhs)
                for k in range(2):
                    h = 2 * p + k
                    cols = pl.ds(pl.multiple_of(t * NQ + h * HD, HD), HD)
                    qkv[:, cols] = (v[:, k * HD:(k + 1) * HD] + bias[h:h + 1, :]).astype(BF16)

        @pl.when(s == B - 1)
        def _():
            for tt, lo, hi in ((0, 0, 4), (1, 4, 12), (2, 12, 16)):
                @pl.when(t == tt)
                def _():
                    for i in range(lo, hi):
                        up_copy(i // 4, i % 4).start()

    def attend():
        with jax.named_scope("attn"):
            def head(t, h):
                return qkv[:, t * NQ + h * HD:t * NQ + (h + 1) * HD]

            logits = [lax.dot_general(head(0, h), head(1, h), (((1,), (1,)), ((), ())), preferred_element_type=F32) for h in range(HEADS)]
            weights = []
            for x in logits:
                x = jnp.where(causal, x * HD ** -0.5, -1e30)
                e = jnp.exp(x - jnp.max(x, axis=-1, keepdims=True))
                weights.append((e * (1.0 / jnp.sum(e, axis=-1, keepdims=True))).astype(BF16))
            for h in range(HEADS):
                ctx[:, h * HD:(h + 1) * HD] = dot(weights[h], head(2, h)).astype(BF16)

    def out_product(s, n):
        @pl.when(s == 0)
        def _():
            for copy in out_copies(n):
                copy.wait()

        c = 4 * s + n
        slot = lax.rem(c, 3)
        with jax.named_scope("out"):
            for p in range(6):
                if n < 3:
                    d = dot(ctx[...], wo[n, :, p * NP:(p + 1) * NP])
                else:
                    d = sum(dot(ctx[:, k * M:(k + 1) * M], ub[:, k * 3 * CW + p * NP:k * 3 * CW + (p + 1) * NP]) for k in range(2))
                g, half = p // 2, p % 2
                part[slot, :, g * S_LOC:(g + 1) * S_LOC, half * NP:(half + 1) * NP] = d.reshape(N_DEV, S_LOC, NP)
        rs_stage1(0, c)

    def out_finish(s, n):
        total = rs_stage4(0, 4 * s + n)
        for g in range(3):
            cols = slice((3 * n + g) * CW, (3 * n + g + 1) * CW)
            out_ref[s, :, cols] = (xv[s, :, cols].astype(F32) + (total[g * S_LOC:(g + 1) * S_LOC] + bo_row[:, cols])).astype(BF16)

    def norm2(s):
        with jax.named_scope("ln2"):
            r = pl.ds(pl.multiple_of(s * S_LOC, S_LOC), S_LOC)
            mean, rstd = row_stats(out_ref[s].astype(F32))
            for u in range(NU):
                cols = slice(u * KC, (u + 1) * KC)
                h = (out_ref[s, :, cols].astype(F32) - mean) * rstd * g2_ref[:, cols] + c2_ref[:, cols]
                hg2[u, me, r, :] = h.astype(BF16)

    a1_step(0)
    start_qkv(1)
    a1_step(1)
    start_qkv(2)
    a1_step(2)
    a1_step(3)
    for n in range(4):
        for copy in out_copies(n):
            copy.start()
    a1_step(4)
    for v in range(5 + AHEAD, NV):
        own(a1(v))

    def seq_body(s, _):
        b0 = 4 * s - 4

        def before(f):
            pl.when(s >= 1)(f)

        with jax.named_scope("a1_complete"):
            for k in range(VK):
                complete(a1(VK * s + k))

        def qkv_body(t, _):
            project(s, t)

            @pl.when(jnp.logical_and(s >= 1, t == 0))
            def _():
                rs_stage2(0, b0 + 3)

            @pl.when(jnp.logical_and(s >= 1, t >= 1))
            def _():
                rs_stage3(0, b0 + t - 1)
            a1_step(VK * s + 5 + t)
            return 0
        lax.fori_loop(0, 3, qkv_body, 0)
        attend()
        before(lambda: rs_stage3(0, b0 + 2))
        a1_step(VK * s + 8)
        out_product(s, 0)
        before(lambda: out_finish(s - 1, 0))
        out_product(s, 1)

        @before
        def _():
            rs_stage3(0, b0 + 3)
            out_finish(s - 1, 1)

        out_product(s, 2)
        rs_stage2(0, 4 * s)
        before(lambda: out_finish(s - 1, 2))
        out_product(s, 3)
        rs_stage2(0, 4 * s + 1)

        @before
        def _():
            out_finish(s - 1, 3)
            norm2(s - 1)

        rs_stage2(0, 4 * s + 2)
        return 0
    lax.fori_loop(0, B, seq_body, 0)

    c0, last = NCH - 4, B - 1
    rs_stage2(0, c0 + 3)
    own(a2(0, 0))
    own(a2(1, 0))
    rs_stage3(0, c0)
    rs_stage3(0, c0 + 1)
    out_finish(last, 0)
    rs_stage3(0, c0 + 2)
    out_finish(last, 1)
    rs_stage3(0, c0 + 3)
    forward(a2(0, 0))
    out_finish(last, 2)
    forward(a2(1, 0))
    forward_diag(a2(0, 0))
    out_finish(last, 3)
    norm2(last)
    own(a2(0, 1))
    own(a2(1, 1))
    forward_diag(a2(1, 0))

    def a1_drain(v, _):
        for j in range(7):
            wait_send(a1(v), j)
        return 0
    lax.fori_loop(0, NV, a1_drain, 0)
    rs_drain(0)

    def up_chunk(u, first=False, final=False):
        for n in range(4):
            up_copy(u, n).wait()
        if not first and not final:
            @pl.when(u <= 2)
            def _():
                for n in range(4):
                    up_copy(u + 3, n).start()
            pl.when(u == 3)(lambda: start_down(0))
            pl.when(u == 4)(lambda: start_down(4))
        with jax.named_scope("up"):
            if final:
                start_down(8)
            lhs = rows2d(hg2[u])
            slot = lax.rem(4 * u, RING)
            for n in range(4):
                for p in range(3):
                    c = slice(n * NC + p * NP, n * NC + (p + 1) * NP)
                    d = dot(lhs, ring[slot + n, :, p * NP:(p + 1) * NP])
                    if first:
                        acc[:, c] = d
                    elif final:
                        ub[:, c] = jax.nn.gelu(acc[:, c] + d + bu_row[:, c], approximate=True).astype(BF16)
                    else:
                        acc[:, c] += d

    def a2_done(u):
        with jax.named_scope("a2_complete"):
            for h in range(2):
                complete(a2(u, h))

    with jax.named_scope("a2_step"):
        forward(a2(0, 1))
        for h in range(2):
            own(a2(2, h))
        forward(a2(1, 1))
        for u in (3, 4):
            for h in range(2):
                own(a2(u, h))
        forward_diag(a2(0, 1))
    a2_done(0)
    up_chunk(0, first=True)

    def up_body(u, _):
        with jax.named_scope("a2_step"):
            for h in range(2):
                forward(a2(u + 1, h))

            @pl.when(u + 4 < NU)
            def _():
                for h in range(2):
                    own(a2(u + 4, h))

            @pl.when(u > 1)
            def _():
                forward_diag(a2(u, 0))
            forward_diag(a2(u, 1))
        a2_done(u)
        up_chunk(u)
        return 0
    lax.fori_loop(1, NU - 1, up_body, 0)

    for h in range(2):
        forward_diag(a2(NU - 1, h))
    a2_done(NU - 1)
    up_chunk(NU - 1, final=True)
    start_down(12)

    def a2_drain(u, _):
        for h in range(2):
            for j in range(7):
                wait_send(a2(u, h), j)
        return 0
    lax.fori_loop(0, NU, a2_drain, 0)

    def down_product(n):
        for k in range(3):
            down_copy(n, k).wait()
        slot = lax.rem(n, 3)
        with jax.named_scope("down"):
            for half in range(2):
                d = sum(dot(ub[:, k * KC:(k + 1) * KC], ring[lax.rem(8 + 3 * n + k, RING), :, half * NP:(half + 1) * NP]) for k in range(3))
                part[slot, :, :, half * NP:(half + 1) * NP] = d.reshape(N_DEV, ROWS, NP)
        rs_stage1(1, n)

        @pl.when(n + 5 < NCH)
        def _():
            down_copy(n + 5, 1).start()
            down_copy(n + 5, 2).start()

        @pl.when(n + 6 < NCH)
        def _():
            down_copy(n + 6, 0).start()

    def down_body(n, _):
        @pl.when(n < NCH)
        def _():
            down_product(n)

        @pl.when(jnp.logical_and(n >= 1, n < NCH + 1))
        def _():
            rs_stage2(1, n - 1)

        @pl.when(jnp.logical_and(n >= 3, n < NCH + 3))
        def _():
            rs_stage3(1, n - 3)

        @pl.when(n >= 5)
        def _():
            total = rs_stage4(1, n - 5)
            cols = pl.ds(pl.multiple_of((n - 5) * CW, CW), CW)
            res = rows2d(out_ref[:, :, cols]).astype(F32) + (total + bd_row[:, cols])
            out_ref[:, :, cols] = res.astype(BF16).reshape(B, S_LOC, CW)
        return 0
    lax.fori_loop(0, NCH + 5, down_body, 0)
    rs_drain(1)


def solution(mesh):
    def device_body(hidden, ln1_gain, ln1_bias, w_qkv, b_qkv, w_out, b_out, ln2_gain, ln2_bias, w_up, b_up, w_down, b_down):
        any_spec = pl.BlockSpec(memory_space=pl.ANY)
        vmem = pl.BlockSpec(memory_space=pltpu.VMEM)

        def row(v):
            return v.reshape(1, -1)

        def tile(v):
            return v.reshape(-1, HD)

        two = pltpu.VMEM((NCH, 2, ROWS, CW), BF16)
        four = pltpu.VMEM((NCH, 4, ROWS, CW), BF16)
        one = pltpu.VMEM((NCH, ROWS, CW), BF16)
        dma = pltpu.SemaphoreType.DMA
        return pl.pallas_call(
            kernel,
            out_shape=jax.ShapeDtypeStruct((B, S_LOC, D), BF16),
            in_specs=[any_spec] * 5 + [vmem] * 8,
            out_specs=vmem,
            scratch_shapes=[
                pltpu.VMEM((B, S_LOC, D), BF16),
                pltpu.VMEM((NV, N_DEV, S_LOC, VW), BF16),
                pltpu.VMEM((NU, N_DEV, ROWS, KC), BF16),
                pltpu.VMEM((M, FF), F32),
                pltpu.VMEM((SEQ, 3 * NQ), BF16),
                pltpu.VMEM((SEQ, NQ), BF16),
                pltpu.VMEM((M, FF), BF16),
                pltpu.VMEM((3, N_DEV, ROWS, CW), F32),
                pltpu.VMEM((4, 4, ROWS, CW), BF16), four, two, two, one, one,
                pltpu.VMEM((8, 2, ROWS, CW), F32),
                pltpu.VMEM((NS, KC, NC), BF16),
                pltpu.VMEM((3, NQ, 3 * CW), BF16),
                pltpu.VMEM((1, D), F32),
                pltpu.VMEM((1, D), F32),
                pltpu.VMEM((1, FF), F32),
                dma, dma((NS,)), dma((5,)),
                dma((NV, 7)), dma((NV, 7)),
                dma((NU, 2, 7)), dma((NU, 2, 7)),
                dma((2, NCH, 3)), dma((2, NCH, 3)),
            ],
            compiler_params=pltpu.CompilerParams(collective_id=0, has_side_effects=True, vmem_limit_bytes=67_043_328),
            name="decoder_layer",
        )(hidden, jnp.transpose(w_qkv, (1, 2, 0, 3)), w_out.reshape(HEADS * HD, D), w_up, w_down,
          row(ln1_gain), row(ln1_bias), b_qkv, tile(b_out), row(ln2_gain), row(ln2_bias), tile(b_up), tile(b_down))

    in_layout = (P("dp", "tp", None), P(), P(), P(None, None, "tp", None), P(None, "tp", None), P("tp", None, None), P(), P(), P(), P(None, "tp"), P("tp"), P("tp", None), P())
    return jax.shard_map(device_body, mesh=mesh, in_specs=in_layout, out_specs=P("dp", "tp", None), check_vma=False)
```

```python
import jax
import jax.numpy as jnp
from jax import lax
from jax.experimental import pallas as pl
from jax.experimental.pallas import tpu as pltpu
from jax.sharding import PartitionSpec as P

MESH = pl.DeviceIdType.MESH
F32 = jnp.float32
BF16 = jnp.bfloat16
LN_EPS = 1e-5

N_DEV = 8
B, S_LOC = 3, 16
ROWS = B * S_LOC
SEQ = N_DEV * S_LOC
M = N_DEV * ROWS
D = 6144
HEADS, HD = 6, 128
NQ = HEADS * HD
FF = 3072
KC = 1024
NC = 768
NP = NC // 3
NU = D // KC
VK = 4
VW = D // VK
NV = VK * B
LAG3, LAG4 = 4, 7
AHEAD = 4
NCH = 12
CW = 512
NS = 18
RING = 16


def rows2d(v):
    return v.reshape(-1, v.shape[-1])


def dot(a, b):
    return jnp.dot(a, b, preferred_element_type=F32)


def kernel(x_hbm, wq_hbm, wo_hbm, wu_hbm, wd_hbm, g1_ref, c1_ref, bq_ref, bo_ref, g2_ref, c2_ref, bu_ref, bd_ref, out_ref,
           xv, hg1, hg2, acc, qkv, ctx, ub, part, s1, r1, s2, r2, s3, r3, keep, ring, wo, bo_row, bd_row, bu_row,
           x_sem, w_sem, wo_sem, a1_send, a1_recv, a2_send, a2_recv, rs_send, rs_recv):
    me = lax.axis_index("tp")
    core = lax.rem(me, 2)
    xbit = lax.rem(me // 2, 2)
    ybit = me // 4
    dx = 2 - 4 * xbit
    dy = 4 - 8 * ybit
    ds = 1 - 2 * core
    sis = me + ds
    n1 = me + (1 - core) * dx + core * dy
    n2 = me + (1 - core) * dy + core * dx
    dg = me + dx + dy
    c_me, c_n1, c_n2, c_dg = me // 2, n1 // 2, n2 // 2, dg // 2

    def start_qkv(t):
        for j in range(NU):
            i = t * NU + j
            for h in range(HEADS):
                pltpu.make_async_copy(wq_hbm.at[t, h, j * KC:(j + 1) * KC, :], ring.at[i, :, h * HD:(h + 1) * HD], w_sem.at[i]).start()

    def up_copy(k, n):
        slot = lax.rem(4 * k, RING) + n
        k0 = pl.multiple_of(k * KC, KC)
        return pltpu.make_async_copy(wu_hbm.at[pl.ds(k0, KC), n * NC:(n + 1) * NC], ring.at[slot], w_sem.at[slot])

    def down_copy(n, k):
        slot = lax.rem(8 + 3 * n + k, RING)
        n0 = pl.multiple_of(n * CW, CW)
        return pltpu.make_async_copy(wd_hbm.at[k * KC:(k + 1) * KC, pl.ds(n0, CW)], ring.at[slot, :, 0:CW], w_sem.at[slot])

    def start_down(first):
        for j in range(first, first + 4):
            down_copy(j // 3, j % 3).start()

    def out_copies(n):
        cols = slice(n * 3 * CW, (n + 1) * 3 * CW)
        if n < 3:
            return [pltpu.make_async_copy(wo_hbm.at[:, cols], wo.at[n], wo_sem.at[n])]
        return [pltpu.make_async_copy(wo_hbm.at[k * M:(k + 1) * M, cols], ub.at[:, k * 3 * CW:(k + 1) * 3 * CW], wo_sem.at[n + k]) for k in range(2)]

    def a1_copy(v, j, block, to):
        ref = hg1.at[v, block]
        return pltpu.make_async_remote_copy(src_ref=ref, dst_ref=ref, send_sem=a1_send.at[v, j], recv_sem=a1_recv.at[v, j],
                                            device_id={"tp": to}, device_id_type=MESH)

    def a2_copy(u, h, j, block, to):
        ref = hg2.at[u, block, pl.ds(32 * h, 32 - 16 * h), :]
        return pltpu.make_async_remote_copy(src_ref=ref, dst_ref=ref, send_sem=a2_send.at[u, h, j], recv_sem=a2_recv.at[u, h, j],
                                            device_id={"tp": to}, device_id_type=MESH)

    def send(make, j):
        make(j, (me, me, me, n1, n1, n2, dg)[j], (n1, n2, sis, n2, sis, sis, sis)[j]).start()

    def wait_send(make, j):
        make(j, (me, me, me, n1, n1, n2, dg)[j], (n1, n2, sis, n2, sis, sis, sis)[j]).wait_send()

    def arrived(make, j):
        make(j, (n1, n2, sis, dg, n2 + ds, n1 + ds, dg + ds)[j], me).wait_recv()

    def own(make):
        for j in (0, 1, 2):
            send(make, j)

    def forward(make):
        arrived(make, 0)
        send(make, 3)
        send(make, 4)
        arrived(make, 1)
        send(make, 5)

    def forward_diag(make):
        arrived(make, 3)
        send(make, 6)

    def complete(make):
        for j in (2, 4, 5, 6):
            arrived(make, j)

    def a1(v):
        return lambda j, block, to: a1_copy(v, j, block, to)

    def a2(u, h):
        return lambda j, block, to: a2_copy(u, h, j, block, to)

    def a1_forward(v):
        with jax.named_scope("a1_forward"):
            @pl.when(v < NV)
            def _():
                forward(a1(v))

    def a1_diag(v):
        with jax.named_scope("a1_diag"):
            @pl.when(v < NV)
            def _():
                forward_diag(a1(v))

    def rs_copy(p, c, j):
        src, dst, to = ((s1, r1, sis), (s2, r2, n1), (s3, r3, n2))[j]
        return pltpu.make_async_remote_copy(src_ref=src.at[lax.rem(c, 4) if j == 0 else c], dst_ref=dst.at[c], send_sem=rs_send.at[p, c, j], recv_sem=rs_recv.at[p, c, j],
                                            device_id={"tp": to}, device_id_type=MESH)

    def rs_stage1(p, c):
        slot = lax.rem(c, 3)

        @pl.when(c >= 4)
        def _():
            rs_copy(p, c - 4, 0).wait_send()

        for q in range(4):
            s1[lax.rem(c, 4), q] = part[slot, 2 * q + 1 - core].astype(BF16)
        rs_copy(p, c, 0).start()

    def rs_stage2(p, c):
        slot = lax.rem(c, 3)
        with jax.named_scope("rs_wait1"):
            rs_copy(p, c, 0).wait_recv()

        def total(q):
            return part[slot, 2 * q + core] + r1[c, q].astype(F32)

        s2[c, 0] = total(c_n1).astype(BF16)
        s2[c, 1] = total(c_dg).astype(BF16)
        keep[lax.rem(c, 8), 0] = total(c_me)
        keep[lax.rem(c, 8), 1] = total(c_n2)
        rs_copy(p, c, 1).start()

    def rs_stage3(p, c):
        with jax.named_scope("rs_wait2"):
            rs_copy(p, c, 1).wait_recv()
        s3[c] = (keep[lax.rem(c, 8), 1] + r2[c, 1].astype(F32)).astype(BF16)
        keep[lax.rem(c, 8), 0] = keep[lax.rem(c, 8), 0] + r2[c, 0].astype(F32)
        rs_copy(p, c, 2).start()

    def rs_stage4(p, c):
        with jax.named_scope("rs_wait3"):
            rs_copy(p, c, 2).wait_recv()
        return keep[lax.rem(c, 8), 0] + r3[c].astype(F32)

    def rs_drain(p):
        def body(c, _):
            for j in (1, 2):
                rs_copy(p, c, j).wait_send()
            return 0
        lax.fori_loop(0, NCH, body, 0)
        for c in range(NCH - 4, NCH):
            rs_copy(p, c, 0).wait_send()

    def row_stats(xf):
        mean = jnp.mean(xf, axis=-1, keepdims=True)
        cen = xf - mean
        var = jnp.mean(cen * cen, axis=-1, keepdims=True)
        return mean, lax.rsqrt(var + LN_EPS)

    x_copy = pltpu.make_async_copy(x_hbm, xv, x_sem)
    x_copy.start()
    barrier = pltpu.get_barrier_semaphore()
    for other in (sis, n1, n2):
        pl.semaphore_signal(barrier, inc=1, device_id={"tp": other}, device_id_type=MESH)
    for dst, src in ((bo_row, bo_ref), (bd_row, bd_ref), (bu_row, bu_ref)):
        wide = src[...].astype(F32)
        for r in range(src.shape[0]):
            dst[:, r * HD:(r + 1) * HD] = wide[r:r + 1, :]
    with jax.named_scope("entry_x"):
        x_copy.wait()
    start_qkv(0)

    with jax.named_scope("ln1"):
        for b in range(B):
            mean, rstd = row_stats(xv[b].astype(F32))
            for k in range(VK):
                cols = slice(k * VW, (k + 1) * VW)
                h = (xv[b, :, cols].astype(F32) - mean) * rstd * g1_ref[:, cols] + c1_ref[:, cols]
                hg1[VK * b + k, me] = h.astype(BF16)
    with jax.named_scope("entry_barrier"):
        pl.semaphore_wait(barrier, 3)
    for v in range(AHEAD):
        own(a1(v))

    causal = lax.broadcasted_iota(jnp.int32, (SEQ, SEQ), 0) >= lax.broadcasted_iota(jnp.int32, (SEQ, SEQ), 1)

    def project(s, t):
        @pl.when(s == 0)
        def _():
            for j in range(NU):
                i = t * NU + j
                pltpu.make_async_copy(wu_hbm.at[0:KC, 0:NC], ring.at[i], w_sem.at[i]).wait()

        with jax.named_scope("qkv"):
            lhs = []
            for f in range(D // 512):
                lhs.append((rows2d(hg1[VK * s + f // 3, :, :, (f % 3) * 512:(f % 3 + 1) * 512]), t * NU + f // 2, (f % 2) * 512))
            bias = bq_ref[t].astype(F32)
            for p in range(3):
                v = sum(dot(a, ring[i, r0:r0 + 512, p * NP:(p + 1) * NP]) for a, i, r0 in lhs)
                for k in range(2):
                    h = 2 * p + k
                    cols = pl.ds(pl.multiple_of(t * NQ + h * HD, HD), HD)
                    qkv[:, cols] = (v[:, k * HD:(k + 1) * HD] + bias[h:h + 1, :]).astype(BF16)

        @pl.when(s == B - 1)
        def _():
            for tt, lo, hi in ((0, 0, 4), (1, 4, 12), (2, 12, 16)):
                @pl.when(t == tt)
                def _():
                    for i in range(lo, hi):
                        up_copy(i // 4, i % 4).start()

    def attend():
        with jax.named_scope("attn"):
            def head(t, h):
                return qkv[:, t * NQ + h * HD:t * NQ + (h + 1) * HD]

            logits = [lax.dot_general(head(0, h), head(1, h), (((1,), (1,)), ((), ())), preferred_element_type=F32) for h in range(HEADS)]
            weights = []
            for x in logits:
                x = jnp.where(causal, x * HD ** -0.5, -1e30)
                e = jnp.exp(x - jnp.max(x, axis=-1, keepdims=True))
                weights.append((e * (1.0 / jnp.sum(e, axis=-1, keepdims=True))).astype(BF16))
            for h in range(HEADS):
                ctx[:, h * HD:(h + 1) * HD] = dot(weights[h], head(2, h)).astype(BF16)

    def out_product(s, n):
        @pl.when(s == 0)
        def _():
            for copy in out_copies(n):
                copy.wait()

        c = 4 * s + n
        slot = lax.rem(c, 3)
        with jax.named_scope("out"):
            for p in range(6):
                if n < 3:
                    d = dot(ctx[...], wo[n, :, p * NP:(p + 1) * NP])
                else:
                    d = sum(dot(ctx[:, k * M:(k + 1) * M], ub[:, k * 3 * CW + p * NP:k * 3 * CW + (p + 1) * NP]) for k in range(2))
                g, half = p // 2, p % 2
                part[slot, :, g * S_LOC:(g + 1) * S_LOC, half * NP:(half + 1) * NP] = d.reshape(N_DEV, S_LOC, NP)
        rs_stage1(0, c)

    def out_finish(s, n):
        total = rs_stage4(0, 4 * s + n)
        for g in range(3):
            cols = slice((3 * n + g) * CW, (3 * n + g + 1) * CW)
            out_ref[s, :, cols] = (xv[s, :, cols].astype(F32) + (total[g * S_LOC:(g + 1) * S_LOC] + bo_row[:, cols])).astype(BF16)

    def norm2(s):
        with jax.named_scope("ln2"):
            r = pl.ds(pl.multiple_of(s * S_LOC, S_LOC), S_LOC)
            mean, rstd = row_stats(out_ref[s].astype(F32))
            for u in range(NU):
                cols = slice(u * KC, (u + 1) * KC)
                h = (out_ref[s, :, cols].astype(F32) - mean) * rstd * g2_ref[:, cols] + c2_ref[:, cols]
                hg2[u, me, r, :] = h.astype(BF16)

    forward(a1(0))
    own(a1(AHEAD))
    start_qkv(1)
    forward(a1(1))
    own(a1(AHEAD + 1))
    forward(a1(2))
    own(a1(AHEAD + 2))
    forward_diag(a1(0))
    start_qkv(2)
    forward(a1(3))
    own(a1(AHEAD + 3))
    forward_diag(a1(1))
    forward(a1(4))
    forward_diag(a1(2))
    for n in range(4):
        for copy in out_copies(n):
            copy.start()
    for v in range(2 * AHEAD, NV):
        own(a1(v))
    forward_diag(a1(3))

    def seq_body(s, _):
        b0 = 4 * s - 4

        def before(f):
            pl.when(s >= 1)(f)

        with jax.named_scope("a1_complete"):
            for k in range(VK):
                complete(a1(VK * s + k))

        def qkv_body(t, _):
            project(s, t)

            @pl.when(jnp.logical_and(s >= 1, t == 0))
            def _():
                rs_stage2(0, b0 + 3)

            @pl.when(jnp.logical_and(s >= 1, t >= 1))
            def _():
                rs_stage3(0, b0 + t - 1)
            a1_forward(VK * s + 5 + t)
            return 0
        lax.fori_loop(0, 3, qkv_body, 0)
        for k in range(2):
            a1_diag(VK * s + 4 + k)
        attend()
        before(lambda: rs_stage3(0, b0 + 2))
        for k in range(2, VK):
            a1_diag(VK * s + 4 + k)
        a1_forward(VK * s + 8)
        out_product(s, 0)
        before(lambda: out_finish(s - 1, 0))
        out_product(s, 1)

        @before
        def _():
            rs_stage3(0, b0 + 3)
            out_finish(s - 1, 1)

        out_product(s, 2)
        rs_stage2(0, 4 * s)
        before(lambda: out_finish(s - 1, 2))
        out_product(s, 3)
        rs_stage2(0, 4 * s + 1)

        @before
        def _():
            out_finish(s - 1, 3)
            norm2(s - 1)

        rs_stage2(0, 4 * s + 2)
        return 0
    lax.fori_loop(0, B, seq_body, 0)

    c0, last = NCH - 4, B - 1
    rs_stage2(0, c0 + 3)
    own(a2(0, 0))
    own(a2(1, 0))
    rs_stage3(0, c0)
    rs_stage3(0, c0 + 1)
    out_finish(last, 0)
    rs_stage3(0, c0 + 2)
    out_finish(last, 1)
    rs_stage3(0, c0 + 3)
    forward(a2(0, 0))
    out_finish(last, 2)
    forward(a2(1, 0))
    forward_diag(a2(0, 0))
    out_finish(last, 3)
    norm2(last)
    own(a2(0, 1))
    own(a2(1, 1))
    for h in range(2):
        own(a2(2, h))
    forward_diag(a2(1, 0))

    def a1_drain(v, _):
        for j in range(7):
            wait_send(a1(v), j)
        return 0
    lax.fori_loop(0, NV, a1_drain, 0)
    rs_drain(0)

    def up_part(u, lo, hi, first=False, final=False):
        for n in range(lo, hi):
            up_copy(u, n).wait()
        with jax.named_scope("up"):
            lhs = rows2d(hg2[u])
            slot = lax.rem(4 * u, RING)
            for n in range(lo, hi):
                for p in range(3):
                    c = slice(n * NC + p * NP, n * NC + (p + 1) * NP)
                    d = dot(lhs, ring[slot + n, :, p * NP:(p + 1) * NP])
                    if first:
                        acc[:, c] = d
                    elif final:
                        ub[:, c] = jax.nn.gelu(acc[:, c] + d + bu_row[:, c], approximate=True).astype(BF16)
                    else:
                        acc[:, c] += d

    def a2_done(u):
        with jax.named_scope("a2_complete"):
            for h in range(2):
                complete(a2(u, h))

    def a2_forward(u, parts=(0, 1)):
        with jax.named_scope("a2_forward"):
            for h in parts:
                forward(a2(u, h))

    def a2_diag(u, parts=(0, 1)):
        with jax.named_scope("a2_diag"):
            for h in parts:
                forward_diag(a2(u, h))

    a2_forward(0, (1,))
    for h in range(2):
        own(a2(3, h))
    a2_forward(1, (1,))
    for h in range(2):
        own(a2(4, h))
    a2_diag(0, (1,))
    a2_done(0)
    up_part(0, 0, 2, first=True)
    a2_forward(2)
    a2_diag(1, (1,))
    up_part(0, 2, 4, first=True)

    def up_body(u, _):
        @pl.when(u == 1)
        def _():
            for h in range(2):
                own(a2(5, h))

        a2_done(u)
        pl.when(u <= 2)(lambda: [up_copy(u + 3, n).start() for n in range(4)] and None)
        pl.when(u == 3)(lambda: start_down(0))
        pl.when(u == 4)(lambda: start_down(4))
        up_part(u, 0, 2)

        @pl.when(u + 2 < NU)
        def _():
            a2_forward(u + 2)
        a2_diag(u + 1)
        up_part(u, 2, 4)
        return 0
    lax.fori_loop(1, NU - 1, up_body, 0)

    a2_done(NU - 1)
    start_down(8)
    up_part(NU - 1, 0, 4, final=True)
    start_down(12)

    def a2_drain(u, _):
        for h in range(2):
            for j in range(7):
                wait_send(a2(u, h), j)
        return 0
    lax.fori_loop(0, NU, a2_drain, 0)

    def down_product(n):
        for k in range(3):
            down_copy(n, k).wait()
        slot = lax.rem(n, 3)
        with jax.named_scope("down"):
            for half in range(2):
                d = sum(dot(ub[:, k * KC:(k + 1) * KC], ring[lax.rem(8 + 3 * n + k, RING), :, half * NP:(half + 1) * NP]) for k in range(3))
                part[slot, :, :, half * NP:(half + 1) * NP] = d.reshape(N_DEV, ROWS, NP)
        rs_stage1(1, n)

        @pl.when(n + 5 < NCH)
        def _():
            down_copy(n + 5, 1).start()
            down_copy(n + 5, 2).start()

        @pl.when(n + 6 < NCH)
        def _():
            down_copy(n + 6, 0).start()

    def down_body(n, _):
        @pl.when(n < NCH)
        def _():
            down_product(n)

        @pl.when(jnp.logical_and(n >= 1, n < NCH + 1))
        def _():
            rs_stage2(1, n - 1)

        @pl.when(jnp.logical_and(n >= LAG3, n < NCH + LAG3))
        def _():
            rs_stage3(1, n - LAG3)

        @pl.when(n >= LAG4)
        def _():
            m = n - LAG4
            total = rs_stage4(1, m)
            cols = pl.ds(pl.multiple_of(m * CW, CW), CW)
            res = rows2d(out_ref[:, :, cols]).astype(F32) + (total + bd_row[:, cols])
            out_ref[:, :, cols] = res.astype(BF16).reshape(B, S_LOC, CW)
        return 0
    lax.fori_loop(0, NCH + LAG4, down_body, 0)
    rs_drain(1)


def solution(mesh):
    def device_body(hidden, ln1_gain, ln1_bias, w_qkv, b_qkv, w_out, b_out, ln2_gain, ln2_bias, w_up, b_up, w_down, b_down):
        any_spec = pl.BlockSpec(memory_space=pl.ANY)
        vmem = pl.BlockSpec(memory_space=pltpu.VMEM)

        def row(v):
            return v.reshape(1, -1)

        def tile(v):
            return v.reshape(-1, HD)

        two = pltpu.VMEM((NCH, 2, ROWS, CW), BF16)
        four = pltpu.VMEM((NCH, 4, ROWS, CW), BF16)
        one = pltpu.VMEM((NCH, ROWS, CW), BF16)
        dma = pltpu.SemaphoreType.DMA
        return pl.pallas_call(
            kernel,
            out_shape=jax.ShapeDtypeStruct((B, S_LOC, D), BF16),
            in_specs=[any_spec] * 5 + [vmem] * 8,
            out_specs=vmem,
            scratch_shapes=[
                pltpu.VMEM((B, S_LOC, D), BF16),
                pltpu.VMEM((NV, N_DEV, S_LOC, VW), BF16),
                pltpu.VMEM((NU, N_DEV, ROWS, KC), BF16),
                pltpu.VMEM((M, FF), F32),
                pltpu.VMEM((SEQ, 3 * NQ), BF16),
                pltpu.VMEM((SEQ, NQ), BF16),
                pltpu.VMEM((M, FF), BF16),
                pltpu.VMEM((3, N_DEV, ROWS, CW), F32),
                pltpu.VMEM((4, 4, ROWS, CW), BF16), four, two, two, one, one,
                pltpu.VMEM((8, 2, ROWS, CW), F32),
                pltpu.VMEM((NS, KC, NC), BF16),
                pltpu.VMEM((3, NQ, 3 * CW), BF16),
                pltpu.VMEM((1, D), F32),
                pltpu.VMEM((1, D), F32),
                pltpu.VMEM((1, FF), F32),
                dma, dma((NS,)), dma((5,)),
                dma((NV, 7)), dma((NV, 7)),
                dma((NU, 2, 7)), dma((NU, 2, 7)),
                dma((2, NCH, 3)), dma((2, NCH, 3)),
            ],
            compiler_params=pltpu.CompilerParams(collective_id=0, has_side_effects=True, vmem_limit_bytes=67_043_328),
            name="decoder_layer",
        )(hidden, jnp.transpose(w_qkv, (1, 2, 0, 3)), w_out.reshape(HEADS * HD, D), w_up, w_down,
          row(ln1_gain), row(ln1_bias), b_qkv, tile(b_out), row(ln2_gain), row(ln2_bias), tile(b_up), tile(b_down))

    in_layout = (P("dp", "tp", None), P(), P(), P(None, None, "tp", None), P(None, "tp", None), P("tp", None, None), P(), P(), P(), P(None, "tp"), P("tp"), P("tp", None), P())
    return jax.shard_map(device_body, mesh=mesh, in_specs=in_layout, out_specs=P("dp", "tp", None), check_vma=False)
```

```python
import jax
import jax.numpy as jnp
from jax import lax
from jax.experimental import pallas as pl
from jax.experimental.pallas import tpu as pltpu
from jax.sharding import PartitionSpec as P

MESH = pl.DeviceIdType.MESH
F32 = jnp.float32
BF16 = jnp.bfloat16
LN_EPS = 1e-5

N_DEV = 8
B, S_LOC = 3, 16
ROWS = B * S_LOC
SEQ = N_DEV * S_LOC
M = N_DEV * ROWS
D = 6144
HEADS, HD = 6, 128
NQ = HEADS * HD
FF = 3072
KC = 1024
NC = 768
NP = NC // 3
NU = D // KC
VK = 4
VW = D // VK
NV = VK * B
LAG3, LAG4 = 4, 7
AHEAD = 4
NCH = 12
CW = 512
NS = 18
RING = 16


def rows2d(v):
    return v.reshape(-1, v.shape[-1])


def dot(a, b):
    return jnp.dot(a, b, preferred_element_type=F32)


def kernel(x_hbm, wq_hbm, wo_hbm, wu_hbm, wd_hbm, g1_ref, c1_ref, bq_ref, bo_ref, g2_ref, c2_ref, bu_ref, bd_ref, out_hbm,
           xv, hg1, hg2, acc, qkv, ctx, ub, part, s1, r1, s2, r2, s3, r3, keep, res, ring, wo, bo_row, bd_row, bu_row,
           x_sem, o_sem, w_sem, wo_sem, a1_send, a1_recv, a2_send, a2_recv, rs_send, rs_recv):
    me = lax.axis_index("tp")
    core = lax.rem(me, 2)
    xbit = lax.rem(me // 2, 2)
    ybit = me // 4
    dx = 2 - 4 * xbit
    dy = 4 - 8 * ybit
    ds = 1 - 2 * core
    sis = me + ds
    n1 = me + (1 - core) * dx + core * dy
    n2 = me + (1 - core) * dy + core * dx
    dg = me + dx + dy
    c_me, c_n1, c_n2, c_dg = me // 2, n1 // 2, n2 // 2, dg // 2

    def start_qkv(t):
        for j in range(NU):
            i = t * NU + j
            for h in range(HEADS):
                pltpu.make_async_copy(wq_hbm.at[t, h, j * KC:(j + 1) * KC, :], ring.at[i, :, h * HD:(h + 1) * HD], w_sem.at[i]).start()

    def up_copy(k, n):
        slot = lax.rem(4 * k, RING) + n
        k0 = pl.multiple_of(k * KC, KC)
        return pltpu.make_async_copy(wu_hbm.at[pl.ds(k0, KC), n * NC:(n + 1) * NC], ring.at[slot], w_sem.at[slot])

    def down_copy(n, k):
        slot = lax.rem(8 + 3 * n + k, RING)
        n0 = pl.multiple_of(n * CW, CW)
        return pltpu.make_async_copy(wd_hbm.at[k * KC:(k + 1) * KC, pl.ds(n0, CW)], ring.at[slot, :, 0:CW], w_sem.at[slot])

    def start_down(first):
        for j in range(first, first + 4):
            down_copy(j // 3, j % 3).start()

    def out_copies(n):
        cols = slice(n * 3 * CW, (n + 1) * 3 * CW)
        if n < 3:
            return [pltpu.make_async_copy(wo_hbm.at[:, cols], wo.at[n], wo_sem.at[n])]
        return [pltpu.make_async_copy(wo_hbm.at[k * M:(k + 1) * M, cols], ub.at[:, k * 3 * CW:(k + 1) * 3 * CW], wo_sem.at[n + k]) for k in range(2)]

    def a1_copy(v, j, block, to):
        ref = hg1.at[v, block]
        return pltpu.make_async_remote_copy(src_ref=ref, dst_ref=ref, send_sem=a1_send.at[v, j], recv_sem=a1_recv.at[v, j],
                                            device_id={"tp": to}, device_id_type=MESH)

    def a2_copy(u, h, j, block, to):
        ref = hg2.at[u, block, pl.ds(32 * h, 32 - 16 * h), :]
        return pltpu.make_async_remote_copy(src_ref=ref, dst_ref=ref, send_sem=a2_send.at[u, h, j], recv_sem=a2_recv.at[u, h, j],
                                            device_id={"tp": to}, device_id_type=MESH)

    def send(make, j):
        make(j, (me, me, me, n1, n1, n2, dg)[j], (n1, n2, sis, n2, sis, sis, sis)[j]).start()

    def wait_send(make, j):
        make(j, (me, me, me, n1, n1, n2, dg)[j], (n1, n2, sis, n2, sis, sis, sis)[j]).wait_send()

    def arrived(make, j):
        make(j, (n1, n2, sis, dg, n2 + ds, n1 + ds, dg + ds)[j], me).wait_recv()

    def own(make):
        for j in (0, 1, 2):
            send(make, j)

    def forward(make):
        arrived(make, 0)
        send(make, 3)
        send(make, 4)
        arrived(make, 1)
        send(make, 5)

    def forward_diag(make):
        arrived(make, 3)
        send(make, 6)

    def complete(make):
        for j in (2, 4, 5, 6):
            arrived(make, j)

    def a1(v):
        return lambda j, block, to: a1_copy(v, j, block, to)

    def a2(u, h):
        return lambda j, block, to: a2_copy(u, h, j, block, to)

    def a1_forward(v):
        with jax.named_scope("a1_forward"):
            @pl.when(v < NV)
            def _():
                forward(a1(v))

    def a1_diag(v):
        with jax.named_scope("a1_diag"):
            @pl.when(v < NV)
            def _():
                forward_diag(a1(v))

    def rs_copy(p, c, j):
        src, dst, to = ((s1, r1, sis), (s2, r2, n1), (s3, r3, n2))[j]
        return pltpu.make_async_remote_copy(src_ref=src.at[lax.rem(c, 4) if j == 0 else c], dst_ref=dst.at[c], send_sem=rs_send.at[p, c, j], recv_sem=rs_recv.at[p, c, j],
                                            device_id={"tp": to}, device_id_type=MESH)

    def rs_stage1(p, c):
        slot = lax.rem(c, 3)

        @pl.when(c >= 4)
        def _():
            rs_copy(p, c - 4, 0).wait_send()

        for q in range(4):
            s1[lax.rem(c, 4), q] = part[slot, 2 * q + 1 - core].astype(BF16)
        rs_copy(p, c, 0).start()

    def rs_stage2(p, c):
        slot = lax.rem(c, 3)
        with jax.named_scope("rs_wait1"):
            rs_copy(p, c, 0).wait_recv()

        def total(q):
            return part[slot, 2 * q + core] + r1[c, q].astype(F32)

        s2[c, 0] = total(c_n1).astype(BF16)
        s2[c, 1] = total(c_dg).astype(BF16)
        keep[lax.rem(c, 8), 0] = total(c_me)
        keep[lax.rem(c, 8), 1] = total(c_n2)
        rs_copy(p, c, 1).start()

    def rs_stage3(p, c):
        with jax.named_scope("rs_wait2"):
            rs_copy(p, c, 1).wait_recv()
        s3[c] = (keep[lax.rem(c, 8), 1] + r2[c, 1].astype(F32)).astype(BF16)
        keep[lax.rem(c, 8), 0] = keep[lax.rem(c, 8), 0] + r2[c, 0].astype(F32)
        rs_copy(p, c, 2).start()

    def rs_stage4(p, c):
        with jax.named_scope("rs_wait3"):
            rs_copy(p, c, 2).wait_recv()
        return keep[lax.rem(c, 8), 0] + r3[c].astype(F32)

    def rs_drain(p):
        def body(c, _):
            for j in (1, 2):
                rs_copy(p, c, j).wait_send()
            return 0
        lax.fori_loop(0, NCH, body, 0)
        for c in range(NCH - 4, NCH):
            rs_copy(p, c, 0).wait_send()

    def row_stats(xf):
        mean = jnp.mean(xf, axis=-1, keepdims=True)
        cen = xf - mean
        var = jnp.mean(cen * cen, axis=-1, keepdims=True)
        return mean, lax.rsqrt(var + LN_EPS)

    x_copy = pltpu.make_async_copy(x_hbm, xv, x_sem)
    x_copy.start()
    barrier = pltpu.get_barrier_semaphore()
    for other in (sis, n1, n2):
        pl.semaphore_signal(barrier, inc=1, device_id={"tp": other}, device_id_type=MESH)
    for dst, src in ((bo_row, bo_ref), (bd_row, bd_ref), (bu_row, bu_ref)):
        wide = src[...].astype(F32)
        for r in range(src.shape[0]):
            dst[:, r * HD:(r + 1) * HD] = wide[r:r + 1, :]
    with jax.named_scope("entry_x"):
        x_copy.wait()
    start_qkv(0)

    with jax.named_scope("ln1"):
        for b in range(B):
            mean, rstd = row_stats(xv[b].astype(F32))
            for k in range(VK):
                cols = slice(k * VW, (k + 1) * VW)
                h = (xv[b, :, cols].astype(F32) - mean) * rstd * g1_ref[:, cols] + c1_ref[:, cols]
                hg1[VK * b + k, me] = h.astype(BF16)
    with jax.named_scope("entry_barrier"):
        pl.semaphore_wait(barrier, 3)
    for v in range(VK):
        own(a1(v))
    start_qkv(1)

    causal = lax.broadcasted_iota(jnp.int32, (SEQ, SEQ), 0) >= lax.broadcasted_iota(jnp.int32, (SEQ, SEQ), 1)

    def project_piece(v):
        with jax.named_scope("qkv0"):
            for t in range(3):
                bias = bq_ref[t].astype(F32)
                for p in range(3):
                    cols = slice(t * NQ + p * NP, t * NQ + (p + 1) * NP)
                    d = sum(dot(rows2d(hg1[v, :, :, (f % 3) * 512:(f % 3 + 1) * 512]), ring[t * NU + f // 2, (f % 2) * 512:(f % 2 + 1) * 512, p * NP:(p + 1) * NP])
                            for f in range(3 * v, 3 * v + 3))
                    if v == 0:
                        acc[0:SEQ, cols] = d
                    elif v < VK - 1:
                        acc[0:SEQ, cols] += d
                    else:
                        d = acc[0:SEQ, cols] + d
                        for k in range(2):
                            h = 2 * p + k
                            qkv[:, t * NQ + h * HD:t * NQ + (h + 1) * HD] = (d[:, k * HD:(k + 1) * HD] + bias[h:h + 1, :]).astype(BF16)

    def project(s, t):
        with jax.named_scope("qkv"):
            lhs = []
            for f in range(D // 512):
                lhs.append((rows2d(hg1[VK * s + f // 3, :, :, (f % 3) * 512:(f % 3 + 1) * 512]), t * NU + f // 2, (f % 2) * 512))
            bias = bq_ref[t].astype(F32)
            for p in range(3):
                v = sum(dot(a, ring[i, r0:r0 + 512, p * NP:(p + 1) * NP]) for a, i, r0 in lhs)
                for k in range(2):
                    h = 2 * p + k
                    cols = pl.ds(pl.multiple_of(t * NQ + h * HD, HD), HD)
                    qkv[:, cols] = (v[:, k * HD:(k + 1) * HD] + bias[h:h + 1, :]).astype(BF16)

        @pl.when(s == B - 1)
        def _():
            for tt, lo, hi in ((0, 0, 4), (1, 4, 12), (2, 12, 16)):
                @pl.when(t == tt)
                def _():
                    for i in range(lo, hi):
                        up_copy(i // 4, i % 4).start()

    def attend():
        with jax.named_scope("attn"):
            def head(t, h):
                return qkv[:, t * NQ + h * HD:t * NQ + (h + 1) * HD]

            logits = [lax.dot_general(head(0, h), head(1, h), (((1,), (1,)), ((), ())), preferred_element_type=F32) for h in range(HEADS)]
            weights = []
            for x in logits:
                x = jnp.where(causal, x * HD ** -0.5, -1e30)
                e = jnp.exp(x - jnp.max(x, axis=-1, keepdims=True))
                weights.append((e * (1.0 / jnp.sum(e, axis=-1, keepdims=True))).astype(BF16))
            for h in range(HEADS):
                ctx[:, h * HD:(h + 1) * HD] = dot(weights[h], head(2, h)).astype(BF16)

    def out_product(s, n):
        @pl.when(s == 0)
        def _():
            for copy in out_copies(n):
                copy.wait()

        c = 4 * s + n
        slot = lax.rem(c, 3)
        with jax.named_scope("out"):
            for p in range(6):
                if n < 3:
                    d = dot(ctx[...], wo[n, :, p * NP:(p + 1) * NP])
                else:
                    d = sum(dot(ctx[:, k * M:(k + 1) * M], ub[:, k * 3 * CW + p * NP:k * 3 * CW + (p + 1) * NP]) for k in range(2))
                g, half = p // 2, p % 2
                part[slot, :, g * S_LOC:(g + 1) * S_LOC, half * NP:(half + 1) * NP] = d.reshape(N_DEV, S_LOC, NP)
        rs_stage1(0, c)

    def out_finish(s, n):
        total = rs_stage4(0, 4 * s + n)
        for g in range(3):
            cols = slice((3 * n + g) * CW, (3 * n + g + 1) * CW)
            res[s, :, cols] = (xv[s, :, cols].astype(F32) + (total[g * S_LOC:(g + 1) * S_LOC] + bo_row[:, cols])).astype(BF16)

    def norm2(s):
        with jax.named_scope("ln2"):
            r = pl.ds(pl.multiple_of(s * S_LOC, S_LOC), S_LOC)
            mean, rstd = row_stats(res[s].astype(F32))
            for u in range(NU):
                cols = slice(u * KC, (u + 1) * KC)
                h = (res[s, :, cols].astype(F32) - mean) * rstd * g2_ref[:, cols] + c2_ref[:, cols]
                hg2[u, me, r, :] = h.astype(BF16)

    for v in range(VK):
        with jax.named_scope("a1_forward"):
            forward(a1(v))
        if v == 0:
            start_qkv(2)
    for v in range(VK, 2 * VK):
        own(a1(v))
    forward_diag(a1(0))
    for v in range(VK):
        if v + 1 < VK:
            with jax.named_scope("a1_diag"):
                forward_diag(a1(v + 1))
        with jax.named_scope("a1_complete"):
            complete(a1(v))
        if v == 0:
            for i in range(NS):
                pltpu.make_async_copy(wu_hbm.at[0:KC, 0:NC], ring.at[i], w_sem.at[i]).wait()
            for n in range(4):
                for copy in out_copies(n):
                    copy.start()
        project_piece(v)
        if v == 1:
            forward(a1(VK))
            for k in range(2 * VK, NV):
                own(a1(k))

    def seq_body(s, _):
        b0 = 4 * s - 4

        def before(f):
            pl.when(s >= 1)(f)

        @pl.when(s >= 1)
        def _():
            with jax.named_scope("a1_complete"):
                for k in range(VK):
                    complete(a1(VK * s + k))

        def qkv_body(t, _):
            pl.when(s >= 1)(lambda: project(s, t))

            @pl.when(jnp.logical_and(s >= 1, t == 0))
            def _():
                rs_stage2(0, b0 + 3)

            @pl.when(jnp.logical_and(s >= 1, t >= 1))
            def _():
                rs_stage3(0, b0 + t - 1)
            a1_forward(VK * s + 5 + t)
            return 0
        lax.fori_loop(0, 3, qkv_body, 0)
        attend()
        before(lambda: rs_stage3(0, b0 + 2))
        out_product(s, 0)
        for k in range(2):
            a1_diag(VK * s + 4 + k)
        before(lambda: out_finish(s - 1, 0))
        out_product(s, 1)

        @before
        def _():
            rs_stage3(0, b0 + 3)
            out_finish(s - 1, 1)

        for k in range(2, VK):
            a1_diag(VK * s + 4 + k)
        a1_forward(VK * s + 8)
        out_product(s, 2)
        rs_stage2(0, 4 * s)
        before(lambda: out_finish(s - 1, 2))
        out_product(s, 3)
        rs_stage2(0, 4 * s + 1)

        @before
        def _():
            out_finish(s - 1, 3)
            norm2(s - 1)

        rs_stage2(0, 4 * s + 2)
        return 0
    lax.fori_loop(0, B, seq_body, 0)

    c0, last = NCH - 4, B - 1
    rs_stage2(0, c0 + 3)
    for k in range(4):
        rs_stage3(0, c0 + k)
    own(a2(0, 0))
    own(a2(1, 0))
    for k in range(4):
        out_finish(last, k)
    norm2(last)
    own(a2(0, 1))
    own(a2(1, 1))
    with jax.named_scope("a2_forward"):
        for u in range(2):
            forward(a2(u, 0))
    for h in range(2):
        own(a2(2, h))

    def a1_drain(v, _):
        for j in range(7):
            wait_send(a1(v), j)
        return 0
    lax.fori_loop(0, NV, a1_drain, 0)
    rs_drain(0)

    def up_part(u, lo, hi, first=False, final=False):
        for n in range(lo, hi):
            up_copy(u, n).wait()
        with jax.named_scope("up"):
            lhs = rows2d(hg2[u])
            slot = lax.rem(4 * u, RING)
            for n in range(lo, hi):
                for p in range(3):
                    c = slice(n * NC + p * NP, n * NC + (p + 1) * NP)
                    d = dot(lhs, ring[slot + n, :, p * NP:(p + 1) * NP])
                    if first:
                        acc[:, c] = d
                    elif final:
                        ub[:, c] = jax.nn.gelu(acc[:, c] + d + bu_row[:, c], approximate=True).astype(BF16)
                    else:
                        acc[:, c] += d

    def a2_done(u):
        with jax.named_scope("a2_complete"):
            for h in range(2):
                complete(a2(u, h))

    def a2_forward(u, parts=(0, 1)):
        with jax.named_scope("a2_forward"):
            for h in parts:
                forward(a2(u, h))

    def a2_diag(u, parts=(0, 1)):
        with jax.named_scope("a2_diag"):
            for h in parts:
                forward_diag(a2(u, h))

    a2_forward(0, (1,))
    for h in range(2):
        own(a2(3, h))
    a2_forward(1, (1,))
    for h in range(2):
        own(a2(4, h))
    a2_diag(0)
    a2_done(0)
    up_part(0, 0, 2, first=True)
    a2_forward(2)
    a2_diag(1)
    up_part(0, 2, 4, first=True)

    def up_body(u, _):
        @pl.when(u == 1)
        def _():
            for h in range(2):
                own(a2(5, h))

        a2_done(u)
        pl.when(u <= 2)(lambda: [up_copy(u + 3, n).start() for n in range(4)] and None)
        pl.when(u == 3)(lambda: start_down(0))
        pl.when(u == 4)(lambda: start_down(4))
        up_part(u, 0, 2)

        @pl.when(u + 2 < NU)
        def _():
            a2_forward(u + 2)
        a2_diag(u + 1)
        up_part(u, 2, 4)
        return 0
    lax.fori_loop(1, NU - 1, up_body, 0)

    a2_done(NU - 1)
    start_down(8)
    up_part(NU - 1, 0, 4, final=True)
    start_down(12)

    def a2_drain(u, _):
        for h in range(2):
            for j in range(7):
                wait_send(a2(u, h), j)
        return 0
    lax.fori_loop(0, NU, a2_drain, 0)

    def down_product(n):
        for k in range(3):
            down_copy(n, k).wait()
        slot = lax.rem(n, 3)
        with jax.named_scope("down"):
            for half in range(2):
                d = sum(dot(ub[:, k * KC:(k + 1) * KC], ring[lax.rem(8 + 3 * n + k, RING), :, half * NP:(half + 1) * NP]) for k in range(3))
                part[slot, :, :, half * NP:(half + 1) * NP] = d.reshape(N_DEV, ROWS, NP)
        rs_stage1(1, n)

        @pl.when(n + 5 < NCH)
        def _():
            down_copy(n + 5, 1).start()
            down_copy(n + 5, 2).start()

        @pl.when(n + 6 < NCH)
        def _():
            down_copy(n + 6, 0).start()

    def down_body(n, _):
        @pl.when(n < NCH)
        def _():
            down_product(n)

        @pl.when(jnp.logical_and(n >= 1, n < NCH + 1))
        def _():
            rs_stage2(1, n - 1)

        @pl.when(jnp.logical_and(n >= LAG3, n < NCH + LAG3))
        def _():
            rs_stage3(1, n - LAG3)

        @pl.when(n >= LAG4)
        def _():
            m = n - LAG4
            total = rs_stage4(1, m)
            cols = pl.ds(pl.multiple_of(m * CW, CW), CW)
            v = rows2d(res[:, :, cols]).astype(F32) + (total + bd_row[:, cols])
            res[:, :, cols] = v.astype(BF16).reshape(B, S_LOC, CW)
            pltpu.make_async_copy(res.at[:, :, cols], out_hbm.at[:, :, cols], o_sem).start()
        return 0
    lax.fori_loop(0, NCH + LAG4, down_body, 0)
    with jax.named_scope("drain"):
        rs_drain(1)
        pltpu.make_async_copy(res, out_hbm, o_sem).wait()


def solution(mesh):
    def device_body(hidden, ln1_gain, ln1_bias, w_qkv, b_qkv, w_out, b_out, ln2_gain, ln2_bias, w_up, b_up, w_down, b_down):
        any_spec = pl.BlockSpec(memory_space=pl.ANY)
        vmem = pl.BlockSpec(memory_space=pltpu.VMEM)

        def row(v):
            return v.reshape(1, -1)

        def tile(v):
            return v.reshape(-1, HD)

        two = pltpu.VMEM((NCH, 2, ROWS, CW), BF16)
        four = pltpu.VMEM((NCH, 4, ROWS, CW), BF16)
        one = pltpu.VMEM((NCH, ROWS, CW), BF16)
        dma = pltpu.SemaphoreType.DMA
        return pl.pallas_call(
            kernel,
            out_shape=jax.ShapeDtypeStruct((B, S_LOC, D), BF16),
            in_specs=[any_spec] * 5 + [vmem] * 8,
            out_specs=any_spec,
            scratch_shapes=[
                pltpu.VMEM((B, S_LOC, D), BF16),
                pltpu.VMEM((NV, N_DEV, S_LOC, VW), BF16),
                pltpu.VMEM((NU, N_DEV, ROWS, KC), BF16),
                pltpu.VMEM((M, FF), F32),
                pltpu.VMEM((SEQ, 3 * NQ), BF16),
                pltpu.VMEM((SEQ, NQ), BF16),
                pltpu.VMEM((M, FF), BF16),
                pltpu.VMEM((3, N_DEV, ROWS, CW), F32),
                pltpu.VMEM((4, 4, ROWS, CW), BF16), four, two, two, one, one,
                pltpu.VMEM((8, 2, ROWS, CW), F32),
                pltpu.VMEM((B, S_LOC, D), BF16),
                pltpu.VMEM((NS, KC, NC), BF16),
                pltpu.VMEM((3, NQ, 3 * CW), BF16),
                pltpu.VMEM((1, D), F32),
                pltpu.VMEM((1, D), F32),
                pltpu.VMEM((1, FF), F32),
                dma, dma, dma((NS,)), dma((5,)),
                dma((NV, 7)), dma((NV, 7)),
                dma((NU, 2, 7)), dma((NU, 2, 7)),
                dma((2, NCH, 3)), dma((2, NCH, 3)),
            ],
            compiler_params=pltpu.CompilerParams(collective_id=0, has_side_effects=True, vmem_limit_bytes=67_043_328),
            name="decoder_layer",
        )(hidden, jnp.transpose(w_qkv, (1, 2, 0, 3)), w_out.reshape(HEADS * HD, D), w_up, w_down,
          row(ln1_gain), row(ln1_bias), b_qkv, tile(b_out), row(ln2_gain), row(ln2_bias), tile(b_up), tile(b_down))

    in_layout = (P("dp", "tp", None), P(), P(), P(None, None, "tp", None), P(None, "tp", None), P("tp", None, None), P(), P(), P(), P(None, "tp"), P("tp"), P("tp", None), P())
    return jax.shard_map(device_body, mesh=mesh, in_specs=in_layout, out_specs=P("dp", "tp", None), check_vma=False)
```

```python
import jax
import jax.numpy as jnp
from jax import lax
from jax.experimental import pallas as pl
from jax.experimental.pallas import tpu as pltpu
from jax.sharding import PartitionSpec as P

MESH = pl.DeviceIdType.MESH
F32 = jnp.float32
BF16 = jnp.bfloat16
LN_EPS = 1e-5

N_DEV = 8
B, S_LOC = 3, 16
ROWS = B * S_LOC
SEQ = N_DEV * S_LOC
M = N_DEV * ROWS
D = 6144
HEADS, HD = 6, 128
NQ = HEADS * HD
FF = 3072
KC = 1024
NC = 768
NP = NC // 3
NU = D // KC
VK = 4
VW = D // VK
NV = VK * B
LAG3, LAG4 = 4, 7
AHEAD = 4
NCH = 12
CW = 512
NS = 18
RING = 16


def rows2d(v):
    return v.reshape(-1, v.shape[-1])


def dot(a, b):
    return jnp.dot(a, b, preferred_element_type=F32)


def kernel(x_hbm, wq_hbm, wo_hbm, wu_hbm, wd_hbm, g1_ref, c1_ref, bq_ref, bo_ref, g2_ref, c2_ref, bu_ref, bd_ref, out_hbm,
           xv, hg1, hg2, acc, qkv, ctx, ub, part, s1, r1, s2, r2, s3, r3, keep, res, ring, wo, bo_row, bd_row, bu_row,
           x_sem, o_sem, w_sem, wo_sem, a1_send, a1_recv, a2_send, a2_recv, a2_side, rs_first, rs_send, rs_recv):
    me = lax.axis_index("tp")
    core = lax.rem(me, 2)
    xbit = lax.rem(me // 2, 2)
    ybit = me // 4
    dx = 2 - 4 * xbit
    dy = 4 - 8 * ybit
    ds = 1 - 2 * core
    sis = me + ds
    n1 = me + (1 - core) * dx + core * dy
    n2 = me + (1 - core) * dy + core * dx
    dg = me + dx + dy
    c_me, c_n1, c_n2, c_dg = me // 2, n1 // 2, n2 // 2, dg // 2

    def start_qkv(t):
        for j in range(NU):
            i = t * NU + j
            for h in range(HEADS):
                pltpu.make_async_copy(wq_hbm.at[t, h, j * KC:(j + 1) * KC, :], ring.at[i, :, h * HD:(h + 1) * HD], w_sem.at[i]).start()

    def up_copy(k, n):
        slot = lax.rem(4 * k, RING) + n
        k0 = pl.multiple_of(k * KC, KC)
        return pltpu.make_async_copy(wu_hbm.at[pl.ds(k0, KC), n * NC:(n + 1) * NC], ring.at[slot], w_sem.at[slot])

    def down_copy(n, k):
        slot = lax.rem(8 + 3 * n + k, RING)
        n0 = pl.multiple_of(n * CW, CW)
        return pltpu.make_async_copy(wd_hbm.at[k * KC:(k + 1) * KC, pl.ds(n0, CW)], ring.at[slot, :, 0:CW], w_sem.at[slot])

    def start_down(first):
        for j in range(first, first + 4):
            down_copy(j // 3, j % 3).start()

    def out_copies(n):
        cols = slice(n * 3 * CW, (n + 1) * 3 * CW)
        if n < 3:
            return [pltpu.make_async_copy(wo_hbm.at[:, cols], wo.at[n], wo_sem.at[n])]
        return [pltpu.make_async_copy(wo_hbm.at[k * M:(k + 1) * M, cols], ub.at[:, k * 3 * CW:(k + 1) * 3 * CW], wo_sem.at[n + k]) for k in range(2)]

    kind = (0, 0, 2, 1, 2, 2, 2)

    def a1_copy(v, j, block, to):
        ref = hg1.at[v, block]
        return pltpu.make_async_remote_copy(src_ref=ref, dst_ref=ref, send_sem=a1_send, recv_sem=a1_recv.at[v, kind[j]],
                                            device_id={"tp": to}, device_id_type=MESH)

    def a2_copy(u, h, j, block, to):
        ref = hg2.at[u, block, pl.ds(32 * h, 32 - 16 * h), :]
        sem = a2_side.at[u] if kind[j] == 2 else a2_recv.at[u, h, kind[j]]
        return pltpu.make_async_remote_copy(src_ref=ref, dst_ref=ref, send_sem=a2_send, recv_sem=sem,
                                            device_id={"tp": to}, device_id_type=MESH)

    def wait_bytes(ref, sem):
        pltpu.make_async_remote_copy(src_ref=ref, dst_ref=ref, send_sem=sem, recv_sem=sem, device_id={"tp": me}, device_id_type=MESH).wait_recv()

    def wait_sent(ref, sem):
        pltpu.make_async_remote_copy(src_ref=ref, dst_ref=ref, send_sem=sem, recv_sem=sem, device_id={"tp": me}, device_id_type=MESH).wait_send()

    class Gather:
        def __init__(self, copy, blocks, sems):
            self.copy, self.blocks, self.sems = copy, blocks, sems

        def send(self, j):
            self.copy(j, (me, me, me, n1, n1, n2, dg)[j], (n1, n2, sis, n2, sis, sis, sis)[j]).start()

        def wait(self, k):
            wait_bytes(self.blocks((2, 1, 4)[k]), self.sems(k))

    def own(g):
        for j in (0, 1, 2):
            g.send(j)

    def forward(g):
        g.wait(0)
        for j in (3, 4, 5):
            g.send(j)

    def forward_diag(g):
        g.wait(1)
        g.send(6)

    def complete(g):
        g.wait(2)

    def a1(v):
        return Gather(lambda j, block, to: a1_copy(v, j, block, to), lambda n: hg1.at[v, 0:n], lambda k: a1_recv.at[v, k])

    def a2(u, h):
        return Gather(lambda j, block, to: a2_copy(u, h, j, block, to), lambda n: hg2.at[u, 0:n, pl.ds(32 * h, 32 - 16 * h), :],
                      lambda k: a2_recv.at[u, h, k])

    def a1_forward(v):
        with jax.named_scope("a1_forward"):
            @pl.when(v < NV)
            def _():
                forward(a1(v))

    def a1_diag(v):
        with jax.named_scope("a1_diag"):
            @pl.when(v < NV)
            def _():
                forward_diag(a1(v))

    def rs_copy(p, c, j):
        src, dst, to = ((s1, r1, sis), (s2, r2, n1), (s3, r3, n2))[j]
        return pltpu.make_async_remote_copy(src_ref=src.at[lax.rem(c, 4) if j == 0 else c], dst_ref=dst.at[c], send_sem=rs_first.at[lax.rem(c, 4)] if j == 0 else rs_send.at[j], recv_sem=rs_recv.at[c, j],
                                            device_id={"tp": to}, device_id_type=MESH)

    def rs_stage1(p, c):
        slot = lax.rem(c, 3)

        @pl.when(c >= 4)
        def _():
            rs_copy(p, c - 4, 0).wait_send()

        for q in range(4):
            s1[lax.rem(c, 4), q] = part[slot, 2 * q + 1 - core].astype(BF16)
        rs_copy(p, c, 0).start()

    def rs_stage2(p, c):
        slot = lax.rem(c, 3)
        with jax.named_scope("rs_wait1"):
            rs_copy(p, c, 0).wait_recv()

        def total(q):
            return part[slot, 2 * q + core] + r1[c, q].astype(F32)

        s2[c, 0] = total(c_n1).astype(BF16)
        s2[c, 1] = total(c_dg).astype(BF16)
        keep[lax.rem(c, 8), 0] = total(c_me)
        keep[lax.rem(c, 8), 1] = total(c_n2)
        rs_copy(p, c, 1).start()

    def rs_stage3(p, c):
        with jax.named_scope("rs_wait2"):
            rs_copy(p, c, 1).wait_recv()
        s3[c] = (keep[lax.rem(c, 8), 1] + r2[c, 1].astype(F32)).astype(BF16)
        keep[lax.rem(c, 8), 0] = keep[lax.rem(c, 8), 0] + r2[c, 0].astype(F32)
        rs_copy(p, c, 2).start()

    def rs_stage4(p, c):
        with jax.named_scope("rs_wait3"):
            rs_copy(p, c, 2).wait_recv()
        return keep[lax.rem(c, 8), 0] + r3[c].astype(F32)

    def rs_drain(p):
        wait_sent(s2, rs_send.at[1])
        wait_sent(s3, rs_send.at[2])
        for c in range(NCH - 4, NCH):
            rs_copy(p, c, 0).wait_send()

    def row_stats(xf):
        mean = jnp.mean(xf, axis=-1, keepdims=True)
        cen = xf - mean
        var = jnp.mean(cen * cen, axis=-1, keepdims=True)
        return mean, lax.rsqrt(var + LN_EPS)

    x_copy = pltpu.make_async_copy(x_hbm, xv, x_sem)
    x_copy.start()
    barrier = pltpu.get_barrier_semaphore()
    for other in (sis, n1, n2):
        pl.semaphore_signal(barrier, inc=1, device_id={"tp": other}, device_id_type=MESH)
    for dst, src in ((bo_row, bo_ref), (bd_row, bd_ref), (bu_row, bu_ref)):
        wide = src[...].astype(F32)
        for r in range(src.shape[0]):
            dst[:, r * HD:(r + 1) * HD] = wide[r:r + 1, :]
    with jax.named_scope("entry_x"):
        x_copy.wait()
    start_qkv(0)

    with jax.named_scope("ln1"):
        for b in range(B):
            mean, rstd = row_stats(xv[b].astype(F32))
            for k in range(VK):
                cols = slice(k * VW, (k + 1) * VW)
                h = (xv[b, :, cols].astype(F32) - mean) * rstd * g1_ref[:, cols] + c1_ref[:, cols]
                hg1[VK * b + k, me] = h.astype(BF16)
    with jax.named_scope("entry_barrier"):
        pl.semaphore_wait(barrier, 3)
    for v in range(VK):
        own(a1(v))
    start_qkv(1)

    causal = lax.broadcasted_iota(jnp.int32, (SEQ, SEQ), 0) >= lax.broadcasted_iota(jnp.int32, (SEQ, SEQ), 1)

    def project_piece(v):
        with jax.named_scope("qkv0"):
            for t in range(3):
                bias = bq_ref[t].astype(F32)
                for p in range(3):
                    cols = slice(t * NQ + p * NP, t * NQ + (p + 1) * NP)
                    d = sum(dot(rows2d(hg1[v, :, :, (f % 3) * 512:(f % 3 + 1) * 512]), ring[t * NU + f // 2, (f % 2) * 512:(f % 2 + 1) * 512, p * NP:(p + 1) * NP])
                            for f in range(3 * v, 3 * v + 3))
                    if v == 0:
                        acc[0:SEQ, cols] = d
                    elif v < VK - 1:
                        acc[0:SEQ, cols] += d
                    else:
                        d = acc[0:SEQ, cols] + d
                        for k in range(2):
                            h = 2 * p + k
                            qkv[:, t * NQ + h * HD:t * NQ + (h + 1) * HD] = (d[:, k * HD:(k + 1) * HD] + bias[h:h + 1, :]).astype(BF16)

    def project(s, t):
        with jax.named_scope("qkv"):
            lhs = []
            for f in range(D // 512):
                lhs.append((rows2d(hg1[VK * s + f // 3, :, :, (f % 3) * 512:(f % 3 + 1) * 512]), t * NU + f // 2, (f % 2) * 512))
            bias = bq_ref[t].astype(F32)
            for p in range(3):
                v = sum(dot(a, ring[i, r0:r0 + 512, p * NP:(p + 1) * NP]) for a, i, r0 in lhs)
                for k in range(2):
                    h = 2 * p + k
                    cols = pl.ds(pl.multiple_of(t * NQ + h * HD, HD), HD)
                    qkv[:, cols] = (v[:, k * HD:(k + 1) * HD] + bias[h:h + 1, :]).astype(BF16)

        @pl.when(s == B - 1)
        def _():
            for tt, lo, hi in ((0, 0, 4), (1, 4, 12), (2, 12, 16)):
                @pl.when(t == tt)
                def _():
                    for i in range(lo, hi):
                        up_copy(i // 4, i % 4).start()

    def attend():
        with jax.named_scope("attn"):
            def head(t, h):
                return qkv[:, t * NQ + h * HD:t * NQ + (h + 1) * HD]

            logits = [lax.dot_general(head(0, h), head(1, h), (((1,), (1,)), ((), ())), preferred_element_type=F32) for h in range(HEADS)]
            weights = []
            for x in logits:
                x = jnp.where(causal, x * HD ** -0.5, -1e30)
                e = jnp.exp(x - jnp.max(x, axis=-1, keepdims=True))
                weights.append((e * (1.0 / jnp.sum(e, axis=-1, keepdims=True))).astype(BF16))
            for h in range(HEADS):
                ctx[:, h * HD:(h + 1) * HD] = dot(weights[h], head(2, h)).astype(BF16)

    def out_product(s, n):
        @pl.when(s == 0)
        def _():
            for copy in out_copies(n):
                copy.wait()

        c = 4 * s + n
        slot = lax.rem(c, 3)
        with jax.named_scope("out"):
            for p in range(6):
                if n < 3:
                    d = dot(ctx[...], wo[n, :, p * NP:(p + 1) * NP])
                else:
                    d = sum(dot(ctx[:, k * M:(k + 1) * M], ub[:, k * 3 * CW + p * NP:k * 3 * CW + (p + 1) * NP]) for k in range(2))
                g, half = p // 2, p % 2
                part[slot, :, g * S_LOC:(g + 1) * S_LOC, half * NP:(half + 1) * NP] = d.reshape(N_DEV, S_LOC, NP)
        rs_stage1(0, c)

    def out_finish(s, n):
        total = rs_stage4(0, 4 * s + n)
        for g in range(3):
            cols = slice((3 * n + g) * CW, (3 * n + g + 1) * CW)
            res[s, :, cols] = (xv[s, :, cols].astype(F32) + (total[g * S_LOC:(g + 1) * S_LOC] + bo_row[:, cols])).astype(BF16)

    def norm2(s):
        with jax.named_scope("ln2"):
            r = pl.ds(pl.multiple_of(s * S_LOC, S_LOC), S_LOC)
            mean, rstd = row_stats(res[s].astype(F32))
            for u in range(NU):
                cols = slice(u * KC, (u + 1) * KC)
                h = (res[s, :, cols].astype(F32) - mean) * rstd * g2_ref[:, cols] + c2_ref[:, cols]
                hg2[u, me, r, :] = h.astype(BF16)

    for v in range(VK):
        with jax.named_scope("a1_forward"):
            forward(a1(v))
        if v == 0:
            start_qkv(2)
    for v in range(VK, 2 * VK):
        own(a1(v))
    forward_diag(a1(0))
    for v in range(VK):
        if v + 1 < VK:
            with jax.named_scope("a1_diag"):
                forward_diag(a1(v + 1))
        with jax.named_scope("a1_complete"):
            complete(a1(v))
        if v == 0:
            for i in range(NS):
                pltpu.make_async_copy(wu_hbm.at[0:KC, 0:NC], ring.at[i], w_sem.at[i]).wait()
            for n in range(4):
                for copy in out_copies(n):
                    copy.start()
        project_piece(v)
        if v == 1:
            forward(a1(VK))
            for k in range(2 * VK, NV):
                own(a1(k))

    def seq_body(s, _):
        b0 = 4 * s - 4

        def before(f):
            pl.when(s >= 1)(f)

        @pl.when(s >= 1)
        def _():
            with jax.named_scope("a1_complete"):
                for k in range(VK):
                    complete(a1(VK * s + k))

        def qkv_body(t, _):
            pl.when(s >= 1)(lambda: project(s, t))

            @pl.when(jnp.logical_and(s >= 1, t == 0))
            def _():
                rs_stage2(0, b0 + 3)

            @pl.when(jnp.logical_and(s >= 1, t >= 1))
            def _():
                rs_stage3(0, b0 + t - 1)
            a1_forward(VK * s + 5 + t)
            return 0
        lax.fori_loop(0, 3, qkv_body, 0)

        @pl.when(s >= 2)
        def _():
            for k in range(4):
                out_finish(s - 2, k)
            norm2(s - 2)

        attend()
        before(lambda: rs_stage3(0, b0 + 2))
        out_product(s, 0)
        before(lambda: rs_stage3(0, b0 + 3))
        out_product(s, 1)
        out_product(s, 2)
        rs_stage2(0, 4 * s)
        for k in range(2):
            a1_diag(VK * s + 4 + k)
        out_product(s, 3)
        rs_stage2(0, 4 * s + 1)
        for k in range(2, VK):
            a1_diag(VK * s + 4 + k)
        a1_forward(VK * s + 8)
        rs_stage2(0, 4 * s + 2)
        return 0
    lax.fori_loop(0, B, seq_body, 0)

    c0, last = NCH - 4, B - 1
    rs_stage2(0, c0 + 3)
    for k in range(4):
        out_finish(last - 1, k)
    rs_stage3(0, c0)
    norm2(last - 1)
    for k in range(1, 4):
        rs_stage3(0, c0 + k)
    out_finish(last, 0)
    out_finish(last, 1)
    own(a2(0, 0))
    own(a2(1, 0))
    out_finish(last, 2)
    out_finish(last, 3)
    norm2(last)
    own(a2(0, 1))
    own(a2(1, 1))
    with jax.named_scope("a2_forward"):
        for u in range(2):
            forward(a2(u, 0))
    wait_sent(hg1.at[:, 0:7], a1_send)
    rs_drain(0)

    def up_part(u, lo, hi, first=False, final=False):
        for n in range(lo, hi):
            up_copy(u, n).wait()
        with jax.named_scope("up"):
            lhs = rows2d(hg2[u])
            slot = lax.rem(4 * u, RING)
            for n in range(lo, hi):
                for p in range(3):
                    c = slice(n * NC + p * NP, n * NC + (p + 1) * NP)
                    d = dot(lhs, ring[slot + n, :, p * NP:(p + 1) * NP])
                    if first:
                        acc[:, c] = d
                    elif final:
                        ub[:, c] = jax.nn.gelu(acc[:, c] + d + bu_row[:, c], approximate=True).astype(BF16)
                    else:
                        acc[:, c] += d

    def a2_done(u):
        with jax.named_scope("a2_complete"):
            wait_bytes(hg2.at[u, 0:4], a2_side.at[u])

    def a2_forward(u, parts=(0, 1)):
        with jax.named_scope("a2_forward"):
            for h in parts:
                forward(a2(u, h))

    def a2_diag(u, parts=(0, 1)):
        with jax.named_scope("a2_diag"):
            for h in parts:
                forward_diag(a2(u, h))

    a2_forward(0, (1,))
    a2_forward(1, (1,))
    for u in (2, 3):
        for h in range(2):
            own(a2(u, h))
    a2_diag(0)
    a2_done(0)
    up_part(0, 0, 2, first=True)
    a2_forward(2)
    a2_diag(1)
    for h in range(2):
        own(a2(4, h))
    up_part(0, 2, 4, first=True)

    def up_body(u, _):
        @pl.when(u == 1)
        def _():
            for h in range(2):
                own(a2(5, h))

        a2_done(u)
        pl.when(u <= 2)(lambda: [up_copy(u + 3, n).start() for n in range(4)] and None)
        pl.when(u == 3)(lambda: start_down(0))
        pl.when(u == 4)(lambda: start_down(4))
        up_part(u, 0, 2)

        @pl.when(u + 2 < NU)
        def _():
            a2_forward(u + 2)
        a2_diag(u + 1)
        up_part(u, 2, 4)
        return 0
    lax.fori_loop(1, NU - 1, up_body, 0)

    a2_done(NU - 1)
    start_down(8)
    up_part(NU - 1, 0, 4, final=True)
    start_down(12)

    wait_sent(hg2.at[:, 0:7], a2_send)

    def down_product(n):
        for k in range(3):
            down_copy(n, k).wait()
        slot = lax.rem(n, 3)
        with jax.named_scope("down"):
            for half in range(2):
                d = sum(dot(ub[:, k * KC:(k + 1) * KC], ring[lax.rem(8 + 3 * n + k, RING), :, half * NP:(half + 1) * NP]) for k in range(3))
                part[slot, :, :, half * NP:(half + 1) * NP] = d.reshape(N_DEV, ROWS, NP)
        rs_stage1(1, n)

        @pl.when(n + 5 < NCH)
        def _():
            down_copy(n + 5, 1).start()
            down_copy(n + 5, 2).start()

        @pl.when(n + 6 < NCH)
        def _():
            down_copy(n + 6, 0).start()

    def down_body(n, _):
        @pl.when(n < NCH)
        def _():
            down_product(n)

        @pl.when(jnp.logical_and(n >= 1, n < NCH + 1))
        def _():
            rs_stage2(1, n - 1)

        @pl.when(jnp.logical_and(n >= LAG3, n < NCH + LAG3))
        def _():
            rs_stage3(1, n - LAG3)

        @pl.when(n >= LAG4)
        def _():
            m = n - LAG4
            total = rs_stage4(1, m)
            cols = pl.ds(pl.multiple_of(m * CW, CW), CW)
            v = rows2d(res[:, :, cols]).astype(F32) + (total + bd_row[:, cols])
            res[:, :, cols] = v.astype(BF16).reshape(B, S_LOC, CW)
            pltpu.make_async_copy(res.at[:, :, cols], out_hbm.at[:, :, cols], o_sem).start()
        return 0
    lax.fori_loop(0, NCH + LAG4, down_body, 0)
    with jax.named_scope("drain"):
        rs_drain(1)
        pltpu.make_async_copy(res, out_hbm, o_sem).wait()


def solution(mesh):
    def device_body(hidden, ln1_gain, ln1_bias, w_qkv, b_qkv, w_out, b_out, ln2_gain, ln2_bias, w_up, b_up, w_down, b_down):
        any_spec = pl.BlockSpec(memory_space=pl.ANY)
        vmem = pl.BlockSpec(memory_space=pltpu.VMEM)

        def row(v):
            return v.reshape(1, -1)

        def tile(v):
            return v.reshape(-1, HD)

        two = pltpu.VMEM((NCH, 2, ROWS, CW), BF16)
        four = pltpu.VMEM((NCH, 4, ROWS, CW), BF16)
        one = pltpu.VMEM((NCH, ROWS, CW), BF16)
        dma = pltpu.SemaphoreType.DMA
        return pl.pallas_call(
            kernel,
            out_shape=jax.ShapeDtypeStruct((B, S_LOC, D), BF16),
            in_specs=[any_spec] * 5 + [vmem] * 8,
            out_specs=any_spec,
            scratch_shapes=[
                pltpu.VMEM((B, S_LOC, D), BF16),
                pltpu.VMEM((NV, N_DEV, S_LOC, VW), BF16),
                pltpu.VMEM((NU, N_DEV, ROWS, KC), BF16),
                pltpu.VMEM((M, FF), F32),
                pltpu.VMEM((SEQ, 3 * NQ), BF16),
                pltpu.VMEM((SEQ, NQ), BF16),
                pltpu.VMEM((M, FF), BF16),
                pltpu.VMEM((3, N_DEV, ROWS, CW), F32),
                pltpu.VMEM((4, 4, ROWS, CW), BF16), four, two, two, one, one,
                pltpu.VMEM((8, 2, ROWS, CW), F32),
                pltpu.VMEM((B, S_LOC, D), BF16),
                pltpu.VMEM((NS, KC, NC), BF16),
                pltpu.VMEM((3, NQ, 3 * CW), BF16),
                pltpu.VMEM((1, D), F32),
                pltpu.VMEM((1, D), F32),
                pltpu.VMEM((1, FF), F32),
                dma, dma, dma((NS,)), dma((5,)),
                dma, dma((NV, 3)),
                dma, dma((NU, 2, 2)), dma((NU,)),
                dma((4,)), dma((3,)), dma((NCH, 3)),
            ],
            compiler_params=pltpu.CompilerParams(collective_id=0, has_side_effects=True, vmem_limit_bytes=67_043_328),
            name="decoder_layer",
        )(hidden, jnp.transpose(w_qkv, (1, 2, 0, 3)), w_out.reshape(HEADS * HD, D), w_up, w_down,
          row(ln1_gain), row(ln1_bias), b_qkv, tile(b_out), row(ln2_gain), row(ln2_bias), tile(b_up), tile(b_down))

    in_layout = (P("dp", "tp", None), P(), P(), P(None, None, "tp", None), P(None, "tp", None), P("tp", None, None), P(), P(), P(), P(None, "tp"), P("tp"), P("tp", None), P())
    return jax.shard_map(device_body, mesh=mesh, in_specs=in_layout, out_specs=P("dp", "tp", None), check_vma=False)
```

```python
import jax
import jax.numpy as jnp
from jax import lax
from jax.experimental import pallas as pl
from jax.experimental.pallas import tpu as pltpu
from jax.sharding import PartitionSpec as P

MESH = pl.DeviceIdType.MESH
F32 = jnp.float32
BF16 = jnp.bfloat16
LN_EPS = 1e-5

N_DEV = 8
B, S_LOC = 3, 16
ROWS = B * S_LOC
SEQ = N_DEV * S_LOC
M = N_DEV * ROWS
D = 6144
HEADS, HD = 6, 128
NQ = HEADS * HD
FF = 3072
KC = 1024
NC = 768
NP = NC // 3
NU = D // KC
UW = 512
NW = D // UW
VK = 4
VW = D // VK
NV = VK * B
LAG3, LAG4 = 4, 7
AHEAD = 4
NCH = 12
CW = 512
NS = 18
RING = 16


def rows2d(v):
    return v.reshape(-1, v.shape[-1])


def dot(a, b):
    return jnp.dot(a, b, preferred_element_type=F32)


def kernel(x_hbm, wq_hbm, wo_hbm, wu_hbm, wd_hbm, g1_ref, c1_ref, bq_ref, bo_ref, g2_ref, c2_ref, bu_ref, bd_ref, out_hbm,
           xv, hg1, hg2, acc, qkv, ctx, ub, part, s1, r1, s2, r2, s3, r3, keep, res, ring, wo, bo_row, bd_row, bu_row,
           x_sem, o_sem, w_sem, wo_sem, a1_send, a1_recv, a2_send, a2_recv, a2_side, rs_first, rs_send, rs_recv):
    me = lax.axis_index("tp")
    core = lax.rem(me, 2)
    xbit = lax.rem(me // 2, 2)
    ybit = me // 4
    dx = 2 - 4 * xbit
    dy = 4 - 8 * ybit
    ds = 1 - 2 * core
    sis = me + ds
    n1 = me + (1 - core) * dx + core * dy
    n2 = me + (1 - core) * dy + core * dx
    dg = me + dx + dy
    c_me, c_n1, c_n2, c_dg = me // 2, n1 // 2, n2 // 2, dg // 2

    def start_qkv(t):
        for j in range(NU):
            i = t * NU + j
            for h in range(HEADS):
                pltpu.make_async_copy(wq_hbm.at[t, h, j * KC:(j + 1) * KC, :], ring.at[i, :, h * HD:(h + 1) * HD], w_sem.at[i]).start()

    def up_copy(k, n):
        slot = lax.rem(4 * k, RING) + n
        k0 = pl.multiple_of(k * KC, KC)
        return pltpu.make_async_copy(wu_hbm.at[pl.ds(k0, KC), n * NC:(n + 1) * NC], ring.at[slot], w_sem.at[slot])

    def down_copy(n, k):
        slot = lax.rem(8 + 3 * n + k, RING)
        n0 = pl.multiple_of(n * CW, CW)
        return pltpu.make_async_copy(wd_hbm.at[k * KC:(k + 1) * KC, pl.ds(n0, CW)], ring.at[slot, :, 0:CW], w_sem.at[slot])

    def start_down(first):
        for j in range(first, first + 4):
            down_copy(j // 3, j % 3).start()

    def out_copies(n):
        cols = slice(n * 3 * CW, (n + 1) * 3 * CW)
        if n < 3:
            return [pltpu.make_async_copy(wo_hbm.at[:, cols], wo.at[n], wo_sem.at[n])]
        return [pltpu.make_async_copy(wo_hbm.at[k * M:(k + 1) * M, cols], ub.at[:, k * 3 * CW:(k + 1) * 3 * CW], wo_sem.at[n + k]) for k in range(2)]

    kind = (0, 0, 2, 1, 2, 2, 2)

    def a1_copy(v, j, block, to):
        ref = hg1.at[v, block]
        return pltpu.make_async_remote_copy(src_ref=ref, dst_ref=ref, send_sem=a1_send, recv_sem=a1_recv.at[v, kind[j]],
                                            device_id={"tp": to}, device_id_type=MESH)

    a2_rows = (slice(0, 2 * S_LOC), slice(2 * S_LOC, ROWS), slice(0, ROWS))

    def a2_index(u, h):
        return u + 2 if h == 2 else 2 * u + h

    def a2_copy(u, h, j, block, to):
        ref = hg2.at[u, block, a2_rows[h], :]
        sem = a2_side.at[u] if kind[j] == 2 else a2_recv.at[a2_index(u, h), kind[j]]
        return pltpu.make_async_remote_copy(src_ref=ref, dst_ref=ref, send_sem=a2_send, recv_sem=sem,
                                            device_id={"tp": to}, device_id_type=MESH)

    def wait_bytes(ref, sem):
        pltpu.make_async_remote_copy(src_ref=ref, dst_ref=ref, send_sem=sem, recv_sem=sem, device_id={"tp": me}, device_id_type=MESH).wait_recv()

    def wait_sent(ref, sem):
        pltpu.make_async_remote_copy(src_ref=ref, dst_ref=ref, send_sem=sem, recv_sem=sem, device_id={"tp": me}, device_id_type=MESH).wait_send()

    class Gather:
        def __init__(self, copy, blocks, sems):
            self.copy, self.blocks, self.sems = copy, blocks, sems

        def send(self, j):
            self.copy(j, (me, me, me, n1, n1, n2, dg)[j], (n1, n2, sis, n2, sis, sis, sis)[j]).start()

        def wait(self, k):
            wait_bytes(self.blocks((2, 1, 4)[k]), self.sems(k))

    def own(g):
        for j in (0, 1, 2):
            g.send(j)

    def forward(g):
        g.wait(0)
        for j in (3, 4, 5):
            g.send(j)

    def forward_diag(g):
        g.wait(1)
        g.send(6)

    def complete(g):
        g.wait(2)

    def a1(v):
        return Gather(lambda j, block, to: a1_copy(v, j, block, to), lambda n: hg1.at[v, 0:n], lambda k: a1_recv.at[v, k])

    def a2(u, h):
        return Gather(lambda j, block, to: a2_copy(u, h, j, block, to), lambda n: hg2.at[u, 0:n, a2_rows[h], :],
                      lambda k: a2_recv.at[a2_index(u, h), k])

    def a1_forward(v):
        with jax.named_scope("a1_forward"):
            @pl.when(v < NV)
            def _():
                forward(a1(v))

    def a1_diag(v):
        with jax.named_scope("a1_diag"):
            @pl.when(v < NV)
            def _():
                forward_diag(a1(v))

    def rs_copy(p, c, j):
        src, dst, to = ((s1, r1, sis), (s2, r2, n1), (s3, r3, n2))[j]
        return pltpu.make_async_remote_copy(src_ref=src.at[lax.rem(c, 4) if j == 0 else c], dst_ref=dst.at[c], send_sem=rs_first.at[lax.rem(c, 4)] if j == 0 else rs_send.at[j], recv_sem=rs_recv.at[c, j],
                                            device_id={"tp": to}, device_id_type=MESH)

    def rs_stage1(p, c):
        slot = lax.rem(c, 3)

        @pl.when(c >= 4)
        def _():
            rs_copy(p, c - 4, 0).wait_send()

        for q in range(4):
            s1[lax.rem(c, 4), q] = part[slot, 2 * q + 1 - core].astype(BF16)
        rs_copy(p, c, 0).start()

    def rs_stage2(p, c):
        slot = lax.rem(c, 3)
        with jax.named_scope("rs_wait1"):
            rs_copy(p, c, 0).wait_recv()

        def total(q):
            return part[slot, 2 * q + core] + r1[c, q].astype(F32)

        s2[c, 0] = total(c_n1).astype(BF16)
        s2[c, 1] = total(c_dg).astype(BF16)
        keep[lax.rem(c, 8), 0] = total(c_me)
        keep[lax.rem(c, 8), 1] = total(c_n2)
        rs_copy(p, c, 1).start()

    def rs_stage3(p, c):
        with jax.named_scope("rs_wait2"):
            rs_copy(p, c, 1).wait_recv()
        s3[c] = (keep[lax.rem(c, 8), 1] + r2[c, 1].astype(F32)).astype(BF16)
        keep[lax.rem(c, 8), 0] = keep[lax.rem(c, 8), 0] + r2[c, 0].astype(F32)
        rs_copy(p, c, 2).start()

    def rs_stage4(p, c):
        with jax.named_scope("rs_wait3"):
            rs_copy(p, c, 2).wait_recv()
        return keep[lax.rem(c, 8), 0] + r3[c].astype(F32)

    def rs_drain(p):
        wait_sent(s2, rs_send.at[1])
        wait_sent(s3, rs_send.at[2])
        for c in range(NCH - 4, NCH):
            rs_copy(p, c, 0).wait_send()

    def row_stats(xf):
        mean = jnp.mean(xf, axis=-1, keepdims=True)
        cen = xf - mean
        var = jnp.mean(cen * cen, axis=-1, keepdims=True)
        return mean, lax.rsqrt(var + LN_EPS)

    x_copy = pltpu.make_async_copy(x_hbm, xv, x_sem)
    x_copy.start()
    barrier = pltpu.get_barrier_semaphore()
    for other in (sis, n1, n2):
        pl.semaphore_signal(barrier, inc=1, device_id={"tp": other}, device_id_type=MESH)
    for dst, src in ((bo_row, bo_ref), (bd_row, bd_ref), (bu_row, bu_ref)):
        wide = src[...].astype(F32)
        for r in range(src.shape[0]):
            dst[:, r * HD:(r + 1) * HD] = wide[r:r + 1, :]
    with jax.named_scope("entry_x"):
        x_copy.wait()
    start_qkv(0)

    with jax.named_scope("ln1"):
        for b in range(B):
            mean, rstd = row_stats(xv[b].astype(F32))
            for k in range(VK):
                cols = slice(k * VW, (k + 1) * VW)
                h = (xv[b, :, cols].astype(F32) - mean) * rstd * g1_ref[:, cols] + c1_ref[:, cols]
                hg1[VK * b + k, me] = h.astype(BF16)
    with jax.named_scope("entry_barrier"):
        pl.semaphore_wait(barrier, 3)
    for v in range(VK):
        own(a1(v))
    start_qkv(1)

    causal = lax.broadcasted_iota(jnp.int32, (SEQ, SEQ), 0) >= lax.broadcasted_iota(jnp.int32, (SEQ, SEQ), 1)

    def project_piece(v):
        with jax.named_scope("qkv0"):
            for t in range(3):
                bias = bq_ref[t].astype(F32)
                for p in range(3):
                    cols = slice(t * NQ + p * NP, t * NQ + (p + 1) * NP)
                    d = sum(dot(rows2d(hg1[v, :, :, (f % 3) * 512:(f % 3 + 1) * 512]), ring[t * NU + f // 2, (f % 2) * 512:(f % 2 + 1) * 512, p * NP:(p + 1) * NP])
                            for f in range(3 * v, 3 * v + 3))
                    if v == 0:
                        acc[0:SEQ, cols] = d
                    elif v < VK - 1:
                        acc[0:SEQ, cols] += d
                    else:
                        d = acc[0:SEQ, cols] + d
                        for k in range(2):
                            h = 2 * p + k
                            qkv[:, t * NQ + h * HD:t * NQ + (h + 1) * HD] = (d[:, k * HD:(k + 1) * HD] + bias[h:h + 1, :]).astype(BF16)

    def project(s, t):
        with jax.named_scope("qkv"):
            lhs = []
            for f in range(D // 512):
                lhs.append((rows2d(hg1[VK * s + f // 3, :, :, (f % 3) * 512:(f % 3 + 1) * 512]), t * NU + f // 2, (f % 2) * 512))
            bias = bq_ref[t].astype(F32)
            for p in range(3):
                v = sum(dot(a, ring[i, r0:r0 + 512, p * NP:(p + 1) * NP]) for a, i, r0 in lhs)
                for k in range(2):
                    h = 2 * p + k
                    cols = pl.ds(pl.multiple_of(t * NQ + h * HD, HD), HD)
                    qkv[:, cols] = (v[:, k * HD:(k + 1) * HD] + bias[h:h + 1, :]).astype(BF16)

        @pl.when(s == B - 1)
        def _():
            for tt, lo, hi in ((0, 0, 4), (1, 4, 12), (2, 12, 16)):
                @pl.when(t == tt)
                def _():
                    for i in range(lo, hi):
                        up_copy(i // 4, i % 4).start()

    def attend():
        with jax.named_scope("attn"):
            def head(t, h):
                return qkv[:, t * NQ + h * HD:t * NQ + (h + 1) * HD]

            logits = [lax.dot_general(head(0, h), head(1, h), (((1,), (1,)), ((), ())), preferred_element_type=F32) for h in range(HEADS)]
            weights = []
            for x in logits:
                x = jnp.where(causal, x * HD ** -0.5, -1e30)
                e = jnp.exp(x - jnp.max(x, axis=-1, keepdims=True))
                weights.append((e * (1.0 / jnp.sum(e, axis=-1, keepdims=True))).astype(BF16))
            for h in range(HEADS):
                ctx[:, h * HD:(h + 1) * HD] = dot(weights[h], head(2, h)).astype(BF16)

    def out_product(s, n):
        @pl.when(s == 0)
        def _():
            for copy in out_copies(n):
                copy.wait()

        c = 4 * s + n
        slot = lax.rem(c, 3)
        with jax.named_scope("out"):
            for p in range(6):
                if n < 3:
                    d = dot(ctx[...], wo[n, :, p * NP:(p + 1) * NP])
                else:
                    d = sum(dot(ctx[:, k * M:(k + 1) * M], ub[:, k * 3 * CW + p * NP:k * 3 * CW + (p + 1) * NP]) for k in range(2))
                g, half = p // 2, p % 2
                part[slot, :, g * S_LOC:(g + 1) * S_LOC, half * NP:(half + 1) * NP] = d.reshape(N_DEV, S_LOC, NP)
        rs_stage1(0, c)

    def out_finish(s, n):
        total = rs_stage4(0, 4 * s + n)
        for g in range(3):
            cols = slice((3 * n + g) * CW, (3 * n + g + 1) * CW)
            res[s, :, cols] = (xv[s, :, cols].astype(F32) + (total[g * S_LOC:(g + 1) * S_LOC] + bo_row[:, cols])).astype(BF16)

    def norm2(s):
        with jax.named_scope("ln2"):
            r = pl.ds(pl.multiple_of(s * S_LOC, S_LOC), S_LOC)
            mean, rstd = row_stats(res[s].astype(F32))
            for u in range(NW):
                cols = slice(u * UW, (u + 1) * UW)
                h = (res[s, :, cols].astype(F32) - mean) * rstd * g2_ref[:, cols] + c2_ref[:, cols]
                hg2[u, me, r, :] = h.astype(BF16)

    for v in range(VK):
        with jax.named_scope("a1_forward"):
            forward(a1(v))
        if v == 0:
            start_qkv(2)
    for v in range(VK, 2 * VK):
        own(a1(v))
    forward_diag(a1(0))
    for v in range(VK):
        if v + 1 < VK:
            with jax.named_scope("a1_diag"):
                forward_diag(a1(v + 1))
        with jax.named_scope("a1_complete"):
            complete(a1(v))
        if v == 0:
            for i in range(NS):
                pltpu.make_async_copy(wu_hbm.at[0:KC, 0:NC], ring.at[i], w_sem.at[i]).wait()
            for n in range(4):
                for copy in out_copies(n):
                    copy.start()
        project_piece(v)
        if v == 1:
            forward(a1(VK))
            for k in range(2 * VK, NV):
                own(a1(k))

    def seq_body(s, _):
        b0 = 4 * s - 4

        def before(f):
            pl.when(s >= 1)(f)

        @pl.when(s >= 1)
        def _():
            with jax.named_scope("a1_complete"):
                for k in range(VK):
                    complete(a1(VK * s + k))

        def qkv_body(t, _):
            pl.when(s >= 1)(lambda: project(s, t))

            @pl.when(jnp.logical_and(s >= 1, t == 0))
            def _():
                rs_stage2(0, b0 + 3)

            @pl.when(jnp.logical_and(s >= 1, t >= 1))
            def _():
                rs_stage3(0, b0 + t - 1)
            a1_forward(VK * s + 5 + t)
            return 0
        lax.fori_loop(0, 3, qkv_body, 0)

        @pl.when(s >= 2)
        def _():
            for k in range(4):
                out_finish(s - 2, k)
            norm2(s - 2)

        attend()
        before(lambda: rs_stage3(0, b0 + 2))
        out_product(s, 0)
        before(lambda: rs_stage3(0, b0 + 3))
        out_product(s, 1)
        out_product(s, 2)
        rs_stage2(0, 4 * s)
        for k in range(2):
            a1_diag(VK * s + 4 + k)
        out_product(s, 3)
        rs_stage2(0, 4 * s + 1)
        for k in range(2, VK):
            a1_diag(VK * s + 4 + k)
        a1_forward(VK * s + 8)
        rs_stage2(0, 4 * s + 2)
        return 0
    lax.fori_loop(0, B, seq_body, 0)

    c0, last = NCH - 4, B - 1
    rs_stage2(0, c0 + 3)
    for k in range(4):
        out_finish(last - 1, k)
    rs_stage3(0, c0)
    norm2(last - 1)
    for k in range(1, 4):
        rs_stage3(0, c0 + k)
    out_finish(last, 0)
    out_finish(last, 1)
    own(a2(0, 0))
    own(a2(1, 0))
    out_finish(last, 2)
    out_finish(last, 3)
    norm2(last)
    own(a2(0, 1))
    own(a2(1, 1))
    own(a2(2, 2))
    with jax.named_scope("a2_forward"):
        forward(a2(0, 0))
        forward(a2(0, 1))
        forward(a2(1, 0))
        forward(a2(1, 1))
    for u in (3, 4, 5):
        own(a2(u, 2))
    wait_sent(hg1.at[:, 0:7], a1_send)
    rs_drain(0)

    def up_chunk(w, first=False, final=False):
        with jax.named_scope("up"):
            lhs = rows2d(hg2[w])
            slot = lax.rem(4 * (w // 2), RING)
            rows = pl.ds(pl.multiple_of(lax.rem(w, 2) * UW, UW), UW)
            for n in range(4):
                for p in range(3):
                    c = slice(n * NC + p * NP, n * NC + (p + 1) * NP)
                    d = dot(lhs, ring[slot + n, rows, p * NP:(p + 1) * NP])
                    if first:
                        acc[:, c] = d
                    elif final:
                        ub[:, c] = jax.nn.gelu(acc[:, c] + d + bu_row[:, c], approximate=True).astype(BF16)
                    else:
                        acc[:, c] += d

    def a2_done(w):
        with jax.named_scope("a2_complete"):
            wait_bytes(hg2.at[w, 0:4], a2_side.at[w])

    def a2_forward(w):
        with jax.named_scope("a2_forward"):
            forward(a2(w, 2))

    def a2_diag(w, parts=(2,)):
        with jax.named_scope("a2_diag"):
            for h in parts:
                forward_diag(a2(w, h))

    for n in range(4):
        up_copy(0, n).wait()
    a2_diag(0, (0, 1))
    a2_forward(2)
    own(a2(6, 2))
    a2_diag(1, (0, 1))
    a2_done(0)
    up_chunk(0, first=True)
    a2_forward(3)
    own(a2(7, 2))
    a2_diag(2)
    a2_forward(4)
    own(a2(8, 2))
    a2_done(1)
    up_chunk(1)

    def up_step(w):
        @pl.when(w + 3 < NW)
        def _():
            a2_forward(w + 3)

        @pl.when(w + 7 < NW)
        def _():
            own(a2(w + 7, 2))

        a2_diag(w + 1)
        a2_done(w)
        k = w // 2

        @pl.when(lax.rem(w, 2) == 0)
        def _():
            for n in range(4):
                up_copy(k, n).wait()

            @pl.when(w <= 4)
            def _():
                for n in range(4):
                    up_copy(k + 3, n).start()
            pl.when(w == 6)(lambda: start_down(0))
            pl.when(w == 8)(lambda: start_down(4))
            pl.when(w == 10)(lambda: start_down(8))
        up_chunk(w)
        return 0

    lax.fori_loop(2, NW - 1, lambda w, c: up_step(w), 0)
    a2_done(NW - 1)
    up_chunk(NW - 1, final=True)
    start_down(12)

    wait_sent(hg2.at[:, 0:7], a2_send)

    def down_product(n):
        for k in range(3):
            down_copy(n, k).wait()
        slot = lax.rem(n, 3)
        with jax.named_scope("down"):
            for half in range(2):
                d = sum(dot(ub[:, k * KC:(k + 1) * KC], ring[lax.rem(8 + 3 * n + k, RING), :, half * NP:(half + 1) * NP]) for k in range(3))
                part[slot, :, :, half * NP:(half + 1) * NP] = d.reshape(N_DEV, ROWS, NP)
        rs_stage1(1, n)

        @pl.when(n + 5 < NCH)
        def _():
            down_copy(n + 5, 1).start()
            down_copy(n + 5, 2).start()

        @pl.when(n + 6 < NCH)
        def _():
            down_copy(n + 6, 0).start()

    def down_body(n, _):
        @pl.when(n < NCH)
        def _():
            down_product(n)

        @pl.when(jnp.logical_and(n >= 1, n < NCH + 1))
        def _():
            rs_stage2(1, n - 1)

        @pl.when(jnp.logical_and(n >= LAG3, n < NCH + LAG3))
        def _():
            rs_stage3(1, n - LAG3)

        @pl.when(n >= LAG4)
        def _():
            m = n - LAG4
            total = rs_stage4(1, m)
            cols = pl.ds(pl.multiple_of(m * CW, CW), CW)
            v = rows2d(res[:, :, cols]).astype(F32) + (total + bd_row[:, cols])
            res[:, :, cols] = v.astype(BF16).reshape(B, S_LOC, CW)
            pltpu.make_async_copy(res.at[:, :, cols], out_hbm.at[:, :, cols], o_sem).start()
        return 0
    lax.fori_loop(0, NCH + LAG4, down_body, 0)
    with jax.named_scope("drain"):
        rs_drain(1)
        pltpu.make_async_copy(res, out_hbm, o_sem).wait()


def solution(mesh):
    def device_body(hidden, ln1_gain, ln1_bias, w_qkv, b_qkv, w_out, b_out, ln2_gain, ln2_bias, w_up, b_up, w_down, b_down):
        any_spec = pl.BlockSpec(memory_space=pl.ANY)
        vmem = pl.BlockSpec(memory_space=pltpu.VMEM)

        def row(v):
            return v.reshape(1, -1)

        def tile(v):
            return v.reshape(-1, HD)

        two = pltpu.VMEM((NCH, 2, ROWS, CW), BF16)
        four = pltpu.VMEM((NCH, 4, ROWS, CW), BF16)
        one = pltpu.VMEM((NCH, ROWS, CW), BF16)
        dma = pltpu.SemaphoreType.DMA
        return pl.pallas_call(
            kernel,
            out_shape=jax.ShapeDtypeStruct((B, S_LOC, D), BF16),
            in_specs=[any_spec] * 5 + [vmem] * 8,
            out_specs=any_spec,
            scratch_shapes=[
                pltpu.VMEM((B, S_LOC, D), BF16),
                pltpu.VMEM((NV, N_DEV, S_LOC, VW), BF16),
                pltpu.VMEM((NW, N_DEV, ROWS, UW), BF16),
                pltpu.VMEM((M, FF), F32),
                pltpu.VMEM((SEQ, 3 * NQ), BF16),
                pltpu.VMEM((SEQ, NQ), BF16),
                pltpu.VMEM((M, FF), BF16),
                pltpu.VMEM((3, N_DEV, ROWS, CW), F32),
                pltpu.VMEM((4, 4, ROWS, CW), BF16), four, two, two, one, one,
                pltpu.VMEM((8, 2, ROWS, CW), F32),
                pltpu.VMEM((B, S_LOC, D), BF16),
                pltpu.VMEM((NS, KC, NC), BF16),
                pltpu.VMEM((3, NQ, 3 * CW), BF16),
                pltpu.VMEM((1, D), F32),
                pltpu.VMEM((1, D), F32),
                pltpu.VMEM((1, FF), F32),
                dma, dma, dma((NS,)), dma((5,)),
                dma, dma((NV, 3)),
                dma, dma((NW + 2, 2)), dma((NW,)),
                dma((4,)), dma((3,)), dma((NCH, 3)),
            ],
            compiler_params=pltpu.CompilerParams(collective_id=0, has_side_effects=True, vmem_limit_bytes=67_043_328),
            name="decoder_layer",
        )(hidden, jnp.transpose(w_qkv, (1, 2, 0, 3)), w_out.reshape(HEADS * HD, D), w_up, w_down,
          row(ln1_gain), row(ln1_bias), b_qkv, tile(b_out), row(ln2_gain), row(ln2_bias), tile(b_up), tile(b_down))

    in_layout = (P("dp", "tp", None), P(), P(), P(None, None, "tp", None), P(None, "tp", None), P("tp", None, None), P(), P(), P(), P(None, "tp"), P("tp"), P("tp", None), P())
    return jax.shard_map(device_body, mesh=mesh, in_specs=in_layout, out_specs=P("dp", "tp", None), check_vma=False)
```

```python
import jax
import jax.numpy as jnp
from jax import lax
from jax.experimental import pallas as pl
from jax.experimental.pallas import tpu as pltpu
from jax.sharding import PartitionSpec as P

MESH = pl.DeviceIdType.MESH
F32 = jnp.float32
BF16 = jnp.bfloat16
LN_EPS = 1e-5

N_DEV = 8
B, S_LOC = 3, 16
ROWS = B * S_LOC
SEQ = N_DEV * S_LOC
M = N_DEV * ROWS
D = 6144
HEADS, HD = 6, 128
NQ = HEADS * HD
FF = 3072
KC = 1024
NC = 768
NP = NC // 3
NU = D // KC
UW = 512
NW = D // UW
VK = 4
VW = D // VK
NV = VK * B
LAG3, LAG4 = 4, 7
AHEAD = 4
NCH = 12
CW = 512
NS = 18
RING = 16


def rows2d(v):
    return v.reshape(-1, v.shape[-1])


def dot(a, b):
    return jnp.dot(a, b, preferred_element_type=F32)


def kernel(x_hbm, wq_hbm, wo_hbm, wu_hbm, wd_hbm, g1_ref, c1_ref, bq_ref, bo_ref, g2_ref, c2_ref, bu_ref, bd_ref, out_hbm,
           xv, hg1, hg2, acc, qkv, ctx, ub, part, s1, r1, s2, r2, s3, r3, keep, res, ring, wo, bo_row, bd_row, bu_row,
           x_sem, o_sem, w_sem, wo_sem, a1_send, a1_recv, a2_send, a2_recv, a2_side, rs_first, rs_send, rs_recv):
    me = lax.axis_index("tp")
    core = lax.rem(me, 2)
    xbit = lax.rem(me // 2, 2)
    ybit = me // 4
    dx = 2 - 4 * xbit
    dy = 4 - 8 * ybit
    ds = 1 - 2 * core
    sis = me + ds
    n1 = me + (1 - core) * dx + core * dy
    n2 = me + (1 - core) * dy + core * dx
    dg = me + dx + dy
    c_me, c_n1, c_n2, c_dg = me // 2, n1 // 2, n2 // 2, dg // 2

    def start_qkv(t):
        for j in range(NU):
            i = t * NU + j
            for h in range(HEADS):
                pltpu.make_async_copy(wq_hbm.at[t, h, j * KC:(j + 1) * KC, :], ring.at[i, :, h * HD:(h + 1) * HD], w_sem.at[i]).start()

    def up_copy(k, n):
        slot = lax.rem(4 * k, RING) + n
        k0 = pl.multiple_of(k * KC, KC)
        return pltpu.make_async_copy(wu_hbm.at[pl.ds(k0, KC), n * NC:(n + 1) * NC], ring.at[slot], w_sem.at[slot])

    def down_copy(n, k):
        slot = lax.rem(8 + 3 * n + k, RING)
        n0 = pl.multiple_of(n * CW, CW)
        return pltpu.make_async_copy(wd_hbm.at[k * KC:(k + 1) * KC, pl.ds(n0, CW)], ring.at[slot, :, 0:CW], w_sem.at[slot])

    def start_down(first):
        for j in range(first, first + 4):
            down_copy(j // 3, j % 3).start()

    def out_copies(n):
        cols = slice(n * 3 * CW, (n + 1) * 3 * CW)
        if n < 3:
            return [pltpu.make_async_copy(wo_hbm.at[:, cols], wo.at[n], wo_sem.at[n])]
        return [pltpu.make_async_copy(wo_hbm.at[k * M:(k + 1) * M, cols], ub.at[:, k * 3 * CW:(k + 1) * 3 * CW], wo_sem.at[n + k]) for k in range(2)]

    kind = (0, 0, 2, 1, 2, 2, 2)

    def a1_copy(v, j, block, to):
        ref = hg1.at[v, block]
        return pltpu.make_async_remote_copy(src_ref=ref, dst_ref=ref, send_sem=a1_send, recv_sem=a1_recv.at[v, kind[j]],
                                            device_id={"tp": to}, device_id_type=MESH)

    a2_rows = (slice(0, 2 * S_LOC), slice(2 * S_LOC, ROWS), slice(0, ROWS))

    def a2_index(u, h):
        return u + 2 if h == 2 else 2 * u + h

    def a2_copy(u, h, j, block, to):
        ref = hg2.at[u, block, a2_rows[h], :]
        sem = a2_side.at[u] if kind[j] == 2 else a2_recv.at[a2_index(u, h), kind[j]]
        return pltpu.make_async_remote_copy(src_ref=ref, dst_ref=ref, send_sem=a2_send, recv_sem=sem,
                                            device_id={"tp": to}, device_id_type=MESH)

    def wait_bytes(ref, sem):
        pltpu.make_async_remote_copy(src_ref=ref, dst_ref=ref, send_sem=sem, recv_sem=sem, device_id={"tp": me}, device_id_type=MESH).wait_recv()

    def wait_sent(ref, sem):
        pltpu.make_async_remote_copy(src_ref=ref, dst_ref=ref, send_sem=sem, recv_sem=sem, device_id={"tp": me}, device_id_type=MESH).wait_send()

    class Gather:
        def __init__(self, copy, blocks, sems):
            self.copy, self.blocks, self.sems = copy, blocks, sems

        def send(self, j):
            self.copy(j, (me, me, me, n1, n1, n2, dg)[j], (n1, n2, sis, n2, sis, sis, sis)[j]).start()

        def wait(self, k):
            wait_bytes(self.blocks((2, 1, 4)[k]), self.sems(k))

    def own(g):
        for j in (0, 1, 2):
            g.send(j)

    def forward(g):
        g.wait(0)
        for j in (3, 4, 5):
            g.send(j)

    def forward_diag(g):
        g.wait(1)
        g.send(6)

    def complete(g):
        g.wait(2)

    def a1(v):
        return Gather(lambda j, block, to: a1_copy(v, j, block, to), lambda n: hg1.at[v, 0:n], lambda k: a1_recv.at[v, k])

    def a2(u, h):
        return Gather(lambda j, block, to: a2_copy(u, h, j, block, to), lambda n: hg2.at[u, 0:n, a2_rows[h], :],
                      lambda k: a2_recv.at[a2_index(u, h), k])

    def a1_forward(v):
        with jax.named_scope("a1_forward"):
            @pl.when(v < NV)
            def _():
                forward(a1(v))

    def a1_diag(v):
        with jax.named_scope("a1_diag"):
            @pl.when(v < NV)
            def _():
                forward_diag(a1(v))

    def rs_copy(p, c, j):
        src, dst, to = ((s1, r1, sis), (s2, r2, n1), (s3, r3, n2))[j]
        return pltpu.make_async_remote_copy(src_ref=src.at[lax.rem(c, 4) if j == 0 else c], dst_ref=dst.at[c], send_sem=rs_first.at[lax.rem(c, 4)] if j == 0 else rs_send.at[j], recv_sem=rs_recv.at[c, j],
                                            device_id={"tp": to}, device_id_type=MESH)

    def rs_stage1(p, c):
        slot = lax.rem(c, 3)

        @pl.when(c >= 4)
        def _():
            rs_copy(p, c - 4, 0).wait_send()

        for q in range(4):
            s1[lax.rem(c, 4), q] = part[slot, 2 * q + 1 - core].astype(BF16)
        rs_copy(p, c, 0).start()

    def rs_stage2(p, c):
        slot = lax.rem(c, 3)
        with jax.named_scope("rs_wait1"):
            rs_copy(p, c, 0).wait_recv()

        def total(q):
            return part[slot, 2 * q + core] + r1[c, q].astype(F32)

        s2[c, 0] = total(c_n1).astype(BF16)
        s2[c, 1] = total(c_dg).astype(BF16)
        keep[lax.rem(c, 8), 0] = total(c_me)
        keep[lax.rem(c, 8), 1] = total(c_n2)
        rs_copy(p, c, 1).start()

    def rs_stage3(p, c):
        with jax.named_scope("rs_wait2"):
            rs_copy(p, c, 1).wait_recv()
        s3[c] = (keep[lax.rem(c, 8), 1] + r2[c, 1].astype(F32)).astype(BF16)
        keep[lax.rem(c, 8), 0] = keep[lax.rem(c, 8), 0] + r2[c, 0].astype(F32)
        rs_copy(p, c, 2).start()

    def rs_stage4(p, c):
        with jax.named_scope("rs_wait3"):
            rs_copy(p, c, 2).wait_recv()
        return keep[lax.rem(c, 8), 0] + r3[c].astype(F32)

    def rs_drain(p):
        wait_sent(s2, rs_send.at[1])
        wait_sent(s3, rs_send.at[2])
        for c in range(NCH - 4, NCH):
            rs_copy(p, c, 0).wait_send()

    def row_stats(xf):
        mean = jnp.mean(xf, axis=-1, keepdims=True)
        cen = xf - mean
        var = jnp.mean(cen * cen, axis=-1, keepdims=True)
        return mean, lax.rsqrt(var + LN_EPS)

    x_copy = pltpu.make_async_copy(x_hbm, xv, x_sem)
    x_copy.start()
    barrier = pltpu.get_barrier_semaphore()
    for other in (sis, n1, n2):
        pl.semaphore_signal(barrier, inc=1, device_id={"tp": other}, device_id_type=MESH)
    for dst, src in ((bo_row, bo_ref), (bd_row, bd_ref), (bu_row, bu_ref)):
        wide = src[...].astype(F32)
        for r in range(src.shape[0]):
            dst[:, r * HD:(r + 1) * HD] = wide[r:r + 1, :]
    with jax.named_scope("entry_x"):
        x_copy.wait()
    start_qkv(0)

    with jax.named_scope("ln1"):
        for b in range(B):
            mean, rstd = row_stats(xv[b].astype(F32))
            for k in range(VK):
                cols = slice(k * VW, (k + 1) * VW)
                h = (xv[b, :, cols].astype(F32) - mean) * rstd * g1_ref[:, cols] + c1_ref[:, cols]
                hg1[VK * b + k, me] = h.astype(BF16)
    with jax.named_scope("entry_barrier"):
        pl.semaphore_wait(barrier, 3)
    own(a1(0))
    own(a1(1))
    start_qkv(1)

    causal = lax.broadcasted_iota(jnp.int32, (SEQ, SEQ), 0) >= lax.broadcasted_iota(jnp.int32, (SEQ, SEQ), 1)

    def project_piece(v):
        with jax.named_scope("qkv0"):
            for t in range(3):
                bias = bq_ref[t].astype(F32)
                for p in range(3):
                    cols = slice(t * NQ + p * NP, t * NQ + (p + 1) * NP)
                    d = sum(dot(rows2d(hg1[v, :, :, (f % 3) * 512:(f % 3 + 1) * 512]), ring[t * NU + f // 2, (f % 2) * 512:(f % 2 + 1) * 512, p * NP:(p + 1) * NP])
                            for f in range(3 * v, 3 * v + 3))
                    if v == 0:
                        acc[0:SEQ, cols] = d
                    elif v < VK - 1:
                        acc[0:SEQ, cols] += d
                    else:
                        d = acc[0:SEQ, cols] + d
                        for k in range(2):
                            h = 2 * p + k
                            qkv[:, t * NQ + h * HD:t * NQ + (h + 1) * HD] = (d[:, k * HD:(k + 1) * HD] + bias[h:h + 1, :]).astype(BF16)

    def project(s, t):
        with jax.named_scope("qkv"):
            lhs = []
            for f in range(D // 512):
                lhs.append((rows2d(hg1[VK * s + f // 3, :, :, (f % 3) * 512:(f % 3 + 1) * 512]), t * NU + f // 2, (f % 2) * 512))
            bias = bq_ref[t].astype(F32)
            for p in range(3):
                v = sum(dot(a, ring[i, r0:r0 + 512, p * NP:(p + 1) * NP]) for a, i, r0 in lhs)
                for k in range(2):
                    h = 2 * p + k
                    cols = pl.ds(pl.multiple_of(t * NQ + h * HD, HD), HD)
                    qkv[:, cols] = (v[:, k * HD:(k + 1) * HD] + bias[h:h + 1, :]).astype(BF16)

        @pl.when(s == B - 1)
        def _():
            for tt, lo, hi in ((0, 0, 4), (1, 4, 12), (2, 12, 16)):
                @pl.when(t == tt)
                def _():
                    for i in range(lo, hi):
                        up_copy(i // 4, i % 4).start()

    def attend():
        with jax.named_scope("attn"):
            def head(t, h):
                return qkv[:, t * NQ + h * HD:t * NQ + (h + 1) * HD]

            logits = [lax.dot_general(head(0, h), head(1, h), (((1,), (1,)), ((), ())), preferred_element_type=F32) for h in range(HEADS)]
            weights = []
            for x in logits:
                x = jnp.where(causal, x * HD ** -0.5, -1e30)
                e = jnp.exp(x - jnp.max(x, axis=-1, keepdims=True))
                weights.append((e * (1.0 / jnp.sum(e, axis=-1, keepdims=True))).astype(BF16))
            for h in range(HEADS):
                ctx[:, h * HD:(h + 1) * HD] = dot(weights[h], head(2, h)).astype(BF16)

    def out_product(s, n):
        @pl.when(s == 0)
        def _():
            for copy in out_copies(n):
                copy.wait()

        c = 4 * s + n
        slot = lax.rem(c, 3)
        with jax.named_scope("out"):
            for p in range(6):
                if n < 3:
                    d = dot(ctx[...], wo[n, :, p * NP:(p + 1) * NP])
                else:
                    d = sum(dot(ctx[:, k * M:(k + 1) * M], ub[:, k * 3 * CW + p * NP:k * 3 * CW + (p + 1) * NP]) for k in range(2))
                g, half = p // 2, p % 2
                part[slot, :, g * S_LOC:(g + 1) * S_LOC, half * NP:(half + 1) * NP] = d.reshape(N_DEV, S_LOC, NP)
        rs_stage1(0, c)

    def out_finish(s, n):
        total = rs_stage4(0, 4 * s + n)
        for g in range(3):
            cols = slice((3 * n + g) * CW, (3 * n + g + 1) * CW)
            res[s, :, cols] = (xv[s, :, cols].astype(F32) + (total[g * S_LOC:(g + 1) * S_LOC] + bo_row[:, cols])).astype(BF16)

    def norm2(s):
        with jax.named_scope("ln2"):
            r = pl.ds(pl.multiple_of(s * S_LOC, S_LOC), S_LOC)
            mean, rstd = row_stats(res[s].astype(F32))
            for u in range(NW):
                cols = slice(u * UW, (u + 1) * UW)
                h = (res[s, :, cols].astype(F32) - mean) * rstd * g2_ref[:, cols] + c2_ref[:, cols]
                hg2[u, me, r, :] = h.astype(BF16)

    with jax.named_scope("a1_forward"):
        forward(a1(0))
    own(a1(2))
    start_qkv(2)
    with jax.named_scope("a1_forward"):
        forward(a1(1))
    own(a1(3))
    with jax.named_scope("a1_diag"):
        forward_diag(a1(0))
    with jax.named_scope("a1_forward"):
        forward(a1(2))
        forward(a1(3))
    for v in range(VK, 2 * VK):
        own(a1(v))
    for v in range(VK):
        if v + 1 < VK:
            with jax.named_scope("a1_diag"):
                forward_diag(a1(v + 1))
        with jax.named_scope("a1_complete"):
            complete(a1(v))
        if v == 0:
            for i in range(NS):
                pltpu.make_async_copy(wu_hbm.at[0:KC, 0:NC], ring.at[i], w_sem.at[i]).wait()
            for n in range(4):
                for copy in out_copies(n):
                    copy.start()
        project_piece(v)
        if v == 1:
            forward(a1(VK))
            for k in range(2 * VK, NV):
                own(a1(k))

    def seq_body(s, _):
        b0 = 4 * s - 4

        def before(f):
            pl.when(s >= 1)(f)

        @pl.when(s >= 1)
        def _():
            with jax.named_scope("a1_complete"):
                for k in range(VK):
                    complete(a1(VK * s + k))

        def qkv_body(t, _):
            pl.when(s >= 1)(lambda: project(s, t))

            @pl.when(jnp.logical_and(s >= 1, t == 0))
            def _():
                rs_stage2(0, b0 + 3)

            @pl.when(jnp.logical_and(s >= 1, t >= 1))
            def _():
                rs_stage3(0, b0 + t - 1)
            a1_forward(VK * s + 5 + t)
            return 0
        lax.fori_loop(0, 3, qkv_body, 0)

        @pl.when(s >= 2)
        def _():
            for k in range(4):
                out_finish(s - 2, k)
            norm2(s - 2)

        attend()
        before(lambda: rs_stage3(0, b0 + 2))
        out_product(s, 0)
        before(lambda: rs_stage3(0, b0 + 3))
        out_product(s, 1)
        out_product(s, 2)
        rs_stage2(0, 4 * s)
        for k in range(2):
            a1_diag(VK * s + 4 + k)
        out_product(s, 3)
        rs_stage2(0, 4 * s + 1)
        for k in range(2, VK):
            a1_diag(VK * s + 4 + k)
        a1_forward(VK * s + 8)
        rs_stage2(0, 4 * s + 2)
        return 0
    lax.fori_loop(0, B, seq_body, 0)

    c0, last = NCH - 4, B - 1
    rs_stage2(0, c0 + 3)
    for k in range(4):
        out_finish(last - 1, k)
    rs_stage3(0, c0)
    norm2(last - 1)
    for k in range(1, 4):
        rs_stage3(0, c0 + k)
    out_finish(last, 0)
    out_finish(last, 1)
    own(a2(0, 0))
    out_finish(last, 2)
    out_finish(last, 3)
    norm2(last)
    own(a2(0, 1))
    own(a2(1, 0))
    own(a2(1, 1))
    with jax.named_scope("a2_forward"):
        forward(a2(0, 0))
        forward(a2(0, 1))
    own(a2(2, 2))
    with jax.named_scope("a2_forward"):
        forward(a2(1, 0))
        forward(a2(1, 1))
    wait_sent(hg1.at[:, 0:7], a1_send)
    rs_drain(0)

    def up_chunk(w, first=False, final=False):
        with jax.named_scope("up"):
            lhs = rows2d(hg2[w])
            slot = lax.rem(4 * (w // 2), RING)
            rows = pl.ds(pl.multiple_of(lax.rem(w, 2) * UW, UW), UW)
            for n in range(4):
                for p in range(3):
                    c = slice(n * NC + p * NP, n * NC + (p + 1) * NP)
                    d = dot(lhs, ring[slot + n, rows, p * NP:(p + 1) * NP])
                    if first:
                        acc[:, c] = d
                    elif final:
                        ub[:, c] = jax.nn.gelu(acc[:, c] + d + bu_row[:, c], approximate=True).astype(BF16)
                    else:
                        acc[:, c] += d

    def a2_done(w):
        with jax.named_scope("a2_complete"):
            wait_bytes(hg2.at[w, 0:4], a2_side.at[w])

    def a2_forward(w):
        with jax.named_scope("a2_forward"):
            forward(a2(w, 2))

    def a2_diag(w, parts=(2,)):
        with jax.named_scope("a2_diag"):
            for h in parts:
                forward_diag(a2(w, h))

    for n in range(4):
        up_copy(0, n).wait()
    a2_diag(0, (0, 1))
    own(a2(3, 2))
    a2_diag(1, (0, 1))
    own(a2(4, 2))
    a2_done(0)
    own(a2(5, 2))
    up_chunk(0, first=True)
    a2_forward(2)
    own(a2(6, 2))
    a2_forward(3)
    own(a2(7, 2))
    a2_diag(2)
    a2_done(1)
    up_chunk(1)
    a2_forward(4)
    own(a2(8, 2))

    def up_step(w):
        @pl.when(w + 3 < NW)
        def _():
            a2_forward(w + 3)

        @pl.when(w + 7 < NW)
        def _():
            own(a2(w + 7, 2))

        a2_diag(w + 1)
        a2_done(w)
        k = w // 2

        @pl.when(lax.rem(w, 2) == 0)
        def _():
            for n in range(4):
                up_copy(k, n).wait()

            @pl.when(w <= 4)
            def _():
                for n in range(4):
                    up_copy(k + 3, n).start()
            pl.when(w == 6)(lambda: start_down(0))
            pl.when(w == 8)(lambda: start_down(4))
            pl.when(w == 10)(lambda: start_down(8))
        up_chunk(w)
        return 0

    lax.fori_loop(2, NW - 1, lambda w, c: up_step(w), 0)
    a2_done(NW - 1)
    up_chunk(NW - 1, final=True)
    start_down(12)

    wait_sent(hg2.at[:, 0:7], a2_send)

    def down_product(n):
        for k in range(3):
            down_copy(n, k).wait()
        slot = lax.rem(n, 3)
        with jax.named_scope("down"):
            for half in range(2):
                d = sum(dot(ub[:, k * KC:(k + 1) * KC], ring[lax.rem(8 + 3 * n + k, RING), :, half * NP:(half + 1) * NP]) for k in range(3))
                part[slot, :, :, half * NP:(half + 1) * NP] = d.reshape(N_DEV, ROWS, NP)
        rs_stage1(1, n)

        @pl.when(n + 5 < NCH)
        def _():
            down_copy(n + 5, 1).start()
            down_copy(n + 5, 2).start()

        @pl.when(n + 6 < NCH)
        def _():
            down_copy(n + 6, 0).start()

    def down_body(n, _):
        @pl.when(n < NCH)
        def _():
            down_product(n)

        @pl.when(jnp.logical_and(n >= 1, n < NCH + 1))
        def _():
            rs_stage2(1, n - 1)

        @pl.when(jnp.logical_and(n >= LAG3, n < NCH + LAG3))
        def _():
            rs_stage3(1, n - LAG3)

        @pl.when(n >= LAG4)
        def _():
            m = n - LAG4
            total = rs_stage4(1, m)
            cols = pl.ds(pl.multiple_of(m * CW, CW), CW)
            v = rows2d(res[:, :, cols]).astype(F32) + (total + bd_row[:, cols])
            res[:, :, cols] = v.astype(BF16).reshape(B, S_LOC, CW)
            pltpu.make_async_copy(res.at[:, :, cols], out_hbm.at[:, :, cols], o_sem).start()
        return 0
    lax.fori_loop(0, NCH + LAG4, down_body, 0)
    with jax.named_scope("drain"):
        rs_drain(1)
        pltpu.make_async_copy(res, out_hbm, o_sem).wait()


def solution(mesh):
    def device_body(hidden, ln1_gain, ln1_bias, w_qkv, b_qkv, w_out, b_out, ln2_gain, ln2_bias, w_up, b_up, w_down, b_down):
        any_spec = pl.BlockSpec(memory_space=pl.ANY)
        vmem = pl.BlockSpec(memory_space=pltpu.VMEM)

        def row(v):
            return v.reshape(1, -1)

        def tile(v):
            return v.reshape(-1, HD)

        two = pltpu.VMEM((NCH, 2, ROWS, CW), BF16)
        four = pltpu.VMEM((NCH, 4, ROWS, CW), BF16)
        one = pltpu.VMEM((NCH, ROWS, CW), BF16)
        dma = pltpu.SemaphoreType.DMA
        return pl.pallas_call(
            kernel,
            out_shape=jax.ShapeDtypeStruct((B, S_LOC, D), BF16),
            in_specs=[any_spec] * 5 + [vmem] * 8,
            out_specs=any_spec,
            scratch_shapes=[
                pltpu.VMEM((B, S_LOC, D), BF16),
                pltpu.VMEM((NV, N_DEV, S_LOC, VW), BF16),
                pltpu.VMEM((NW, N_DEV, ROWS, UW), BF16),
                pltpu.VMEM((M, FF), F32),
                pltpu.VMEM((SEQ, 3 * NQ), BF16),
                pltpu.VMEM((SEQ, NQ), BF16),
                pltpu.VMEM((M, FF), BF16),
                pltpu.VMEM((3, N_DEV, ROWS, CW), F32),
                pltpu.VMEM((4, 4, ROWS, CW), BF16), four, two, two, one, one,
                pltpu.VMEM((8, 2, ROWS, CW), F32),
                pltpu.VMEM((B, S_LOC, D), BF16),
                pltpu.VMEM((NS, KC, NC), BF16),
                pltpu.VMEM((3, NQ, 3 * CW), BF16),
                pltpu.VMEM((1, D), F32),
                pltpu.VMEM((1, D), F32),
                pltpu.VMEM((1, FF), F32),
                dma, dma, dma((NS,)), dma((5,)),
                dma, dma((NV, 3)),
                dma, dma((NW + 2, 2)), dma((NW,)),
                dma((4,)), dma((3,)), dma((NCH, 3)),
            ],
            compiler_params=pltpu.CompilerParams(collective_id=0, has_side_effects=True, vmem_limit_bytes=67_043_328),
            name="decoder_layer",
        )(hidden, jnp.transpose(w_qkv, (1, 2, 0, 3)), w_out.reshape(HEADS * HD, D), w_up, w_down,
          row(ln1_gain), row(ln1_bias), b_qkv, tile(b_out), row(ln2_gain), row(ln2_bias), tile(b_up), tile(b_down))

    in_layout = (P("dp", "tp", None), P(), P(), P(None, None, "tp", None), P(None, "tp", None), P("tp", None, None), P(), P(), P(), P(None, "tp"), P("tp"), P("tp", None), P())
    return jax.shard_map(device_body, mesh=mesh, in_specs=in_layout, out_specs=P("dp", "tp", None), check_vma=False)
```

```python
import jax
import jax.numpy as jnp
from jax import lax
from jax.experimental import pallas as pl
from jax.experimental.pallas import tpu as pltpu
from jax.sharding import PartitionSpec as P

MESH = pl.DeviceIdType.MESH
F32 = jnp.float32
BF16 = jnp.bfloat16
LN_EPS = 1e-5

N_DEV = 8
B, S_LOC = 3, 16
ROWS = B * S_LOC
SEQ = N_DEV * S_LOC
M = N_DEV * ROWS
D = 6144
HEADS, HD = 6, 128
NQ = HEADS * HD
FF = 3072
KC = 1024
NC = 768
NP = NC // 3
NU = D // KC
UW = 512
NW = D // UW
VK = 4
VW = D // VK
NV = VK * B
LAG3, LAG4 = 4, 7
AHEAD = 4
NCH = 12
CW = 512
NS = 18
RING = 16


def rows2d(v):
    return v.reshape(-1, v.shape[-1])


def dot(a, b):
    return jnp.dot(a, b, preferred_element_type=F32)


def kernel(x_hbm, wq_hbm, wo_hbm, wu_hbm, wd_hbm, *rest):
    small_hbm, out_hbm, small, rest = rest[:8], rest[8], rest[9:17], rest[17:]
    g1_ref, c1_ref, bq_ref, bo_ref, g2_ref, c2_ref, bu_ref, bd_ref = small
    (
     xv, hg1, hg2, acc, qkv, ctx, ub, part, s1, r1, s2, r2, s3, r3, keep, res, ring, wo, bo_row, bd_row, bu_row,
     x_sem, small_sem, o_sem, w_sem, wo_sem, a1_send, a1_recv, a2_send, a2_recv, a2_side, rs_first, rs_send, rs_recv) = rest
    me = lax.axis_index("tp")
    core = lax.rem(me, 2)
    xbit = lax.rem(me // 2, 2)
    ybit = me // 4
    dx = 2 - 4 * xbit
    dy = 4 - 8 * ybit
    ds = 1 - 2 * core
    sis = me + ds
    n1 = me + (1 - core) * dx + core * dy
    n2 = me + (1 - core) * dy + core * dx
    dg = me + dx + dy
    c_me, c_n1, c_n2, c_dg = me // 2, n1 // 2, n2 // 2, dg // 2

    def start_qkv(t):
        for j in range(NU):
            i = t * NU + j
            for h in range(HEADS):
                pltpu.make_async_copy(wq_hbm.at[t, h, j * KC:(j + 1) * KC, :], ring.at[i, :, h * HD:(h + 1) * HD], w_sem.at[i]).start()

    def up_copy(k, n):
        slot = lax.rem(4 * k, RING) + n
        k0 = pl.multiple_of(k * KC, KC)
        return pltpu.make_async_copy(wu_hbm.at[pl.ds(k0, KC), n * NC:(n + 1) * NC], ring.at[slot], w_sem.at[slot])

    def down_copy(n, k):
        slot = lax.rem(8 + 3 * n + k, RING)
        n0 = pl.multiple_of(n * CW, CW)
        return pltpu.make_async_copy(wd_hbm.at[k * KC:(k + 1) * KC, pl.ds(n0, CW)], ring.at[slot, :, 0:CW], w_sem.at[slot])

    def start_down(first):
        for j in range(first, first + 4):
            down_copy(j // 3, j % 3).start()

    def out_copies(n):
        cols = slice(n * 3 * CW, (n + 1) * 3 * CW)
        if n < 3:
            return [pltpu.make_async_copy(wo_hbm.at[:, cols], wo.at[n], wo_sem.at[n])]
        return [pltpu.make_async_copy(wo_hbm.at[k * M:(k + 1) * M, cols], ub.at[:, k * 3 * CW:(k + 1) * 3 * CW], wo_sem.at[n + k]) for k in range(2)]

    kind = (0, 0, 2, 1, 2, 2, 2)

    def a1_copy(v, j, block, to):
        ref = hg1.at[v, block]
        return pltpu.make_async_remote_copy(src_ref=ref, dst_ref=ref, send_sem=a1_send, recv_sem=a1_recv.at[v, kind[j]],
                                            device_id={"tp": to}, device_id_type=MESH)

    a2_rows = (slice(0, 2 * S_LOC), slice(2 * S_LOC, ROWS), slice(0, ROWS))

    def a2_index(u, h):
        return u + 2 if h == 2 else 2 * u + h

    def a2_copy(u, h, j, block, to):
        ref = hg2.at[u, block, a2_rows[h], :]
        sem = a2_side.at[u] if kind[j] == 2 else a2_recv.at[a2_index(u, h), kind[j]]
        return pltpu.make_async_remote_copy(src_ref=ref, dst_ref=ref, send_sem=a2_send, recv_sem=sem,
                                            device_id={"tp": to}, device_id_type=MESH)

    def wait_bytes(ref, sem):
        pltpu.make_async_remote_copy(src_ref=ref, dst_ref=ref, send_sem=sem, recv_sem=sem, device_id={"tp": me}, device_id_type=MESH).wait_recv()

    def wait_sent(ref, sem):
        pltpu.make_async_remote_copy(src_ref=ref, dst_ref=ref, send_sem=sem, recv_sem=sem, device_id={"tp": me}, device_id_type=MESH).wait_send()

    class Gather:
        def __init__(self, copy, blocks, sems):
            self.copy, self.blocks, self.sems = copy, blocks, sems

        def send(self, j):
            self.copy(j, (me, me, me, n1, n1, n2, dg)[j], (n1, n2, sis, n2, sis, sis, sis)[j]).start()

        def wait(self, k):
            wait_bytes(self.blocks((2, 1, 4)[k]), self.sems(k))

    def own(g):
        for j in (0, 1, 2):
            g.send(j)

    def forward(g):
        g.wait(0)
        for j in (3, 4, 5):
            g.send(j)

    def forward_diag(g):
        g.wait(1)
        g.send(6)

    def complete(g):
        g.wait(2)

    def a1(v):
        return Gather(lambda j, block, to: a1_copy(v, j, block, to), lambda n: hg1.at[v, 0:n], lambda k: a1_recv.at[v, k])

    def a2(u, h):
        return Gather(lambda j, block, to: a2_copy(u, h, j, block, to), lambda n: hg2.at[u, 0:n, a2_rows[h], :],
                      lambda k: a2_recv.at[a2_index(u, h), k])

    def a1_forward(v):
        with jax.named_scope("a1_forward"):
            @pl.when(v < NV)
            def _():
                forward(a1(v))

    def a1_diag(v):
        with jax.named_scope("a1_diag"):
            @pl.when(v < NV)
            def _():
                forward_diag(a1(v))

    def rs_copy(p, c, j):
        src, dst, to = ((s1, r1, sis), (s2, r2, n1), (s3, r3, n2))[j]
        return pltpu.make_async_remote_copy(src_ref=src.at[lax.rem(c, 4) if j == 0 else c], dst_ref=dst.at[c], send_sem=rs_first.at[lax.rem(c, 4)] if j == 0 else rs_send.at[j], recv_sem=rs_recv.at[c, j],
                                            device_id={"tp": to}, device_id_type=MESH)

    def rs_stage1(p, c):
        slot = lax.rem(c, 3)

        @pl.when(c >= 4)
        def _():
            rs_copy(p, c - 4, 0).wait_send()

        for q in range(4):
            s1[lax.rem(c, 4), q] = part[slot, 2 * q + 1 - core].astype(BF16)
        rs_copy(p, c, 0).start()

    def rs_stage2(p, c):
        slot = lax.rem(c, 3)
        with jax.named_scope("rs_wait1"):
            rs_copy(p, c, 0).wait_recv()

        def total(q):
            return part[slot, 2 * q + core] + r1[c, q].astype(F32)

        s2[c, 0] = total(c_n1).astype(BF16)
        s2[c, 1] = total(c_dg).astype(BF16)
        keep[lax.rem(c, 8), 0] = total(c_me)
        keep[lax.rem(c, 8), 1] = total(c_n2)
        rs_copy(p, c, 1).start()

    def rs_stage3(p, c):
        with jax.named_scope("rs_wait2"):
            rs_copy(p, c, 1).wait_recv()
        s3[c] = (keep[lax.rem(c, 8), 1] + r2[c, 1].astype(F32)).astype(BF16)
        keep[lax.rem(c, 8), 0] = keep[lax.rem(c, 8), 0] + r2[c, 0].astype(F32)
        rs_copy(p, c, 2).start()

    def rs_stage4(p, c):
        with jax.named_scope("rs_wait3"):
            rs_copy(p, c, 2).wait_recv()
        return keep[lax.rem(c, 8), 0] + r3[c].astype(F32)

    def rs_drain(p):
        wait_sent(s2, rs_send.at[1])
        wait_sent(s3, rs_send.at[2])
        for c in range(NCH - 4, NCH):
            rs_copy(p, c, 0).wait_send()

    def row_stats(xf):
        mean = jnp.mean(xf, axis=-1, keepdims=True)
        cen = xf - mean
        var = jnp.mean(cen * cen, axis=-1, keepdims=True)
        return mean, lax.rsqrt(var + LN_EPS)

    x_copy = pltpu.make_async_copy(x_hbm, xv, x_sem)
    x_copy.start()
    small_copies = [pltpu.make_async_copy(a, b, small_sem.at[i]) for i, (a, b) in enumerate(zip(small_hbm, small))]
    for copy in small_copies:
        copy.start()
    barrier = pltpu.get_barrier_semaphore()
    for other in (sis, n1, n2):
        pl.semaphore_signal(barrier, inc=1, device_id={"tp": other}, device_id_type=MESH)
    for copy in small_copies:
        copy.wait()
    for dst, src in ((bo_row, bo_ref), (bd_row, bd_ref), (bu_row, bu_ref)):
        wide = src[...].astype(F32)
        for r in range(src.shape[0]):
            dst[:, r * HD:(r + 1) * HD] = wide[r:r + 1, :]
    with jax.named_scope("entry_x"):
        x_copy.wait()
    start_qkv(0)

    with jax.named_scope("ln1"):
        for b in range(B):
            mean, rstd = row_stats(xv[b].astype(F32))
            for k in range(VK):
                cols = slice(k * VW, (k + 1) * VW)
                h = (xv[b, :, cols].astype(F32) - mean) * rstd * g1_ref[:, cols] + c1_ref[:, cols]
                hg1[VK * b + k, me] = h.astype(BF16)
    with jax.named_scope("entry_barrier"):
        pl.semaphore_wait(barrier, 3)
    for v in range(VK):
        own(a1(v))
    start_qkv(1)

    causal = lax.broadcasted_iota(jnp.int32, (SEQ, SEQ), 0) >= lax.broadcasted_iota(jnp.int32, (SEQ, SEQ), 1)

    def project_piece(v):
        with jax.named_scope("qkv0"):
            for t in range(3):
                bias = bq_ref[t].astype(F32)
                for p in range(3):
                    cols = slice(t * NQ + p * NP, t * NQ + (p + 1) * NP)
                    d = sum(dot(rows2d(hg1[v, :, :, (f % 3) * 512:(f % 3 + 1) * 512]), ring[t * NU + f // 2, (f % 2) * 512:(f % 2 + 1) * 512, p * NP:(p + 1) * NP])
                            for f in range(3 * v, 3 * v + 3))
                    if v == 0:
                        acc[0:SEQ, cols] = d
                    elif v < VK - 1:
                        acc[0:SEQ, cols] += d
                    else:
                        d = acc[0:SEQ, cols] + d
                        for k in range(2):
                            h = 2 * p + k
                            qkv[:, t * NQ + h * HD:t * NQ + (h + 1) * HD] = (d[:, k * HD:(k + 1) * HD] + bias[h:h + 1, :]).astype(BF16)

    def project(s):
        with jax.named_scope("qkv"):
            lhs = []
            for f in range(D // 512):
                lhs.append((rows2d(hg1[VK * s + f // 3, :, :, (f % 3) * 512:(f % 3 + 1) * 512]), f // 2, (f % 2) * 512))
            for t in range(3):
                bias = bq_ref[t].astype(F32)
                for p in range(3):
                    v = sum(dot(a, ring[t * NU + i, r0:r0 + 512, p * NP:(p + 1) * NP]) for a, i, r0 in lhs)
                    for k in range(2):
                        h = 2 * p + k
                        qkv[:, t * NQ + h * HD:t * NQ + (h + 1) * HD] = (v[:, k * HD:(k + 1) * HD] + bias[h:h + 1, :]).astype(BF16)

        @pl.when(s == B - 1)
        def _():
            for i in range(RING):
                up_copy(i // 4, i % 4).start()

    def attend():
        with jax.named_scope("attn"):
            def head(t, h):
                return qkv[:, t * NQ + h * HD:t * NQ + (h + 1) * HD]

            logits = [lax.dot_general(head(0, h), head(1, h), (((1,), (1,)), ((), ())), preferred_element_type=F32) for h in range(HEADS)]
            weights = []
            for x in logits:
                x = jnp.where(causal, x * HD ** -0.5, -1e30)
                e = jnp.exp(x - jnp.max(x, axis=-1, keepdims=True))
                weights.append((e * (1.0 / jnp.sum(e, axis=-1, keepdims=True))).astype(BF16))
            for h in range(HEADS):
                ctx[:, h * HD:(h + 1) * HD] = dot(weights[h], head(2, h)).astype(BF16)

    def out_product(s, n):
        @pl.when(s == 0)
        def _():
            for copy in out_copies(n):
                copy.wait()

        c = 4 * s + n
        slot = lax.rem(c, 3)
        with jax.named_scope("out"):
            for p in range(6):
                if n < 3:
                    d = dot(ctx[...], wo[n, :, p * NP:(p + 1) * NP])
                else:
                    d = sum(dot(ctx[:, k * M:(k + 1) * M], ub[:, k * 3 * CW + p * NP:k * 3 * CW + (p + 1) * NP]) for k in range(2))
                g, half = p // 2, p % 2
                part[slot, :, g * S_LOC:(g + 1) * S_LOC, half * NP:(half + 1) * NP] = d.reshape(N_DEV, S_LOC, NP)
        rs_stage1(0, c)

    def out_finish(s, n):
        total = rs_stage4(0, 4 * s + n)
        for g in range(3):
            cols = slice((3 * n + g) * CW, (3 * n + g + 1) * CW)
            res[s, :, cols] = (xv[s, :, cols].astype(F32) + (total[g * S_LOC:(g + 1) * S_LOC] + bo_row[:, cols])).astype(BF16)

    def norm2(s):
        with jax.named_scope("ln2"):
            r = pl.ds(pl.multiple_of(s * S_LOC, S_LOC), S_LOC)
            mean, rstd = row_stats(res[s].astype(F32))
            for u in range(NW):
                cols = slice(u * UW, (u + 1) * UW)
                h = (res[s, :, cols].astype(F32) - mean) * rstd * g2_ref[:, cols] + c2_ref[:, cols]
                hg2[u, me, r, :] = h.astype(BF16)

    for v in range(VK):
        with jax.named_scope("a1_forward"):
            forward(a1(v))
        if v == 0:
            start_qkv(2)
    for v in range(VK, 2 * VK):
        own(a1(v))
    forward_diag(a1(0))
    for v in range(VK):
        if v + 1 < VK:
            with jax.named_scope("a1_diag"):
                forward_diag(a1(v + 1))
        with jax.named_scope("a1_complete"):
            complete(a1(v))
        if v == 0:
            for i in range(NS):
                pltpu.make_async_copy(wu_hbm.at[0:KC, 0:NC], ring.at[i], w_sem.at[i]).wait()
            for n in range(4):
                for copy in out_copies(n):
                    copy.start()
        project_piece(v)
        if v == 1:
            forward(a1(VK))
            for k in range(2 * VK, NV):
                own(a1(k))

    def seq_body(s, _):
        b0 = 4 * s - 4

        def before(f):
            pl.when(s >= 1)(f)

        @pl.when(s >= 1)
        def _():
            with jax.named_scope("a1_complete"):
                for k in range(VK):
                    complete(a1(VK * s + k))

        @before
        def _():
            project(s)
            rs_stage2(0, b0 + 3)
            rs_stage3(0, b0)
            rs_stage3(0, b0 + 1)

        for t in range(3):
            a1_forward(VK * s + 5 + t)

        @pl.when(s >= 2)
        def _():
            for k in range(4):
                out_finish(s - 2, k)
            norm2(s - 2)

        attend()
        before(lambda: rs_stage3(0, b0 + 2))
        out_product(s, 0)
        out_product(s, 1)
        before(lambda: rs_stage3(0, b0 + 3))
        out_product(s, 2)
        rs_stage2(0, 4 * s)
        for k in range(2):
            a1_diag(VK * s + 4 + k)
        out_product(s, 3)
        rs_stage2(0, 4 * s + 1)
        for k in range(2, VK):
            a1_diag(VK * s + 4 + k)
        a1_forward(VK * s + 8)
        rs_stage2(0, 4 * s + 2)
        return 0
    lax.fori_loop(0, B, seq_body, 0)

    c0, last = NCH - 4, B - 1
    rs_stage2(0, c0 + 3)
    for k in range(4):
        out_finish(last - 1, k)
    rs_stage3(0, c0)
    norm2(last - 1)
    for k in range(1, 4):
        rs_stage3(0, c0 + k)
    out_finish(last, 0)
    out_finish(last, 1)
    own(a2(0, 0))
    own(a2(1, 0))
    out_finish(last, 2)
    out_finish(last, 3)
    norm2(last)
    own(a2(0, 1))
    own(a2(1, 1))
    own(a2(2, 2))
    with jax.named_scope("a2_forward"):
        forward(a2(0, 0))
        forward(a2(0, 1))
        forward(a2(1, 0))
        forward(a2(1, 1))
    for u in (3, 4, 5):
        own(a2(u, 2))
    wait_sent(hg1.at[:, 0:7], a1_send)
    rs_drain(0)

    def up_chunk(w, first=False, final=False):
        with jax.named_scope("up"):
            lhs = rows2d(hg2[w])
            slot = lax.rem(4 * (w // 2), RING)
            rows = pl.ds(pl.multiple_of(lax.rem(w, 2) * UW, UW), UW)
            for n in range(4):
                for p in range(3):
                    c = slice(n * NC + p * NP, n * NC + (p + 1) * NP)
                    d = dot(lhs, ring[slot + n, rows, p * NP:(p + 1) * NP])
                    if first:
                        acc[:, c] = d
                    elif final:
                        ub[:, c] = jax.nn.gelu(acc[:, c] + d + bu_row[:, c], approximate=True).astype(BF16)
                    else:
                        acc[:, c] += d

    def a2_done(w):
        with jax.named_scope("a2_complete"):
            wait_bytes(hg2.at[w, 0:4], a2_side.at[w])

    def a2_forward(w):
        with jax.named_scope("a2_forward"):
            forward(a2(w, 2))

    def a2_diag(w, parts=(2,)):
        with jax.named_scope("a2_diag"):
            for h in parts:
                forward_diag(a2(w, h))

    for n in range(4):
        up_copy(0, n).wait()
    a2_diag(0, (0, 1))
    a2_forward(2)
    own(a2(6, 2))
    a2_diag(1, (0, 1))
    a2_done(0)
    up_chunk(0, first=True)
    a2_forward(3)
    own(a2(7, 2))
    a2_diag(2)
    a2_forward(4)
    own(a2(8, 2))
    a2_done(1)
    up_chunk(1)

    def up_step(w):
        @pl.when(w + 3 < NW)
        def _():
            a2_forward(w + 3)

        @pl.when(w + 7 < NW)
        def _():
            own(a2(w + 7, 2))

        a2_diag(w + 1)
        a2_done(w)
        k = w // 2

        @pl.when(lax.rem(w, 2) == 0)
        def _():
            for n in range(4):
                up_copy(k, n).wait()

            @pl.when(w <= 4)
            def _():
                for n in range(4):
                    up_copy(k + 3, n).start()
            pl.when(w == 6)(lambda: start_down(0))
            pl.when(w == 8)(lambda: start_down(4))
            pl.when(w == 10)(lambda: start_down(8))
        up_chunk(w)
        return 0

    lax.fori_loop(2, NW - 1, lambda w, c: up_step(w), 0)
    a2_done(NW - 1)
    up_chunk(NW - 1, final=True)
    start_down(12)

    wait_sent(hg2.at[:, 0:7], a2_send)

    def down_product(n):
        for k in range(3):
            down_copy(n, k).wait()
        slot = lax.rem(n, 3)
        with jax.named_scope("down"):
            for half in range(2):
                d = sum(dot(ub[:, k * KC:(k + 1) * KC], ring[lax.rem(8 + 3 * n + k, RING), :, half * NP:(half + 1) * NP]) for k in range(3))
                part[slot, :, :, half * NP:(half + 1) * NP] = d.reshape(N_DEV, ROWS, NP)
        rs_stage1(1, n)

        @pl.when(n + 5 < NCH)
        def _():
            down_copy(n + 5, 1).start()
            down_copy(n + 5, 2).start()

        @pl.when(n + 6 < NCH)
        def _():
            down_copy(n + 6, 0).start()

    def down_body(n, _):
        @pl.when(n < NCH)
        def _():
            down_product(n)

        @pl.when(jnp.logical_and(n >= 1, n < NCH + 1))
        def _():
            rs_stage2(1, n - 1)

        @pl.when(jnp.logical_and(n >= LAG3, n < NCH + LAG3))
        def _():
            rs_stage3(1, n - LAG3)

        @pl.when(n >= LAG4)
        def _():
            m = n - LAG4
            total = rs_stage4(1, m)
            cols = pl.ds(pl.multiple_of(m * CW, CW), CW)
            v = rows2d(res[:, :, cols]).astype(F32) + (total + bd_row[:, cols])
            res[:, :, cols] = v.astype(BF16).reshape(B, S_LOC, CW)
            pltpu.make_async_copy(res.at[:, :, cols], out_hbm.at[:, :, cols], o_sem).start()
        return 0
    lax.fori_loop(0, NCH + LAG4, down_body, 0)
    with jax.named_scope("drain"):
        rs_drain(1)
        pltpu.make_async_copy(res, out_hbm, o_sem).wait()


def solution(mesh):
    def device_body(hidden, ln1_gain, ln1_bias, w_qkv, b_qkv, w_out, b_out, ln2_gain, ln2_bias, w_up, b_up, w_down, b_down):
        any_spec = pl.BlockSpec(memory_space=pl.ANY)

        def row(v):
            return v.reshape(1, -1)

        def tile(v):
            return v.reshape(-1, HD)

        two = pltpu.VMEM((NCH, 2, ROWS, CW), BF16)
        four = pltpu.VMEM((NCH, 4, ROWS, CW), BF16)
        one = pltpu.VMEM((NCH, ROWS, CW), BF16)
        dma = pltpu.SemaphoreType.DMA
        return pl.pallas_call(
            kernel,
            out_shape=jax.ShapeDtypeStruct((B, S_LOC, D), BF16),
            in_specs=[any_spec] * 13,
            out_specs=any_spec,
            scratch_shapes=[
                pltpu.VMEM((1, D), F32), pltpu.VMEM((1, D), F32), pltpu.VMEM((3, HEADS, HD), BF16), pltpu.VMEM((D // HD, HD), BF16),
                pltpu.VMEM((1, D), F32), pltpu.VMEM((1, D), F32), pltpu.VMEM((FF // HD, HD), BF16), pltpu.VMEM((D // HD, HD), BF16),
                pltpu.VMEM((B, S_LOC, D), BF16),
                pltpu.VMEM((NV, N_DEV, S_LOC, VW), BF16),
                pltpu.VMEM((NW, N_DEV, ROWS, UW), BF16),
                pltpu.VMEM((M, FF), F32),
                pltpu.VMEM((SEQ, 3 * NQ), BF16),
                pltpu.VMEM((SEQ, NQ), BF16),
                pltpu.VMEM((M, FF), BF16),
                pltpu.VMEM((3, N_DEV, ROWS, CW), F32),
                pltpu.VMEM((4, 4, ROWS, CW), BF16), four, two, two, one, one,
                pltpu.VMEM((8, 2, ROWS, CW), F32),
                pltpu.VMEM((B, S_LOC, D), BF16),
                pltpu.VMEM((NS, KC, NC), BF16),
                pltpu.VMEM((3, NQ, 3 * CW), BF16),
                pltpu.VMEM((1, D), F32),
                pltpu.VMEM((1, D), F32),
                pltpu.VMEM((1, FF), F32),
                dma, dma((8,)), dma, dma((NS,)), dma((5,)),
                dma, dma((NV, 3)),
                dma, dma((NW + 2, 2)), dma((NW,)),
                dma((4,)), dma((3,)), dma((NCH, 3)),
            ],
            compiler_params=pltpu.CompilerParams(collective_id=0, has_side_effects=True, vmem_limit_bytes=67_043_328),
            name="decoder_layer",
        )(hidden, jnp.transpose(w_qkv, (1, 2, 0, 3)), w_out.reshape(HEADS * HD, D), w_up, w_down,
          row(ln1_gain), row(ln1_bias), b_qkv, tile(b_out), row(ln2_gain), row(ln2_bias), tile(b_up), tile(b_down))

    in_layout = (P("dp", "tp", None), P(), P(), P(None, None, "tp", None), P(None, "tp", None), P("tp", None, None), P(), P(), P(), P(None, "tp"), P("tp"), P("tp", None), P())
    return jax.shard_map(device_body, mesh=mesh, in_specs=in_layout, out_specs=P("dp", "tp", None), check_vma=False)
```

```python
import jax
import jax.numpy as jnp
from jax import lax
from jax.experimental import pallas as pl
from jax.experimental.pallas import tpu as pltpu
from jax.sharding import PartitionSpec as P

MESH = pl.DeviceIdType.MESH
F32 = jnp.float32
BF16 = jnp.bfloat16
LN_EPS = 1e-5

N_DEV = 8
B, S_LOC = 3, 16
ROWS = B * S_LOC
SEQ = N_DEV * S_LOC
M = N_DEV * ROWS
D = 6144
HEADS, HD = 6, 128
NQ = HEADS * HD
FF = 3072
KC = 1024
NC = 768
NP = NC // 3
NU = D // KC
UW = 512
NW = D // UW
VK = 4
VW = D // VK
NV = VK * B
LAG3, LAG4 = 4, 7
AHEAD = 4
NCH = 12
CW = 512
NS = 18
RING = 16


def rows2d(v):
    return v.reshape(-1, v.shape[-1])


def dot(a, b):
    return jnp.dot(a, b, preferred_element_type=F32)


def kernel(x_hbm, wq_hbm, wo_hbm, wu_hbm, wd_hbm, *rest):
    small_hbm, out_hbm, small, rest = rest[:8], rest[8], rest[9:17], rest[17:]
    g1_ref, c1_ref, bq_ref, bo_ref, g2_ref, c2_ref, bu_ref, bd_ref = small
    (
     xv, hg1, hg2, acc, qkv, ctx, ub, part, s1, r1, s2, r2, s3, r3, keep, res, ring, wo, bo_row, bd_row, bu_row,
     x_sem, small_sem, o_sem, w_sem, wo_sem, a1_send, a1_recv, a2_send, a2_recv, a2_side, rs_first, rs_send, rs_recv) = rest
    me = lax.axis_index("tp")
    core = lax.rem(me, 2)
    xbit = lax.rem(me // 2, 2)
    ybit = me // 4
    dx = 2 - 4 * xbit
    dy = 4 - 8 * ybit
    ds = 1 - 2 * core
    sis = me + ds
    n1 = me + (1 - core) * dx + core * dy
    n2 = me + (1 - core) * dy + core * dx
    dg = me + dx + dy
    c_me, c_n1, c_n2, c_dg = me // 2, n1 // 2, n2 // 2, dg // 2

    def start_qkv(t):
        for j in range(NU):
            i = t * NU + j
            for h in range(HEADS):
                pltpu.make_async_copy(wq_hbm.at[t, h, j * KC:(j + 1) * KC, :], ring.at[i, :, h * HD:(h + 1) * HD], w_sem.at[i]).start()

    def up_copy(k, n):
        slot = lax.rem(4 * k, RING) + n
        k0 = pl.multiple_of(k * KC, KC)
        return pltpu.make_async_copy(wu_hbm.at[pl.ds(k0, KC), n * NC:(n + 1) * NC], ring.at[slot], w_sem.at[slot])

    def down_copy(n, k):
        slot = lax.rem(8 + 3 * n + k, RING)
        n0 = pl.multiple_of(n * CW, CW)
        return pltpu.make_async_copy(wd_hbm.at[k * KC:(k + 1) * KC, pl.ds(n0, CW)], ring.at[slot, :, 0:CW], w_sem.at[slot])

    def start_down(first):
        for j in range(first, first + 4):
            down_copy(j // 3, j % 3).start()

    def out_copies(n):
        cols = slice(n * 3 * CW, (n + 1) * 3 * CW)
        if n < 3:
            return [pltpu.make_async_copy(wo_hbm.at[:, cols], wo.at[n], wo_sem.at[n])]
        return [pltpu.make_async_copy(wo_hbm.at[k * M:(k + 1) * M, cols], ub.at[:, k * 3 * CW:(k + 1) * 3 * CW], wo_sem.at[n + k]) for k in range(2)]

    kind = (0, 0, 2, 1, 2, 2, 2)

    def a1_copy(v, j, block, to):
        ref = hg1.at[v, block]
        return pltpu.make_async_remote_copy(src_ref=ref, dst_ref=ref, send_sem=a1_send, recv_sem=a1_recv.at[v, kind[j]],
                                            device_id={"tp": to}, device_id_type=MESH)

    a2_rows = (slice(0, 2 * S_LOC), slice(2 * S_LOC, ROWS), slice(0, ROWS))

    def a2_index(u, h):
        return u + 2 if h == 2 else 2 * u + h

    def a2_copy(u, h, j, block, to):
        ref = hg2.at[u, block, a2_rows[h], :]
        sem = a2_side.at[u] if kind[j] == 2 else a2_recv.at[a2_index(u, h), kind[j]]
        return pltpu.make_async_remote_copy(src_ref=ref, dst_ref=ref, send_sem=a2_send, recv_sem=sem,
                                            device_id={"tp": to}, device_id_type=MESH)

    def wait_bytes(ref, sem):
        pltpu.make_async_remote_copy(src_ref=ref, dst_ref=ref, send_sem=sem, recv_sem=sem, device_id={"tp": me}, device_id_type=MESH).wait_recv()

    def wait_sent(ref, sem):
        pltpu.make_async_remote_copy(src_ref=ref, dst_ref=ref, send_sem=sem, recv_sem=sem, device_id={"tp": me}, device_id_type=MESH).wait_send()

    class Gather:
        def __init__(self, copy, blocks, sems):
            self.copy, self.blocks, self.sems = copy, blocks, sems

        def send(self, j):
            self.copy(j, (me, me, me, n1, n1, n2, dg)[j], (n1, n2, sis, n2, sis, sis, sis)[j]).start()

        def wait(self, k):
            wait_bytes(self.blocks((2, 1, 4)[k]), self.sems(k))

    def own(g):
        for j in (0, 1, 2):
            g.send(j)

    def forward(g):
        g.wait(0)
        for j in (3, 4, 5):
            g.send(j)

    def forward_diag(g):
        g.wait(1)
        g.send(6)

    def complete(g):
        g.wait(2)

    def a1(v):
        return Gather(lambda j, block, to: a1_copy(v, j, block, to), lambda n: hg1.at[v, 0:n], lambda k: a1_recv.at[v, k])

    def a2(u, h):
        return Gather(lambda j, block, to: a2_copy(u, h, j, block, to), lambda n: hg2.at[u, 0:n, a2_rows[h], :],
                      lambda k: a2_recv.at[a2_index(u, h), k])

    def a1_forward(v):
        with jax.named_scope("a1_forward"):
            @pl.when(v < NV)
            def _():
                forward(a1(v))

    def a1_diag(v):
        with jax.named_scope("a1_diag"):
            @pl.when(v < NV)
            def _():
                forward_diag(a1(v))

    def rs_copy(p, c, j):
        src, dst, to = ((s1, r1, sis), (s2, r2, n1), (s3, r3, n2))[j]
        return pltpu.make_async_remote_copy(src_ref=src.at[lax.rem(c, 4) if j == 0 else c], dst_ref=dst.at[c], send_sem=rs_first.at[lax.rem(c, 4)] if j == 0 else rs_send.at[j], recv_sem=rs_recv.at[c, j],
                                            device_id={"tp": to}, device_id_type=MESH)

    def rs_stage1(p, c):
        slot = lax.rem(c, 3)

        @pl.when(c >= 4)
        def _():
            rs_copy(p, c - 4, 0).wait_send()

        for q in range(4):
            s1[lax.rem(c, 4), q] = part[slot, 2 * q + 1 - core].astype(BF16)
        rs_copy(p, c, 0).start()

    def rs_stage2(p, c):
        slot = lax.rem(c, 3)
        with jax.named_scope("rs_wait1"):
            rs_copy(p, c, 0).wait_recv()

        def total(q):
            return part[slot, 2 * q + core] + r1[c, q].astype(F32)

        s2[c, 0] = total(c_n1).astype(BF16)
        s2[c, 1] = total(c_dg).astype(BF16)
        keep[lax.rem(c, 8), 0] = total(c_me)
        keep[lax.rem(c, 8), 1] = total(c_n2)
        rs_copy(p, c, 1).start()

    def rs_stage3(p, c):
        with jax.named_scope("rs_wait2"):
            rs_copy(p, c, 1).wait_recv()
        s3[c] = (keep[lax.rem(c, 8), 1] + r2[c, 1].astype(F32)).astype(BF16)
        keep[lax.rem(c, 8), 0] = keep[lax.rem(c, 8), 0] + r2[c, 0].astype(F32)
        rs_copy(p, c, 2).start()

    def rs_stage4(p, c):
        with jax.named_scope("rs_wait3"):
            rs_copy(p, c, 2).wait_recv()
        return keep[lax.rem(c, 8), 0] + r3[c].astype(F32)

    def rs_drain(p):
        wait_sent(s2, rs_send.at[1])
        wait_sent(s3, rs_send.at[2])
        for c in range(NCH - 4, NCH):
            rs_copy(p, c, 0).wait_send()

    def row_stats(xf):
        mean = jnp.mean(xf, axis=-1, keepdims=True)
        cen = xf - mean
        var = jnp.mean(cen * cen, axis=-1, keepdims=True)
        return mean, lax.rsqrt(var + LN_EPS)

    x_copy = pltpu.make_async_copy(x_hbm, xv, x_sem)
    x_copy.start()
    small_copies = [pltpu.make_async_copy(a, b, small_sem.at[i]) for i, (a, b) in enumerate(zip(small_hbm, small))]
    for copy in small_copies:
        copy.start()
    barrier = pltpu.get_barrier_semaphore()
    for other in (sis, n1, n2):
        pl.semaphore_signal(barrier, inc=1, device_id={"tp": other}, device_id_type=MESH)
    for copy in small_copies:
        copy.wait()
    for dst, src in ((bo_row, bo_ref), (bd_row, bd_ref), (bu_row, bu_ref)):
        wide = src[...].astype(F32)
        for r in range(src.shape[0]):
            dst[:, r * HD:(r + 1) * HD] = wide[r:r + 1, :]
    with jax.named_scope("entry_x"):
        x_copy.wait()
    start_qkv(0)

    with jax.named_scope("ln1"):
        for b in range(B):
            mean, rstd = row_stats(xv[b].astype(F32))
            for k in range(VK):
                cols = slice(k * VW, (k + 1) * VW)
                h = (xv[b, :, cols].astype(F32) - mean) * rstd * g1_ref[:, cols] + c1_ref[:, cols]
                hg1[VK * b + k, me] = h.astype(BF16)
    with jax.named_scope("entry_barrier"):
        pl.semaphore_wait(barrier, 3)
    for v in range(VK):
        own(a1(v))
    start_qkv(1)

    causal = lax.broadcasted_iota(jnp.int32, (SEQ, SEQ), 0) >= lax.broadcasted_iota(jnp.int32, (SEQ, SEQ), 1)

    def project_piece(v):
        with jax.named_scope("qkv0"):
            for t in range(3):
                bias = bq_ref[t].astype(F32)
                for p in range(3):
                    cols = slice(t * NQ + p * NP, t * NQ + (p + 1) * NP)
                    d = sum(dot(rows2d(hg1[v, :, :, (f % 3) * 512:(f % 3 + 1) * 512]), ring[t * NU + f // 2, (f % 2) * 512:(f % 2 + 1) * 512, p * NP:(p + 1) * NP])
                            for f in range(3 * v, 3 * v + 3))
                    if v == 0:
                        acc[0:SEQ, cols] = d
                    elif v < VK - 1:
                        acc[0:SEQ, cols] += d
                    else:
                        d = acc[0:SEQ, cols] + d
                        for k in range(2):
                            h = 2 * p + k
                            qkv[:, t * NQ + h * HD:t * NQ + (h + 1) * HD] = (d[:, k * HD:(k + 1) * HD] + bias[h:h + 1, :]).astype(BF16)

    def project(s, t):
        with jax.named_scope("qkv"):
            lhs = []
            for f in range(D // 512):
                lhs.append((rows2d(hg1[VK * s + f // 3, :, :, (f % 3) * 512:(f % 3 + 1) * 512]), t * NU + f // 2, (f % 2) * 512))
            bias = bq_ref[t].astype(F32)
            for p in range(3):
                v = sum(dot(a, ring[i, r0:r0 + 512, p * NP:(p + 1) * NP]) for a, i, r0 in lhs)
                for k in range(2):
                    h = 2 * p + k
                    cols = pl.ds(pl.multiple_of(t * NQ + h * HD, HD), HD)
                    qkv[:, cols] = (v[:, k * HD:(k + 1) * HD] + bias[h:h + 1, :]).astype(BF16)

        @pl.when(s == B - 1)
        def _():
            for tt, lo, hi in ((0, 0, 4), (1, 4, 12), (2, 12, 16)):
                @pl.when(t == tt)
                def _():
                    for i in range(lo, hi):
                        up_copy(i // 4, i % 4).start()

    def attend():
        with jax.named_scope("attn"):
            def head(t, h):
                return qkv[:, t * NQ + h * HD:t * NQ + (h + 1) * HD]

            logits = [lax.dot_general(head(0, h), head(1, h), (((1,), (1,)), ((), ())), preferred_element_type=F32) for h in range(HEADS)]
            weights = []
            for x in logits:
                x = jnp.where(causal, x * HD ** -0.5, -1e30)
                e = jnp.exp(x - jnp.max(x, axis=-1, keepdims=True))
                weights.append((e * (1.0 / jnp.sum(e, axis=-1, keepdims=True))).astype(BF16))
            for h in range(HEADS):
                ctx[:, h * HD:(h + 1) * HD] = dot(weights[h], head(2, h)).astype(BF16)

    def out_product(s, n):
        @pl.when(s == 0)
        def _():
            for copy in out_copies(n):
                copy.wait()

        c = 4 * s + n
        slot = lax.rem(c, 3)
        with jax.named_scope("out"):
            for p in range(6):
                if n < 3:
                    d = dot(ctx[...], wo[n, :, p * NP:(p + 1) * NP])
                else:
                    d = sum(dot(ctx[:, k * M:(k + 1) * M], ub[:, k * 3 * CW + p * NP:k * 3 * CW + (p + 1) * NP]) for k in range(2))
                g, half = p // 2, p % 2
                part[slot, :, g * S_LOC:(g + 1) * S_LOC, half * NP:(half + 1) * NP] = d.reshape(N_DEV, S_LOC, NP)
        rs_stage1(0, c)

    def out_finish(s, n):
        total = rs_stage4(0, 4 * s + n)
        for g in range(3):
            cols = slice((3 * n + g) * CW, (3 * n + g + 1) * CW)
            res[s, :, cols] = (xv[s, :, cols].astype(F32) + (total[g * S_LOC:(g + 1) * S_LOC] + bo_row[:, cols])).astype(BF16)

    def norm2(s):
        with jax.named_scope("ln2"):
            r = pl.ds(pl.multiple_of(s * S_LOC, S_LOC), S_LOC)
            mean, rstd = row_stats(res[s].astype(F32))
            for u in range(NW):
                cols = slice(u * UW, (u + 1) * UW)
                h = (res[s, :, cols].astype(F32) - mean) * rstd * g2_ref[:, cols] + c2_ref[:, cols]
                hg2[u, me, r, :] = h.astype(BF16)

    for v in range(VK):
        with jax.named_scope("a1_forward"):
            forward(a1(v))
        if v == 0:
            start_qkv(2)
    for v in range(VK, 2 * VK):
        own(a1(v))
    forward_diag(a1(0))
    for v in range(VK):
        if v + 1 < VK:
            with jax.named_scope("a1_diag"):
                forward_diag(a1(v + 1))
        with jax.named_scope("a1_complete"):
            complete(a1(v))
        if v == 0:
            for i in range(NS):
                pltpu.make_async_copy(wu_hbm.at[0:KC, 0:NC], ring.at[i], w_sem.at[i]).wait()
            for n in range(4):
                for copy in out_copies(n):
                    copy.start()
        project_piece(v)
        if v == 1:
            forward(a1(VK))
            for k in range(2 * VK, NV):
                own(a1(k))

    def seq_body(s, _):
        b0 = 4 * s - 4

        def before(f):
            pl.when(s >= 1)(f)

        @pl.when(s >= 1)
        def _():
            with jax.named_scope("a1_complete"):
                for k in range(VK):
                    complete(a1(VK * s + k))

        def qkv_body(t, _):
            pl.when(s >= 1)(lambda: project(s, t))

            @pl.when(jnp.logical_and(s >= 1, t == 0))
            def _():
                rs_stage2(0, b0 + 3)

            @pl.when(jnp.logical_and(s >= 1, t >= 1))
            def _():
                rs_stage3(0, b0 + t - 1)
            a1_forward(VK * s + 5 + t)
            return 0
        lax.fori_loop(0, 3, qkv_body, 0)

        @pl.when(s >= 2)
        def _():
            for k in range(4):
                out_finish(s - 2, k)
            norm2(s - 2)

        attend()
        before(lambda: rs_stage3(0, b0 + 2))
        out_product(s, 0)
        before(lambda: rs_stage3(0, b0 + 3))
        out_product(s, 1)
        out_product(s, 2)
        rs_stage2(0, 4 * s)
        for k in range(2):
            a1_diag(VK * s + 4 + k)
        out_product(s, 3)
        rs_stage2(0, 4 * s + 1)
        for k in range(2, VK):
            a1_diag(VK * s + 4 + k)
        a1_forward(VK * s + 8)
        rs_stage2(0, 4 * s + 2)
        return 0
    lax.fori_loop(0, B, seq_body, 0)

    c0, last = NCH - 4, B - 1
    rs_stage2(0, c0 + 3)
    for k in range(4):
        out_finish(last - 1, k)
    rs_stage3(0, c0)
    norm2(last - 1)
    for k in range(1, 4):
        rs_stage3(0, c0 + k)
    out_finish(last, 0)
    out_finish(last, 1)
    own(a2(0, 0))
    own(a2(1, 0))
    out_finish(last, 2)
    out_finish(last, 3)
    norm2(last)
    own(a2(0, 1))
    own(a2(1, 1))
    own(a2(2, 2))
    with jax.named_scope("a2_forward"):
        forward(a2(0, 0))
        forward(a2(0, 1))
        forward(a2(1, 0))
        forward(a2(1, 1))
    for u in (3, 4, 5):
        own(a2(u, 2))
    wait_sent(hg1.at[:, 0:7], a1_send)
    rs_drain(0)

    def up_chunk(w, first=False, final=False):
        with jax.named_scope("up"):
            lhs = rows2d(hg2[w])
            slot = lax.rem(4 * (w // 2), RING)
            rows = pl.ds(pl.multiple_of(lax.rem(w, 2) * UW, UW), UW)
            for n in range(4):
                for p in range(3):
                    c = slice(n * NC + p * NP, n * NC + (p + 1) * NP)
                    d = dot(lhs, ring[slot + n, rows, p * NP:(p + 1) * NP])
                    if first:
                        acc[:, c] = d
                    elif final:
                        ub[:, c] = jax.nn.gelu(acc[:, c] + d + bu_row[:, c], approximate=True).astype(BF16)
                    else:
                        acc[:, c] += d

    def a2_done(w):
        with jax.named_scope("a2_complete"):
            wait_bytes(hg2.at[w, 0:4], a2_side.at[w])

    def a2_forward(w):
        with jax.named_scope("a2_forward"):
            forward(a2(w, 2))

    def a2_diag(w, parts=(2,)):
        with jax.named_scope("a2_diag"):
            for h in parts:
                forward_diag(a2(w, h))

    for n in range(4):
        up_copy(0, n).wait()
    a2_diag(0, (0, 1))
    a2_forward(2)
    own(a2(6, 2))
    a2_diag(1, (0, 1))
    a2_done(0)
    up_chunk(0, first=True)
    a2_forward(3)
    own(a2(7, 2))
    a2_diag(2)
    a2_forward(4)
    own(a2(8, 2))
    a2_done(1)
    up_chunk(1)

    def up_step(w):
        @pl.when(w + 3 < NW)
        def _():
            a2_forward(w + 3)

        @pl.when(w + 7 < NW)
        def _():
            own(a2(w + 7, 2))

        a2_diag(w + 1)
        a2_done(w)
        k = w // 2

        @pl.when(lax.rem(w, 2) == 0)
        def _():
            for n in range(4):
                up_copy(k, n).wait()

            @pl.when(w <= 4)
            def _():
                for n in range(4):
                    up_copy(k + 3, n).start()
            pl.when(w == 6)(lambda: start_down(0))
            pl.when(w == 8)(lambda: start_down(4))
            pl.when(w == 10)(lambda: start_down(8))
        up_chunk(w)
        return 0

    lax.fori_loop(2, NW - 1, lambda w, c: up_step(w), 0)
    a2_done(NW - 1)
    up_chunk(NW - 1, final=True)
    start_down(12)

    wait_sent(hg2.at[:, 0:7], a2_send)

    def down_product(n):
        for k in range(3):
            down_copy(n, k).wait()
        slot = lax.rem(n, 3)
        with jax.named_scope("down"):
            for half in range(2):
                d = sum(dot(ub[:, k * KC:(k + 1) * KC], ring[lax.rem(8 + 3 * n + k, RING), :, half * NP:(half + 1) * NP]) for k in range(3))
                part[slot, :, :, half * NP:(half + 1) * NP] = d.reshape(N_DEV, ROWS, NP)
        rs_stage1(1, n)

        @pl.when(n + 5 < NCH)
        def _():
            down_copy(n + 5, 1).start()
            down_copy(n + 5, 2).start()

        @pl.when(n + 6 < NCH)
        def _():
            down_copy(n + 6, 0).start()

    def down_body(n, _):
        @pl.when(n < NCH)
        def _():
            down_product(n)

        @pl.when(jnp.logical_and(n >= 1, n < NCH + 1))
        def _():
            rs_stage2(1, n - 1)

        @pl.when(jnp.logical_and(n >= LAG3, n < NCH + LAG3))
        def _():
            rs_stage3(1, n - LAG3)

        @pl.when(n >= LAG4)
        def _():
            m = n - LAG4
            total = rs_stage4(1, m)
            cols = pl.ds(pl.multiple_of(m * CW, CW), CW)
            v = rows2d(res[:, :, cols]).astype(F32) + (total + bd_row[:, cols])
            res[:, :, cols] = v.astype(BF16).reshape(B, S_LOC, CW)
            pltpu.make_async_copy(res.at[:, :, cols], out_hbm.at[:, :, cols], o_sem).start()
        return 0
    lax.fori_loop(0, NCH + LAG4, down_body, 0)
    with jax.named_scope("drain"):
        rs_drain(1)
        pltpu.make_async_copy(res, out_hbm, o_sem).wait()


def solution(mesh):
    def device_body(hidden, ln1_gain, ln1_bias, w_qkv, b_qkv, w_out, b_out, ln2_gain, ln2_bias, w_up, b_up, w_down, b_down):
        any_spec = pl.BlockSpec(memory_space=pl.ANY)

        def row(v):
            return v.reshape(1, -1)

        def tile(v):
            return v.reshape(-1, HD)

        two = pltpu.VMEM((NCH, 2, ROWS, CW), BF16)
        four = pltpu.VMEM((NCH, 4, ROWS, CW), BF16)
        one = pltpu.VMEM((NCH, ROWS, CW), BF16)
        dma = pltpu.SemaphoreType.DMA
        return pl.pallas_call(
            kernel,
            out_shape=jax.ShapeDtypeStruct((B, S_LOC, D), BF16),
            in_specs=[any_spec] * 13,
            out_specs=any_spec,
            scratch_shapes=[
                pltpu.VMEM((1, D), F32), pltpu.VMEM((1, D), F32), pltpu.VMEM((3, HEADS, HD), BF16), pltpu.VMEM((D // HD, HD), BF16),
                pltpu.VMEM((1, D), F32), pltpu.VMEM((1, D), F32), pltpu.VMEM((FF // HD, HD), BF16), pltpu.VMEM((D // HD, HD), BF16),
                pltpu.VMEM((B, S_LOC, D), BF16),
                pltpu.VMEM((NV, N_DEV, S_LOC, VW), BF16),
                pltpu.VMEM((NW, N_DEV, ROWS, UW), BF16),
                pltpu.VMEM((M, FF), F32),
                pltpu.VMEM((SEQ, 3 * NQ), BF16),
                pltpu.VMEM((SEQ, NQ), BF16),
                pltpu.VMEM((M, FF), BF16),
                pltpu.VMEM((3, N_DEV, ROWS, CW), F32),
                pltpu.VMEM((4, 4, ROWS, CW), BF16), four, two, two, one, one,
                pltpu.VMEM((8, 2, ROWS, CW), F32),
                pltpu.VMEM((B, S_LOC, D), BF16),
                pltpu.VMEM((NS, KC, NC), BF16),
                pltpu.VMEM((3, NQ, 3 * CW), BF16),
                pltpu.VMEM((1, D), F32),
                pltpu.VMEM((1, D), F32),
                pltpu.VMEM((1, FF), F32),
                dma, dma((8,)), dma, dma((NS,)), dma((5,)),
                dma, dma((NV, 3)),
                dma, dma((NW + 2, 2)), dma((NW,)),
                dma((4,)), dma((3,)), dma((NCH, 3)),
            ],
            compiler_params=pltpu.CompilerParams(collective_id=0, has_side_effects=True, vmem_limit_bytes=67_043_328),
            name="decoder_layer",
        )(hidden, jnp.transpose(w_qkv, (1, 2, 0, 3)), w_out.reshape(HEADS * HD, D), w_up, w_down,
          row(ln1_gain), row(ln1_bias), b_qkv, tile(b_out), row(ln2_gain), row(ln2_bias), tile(b_up), tile(b_down))

    in_layout = (P("dp", "tp", None), P(), P(), P(None, None, "tp", None), P(None, "tp", None), P("tp", None, None), P(), P(), P(), P(None, "tp"), P("tp"), P("tp", None), P())
    return jax.shard_map(device_body, mesh=mesh, in_specs=in_layout, out_specs=P("dp", "tp", None), check_vma=False)
```
